32 devices in a mesh: data: 1 (over z), tp: 32 (over y, x, core).
Axes of the slice: x: 4, y: 4, z: 1, core: 2. Of those that a mesh axis runs over, the one named last changes fastest.
The devices are a block of a 4x4x8 slice.
Arguments:
- x_tokens: bfloat16 [8192, 2560], P(('data', 'tp'))
- ln_gamma: float32 [2560], replicated
- w_qkv: bfloat16 [2560, 32, 240], P(None, 'tp')
- w_out: bfloat16 [32, 80, 2560], P('tp')
- w_up: bfloat16 [2560, 10240], P(None, 'tp')
- w_down: bfloat16 [10240, 2560], P('tp')
Outputs:
- output: bfloat16 [8192, 2560], P(('data', 'tp'))
All inputs are finite; a program needn't handle non-finite values.
Results may differ from the reference program's by a relative error of at most 0.00250589.
Values are sent between devices in bfloat16 or wider.
A program may use at most 768 MiB of HBM per device.

```python
import math
import jax
import jax.numpy as jnp
from jax import lax

SEQ_LEN = 8192
MODEL_DIM = 2560
FF_DIM = 10240
NUM_HEADS = 32
HEAD_DIM = MODEL_DIM // NUM_HEADS
BLOCK_ROWS = min(SEQ_LEN, 256)
N_BLOCKS = SEQ_LEN // BLOCK_ROWS
ATTN_SCALE = HEAD_DIM ** -0.5
LN_EPS = 1e-6
QK_GAIN = max(math.log(SEQ_LEN) - 2.0, 1.0) ** 0.25


def setup_inputs(seed: int = 0, part: int = 0) -> dict:
    rand_keys = jax.random.split(jax.random.key(seed), 6)
    tokens = jax.random.normal(jax.random.fold_in(rand_keys[0], part), (SEQ_LEN, MODEL_DIM), jnp.float32)
    ln_gain = 1.0 + 0.5 * jax.random.normal(rand_keys[1], (MODEL_DIM,), jnp.float32)
    qkv_gain = jnp.array([QK_GAIN, QK_GAIN, 1.0], jnp.float32).reshape(1, 1, 3, 1)
    w_qkv = jax.random.normal(rand_keys[2], (MODEL_DIM, NUM_HEADS, 3, HEAD_DIM), jnp.float32) * qkv_gain * MODEL_DIM ** -0.5
    w_out = jax.random.normal(rand_keys[3], (NUM_HEADS, HEAD_DIM, MODEL_DIM), jnp.float32) * (2.0 * MODEL_DIM ** -0.5)
    w_up = jax.random.normal(rand_keys[4], (MODEL_DIM, FF_DIM), jnp.float32) * MODEL_DIM ** -0.5
    w_down = jax.random.normal(rand_keys[5], (FF_DIM, MODEL_DIM), jnp.float32) * (1.5 * FF_DIM ** -0.5)
    return {
        "x_tokens": tokens.astype(jnp.bfloat16),
        "ln_gamma": ln_gain,
        "w_qkv": w_qkv.reshape(MODEL_DIM, NUM_HEADS, 3 * HEAD_DIM).astype(jnp.bfloat16),
        "w_out": w_out.astype(jnp.bfloat16),
        "w_up": w_up.astype(jnp.bfloat16),
        "w_down": w_down.astype(jnp.bfloat16),
    }


def layer_norm(row_vals, ln_gain):
    row_mean = jnp.mean(row_vals, axis=-1, keepdims=True)
    centered = row_vals - row_mean
    row_var = jnp.mean(centered * centered, axis=-1, keepdims=True)
    return centered * lax.rsqrt(row_var + LN_EPS) * ln_gain


def reference(x_tokens, ln_gamma, w_qkv, w_out, w_up, w_down):
    residual = x_tokens.astype(jnp.float32)
    normed = layer_norm(residual, ln_gamma).astype(jnp.bfloat16)

    def head_step(attn_acc, head_weights):
        wqkv_head, wout_head = head_weights
        qkv_rows = jnp.dot(normed, wqkv_head, preferred_element_type=jnp.float32).astype(jnp.bfloat16)
        query_rows = qkv_rows[:, :HEAD_DIM]
        key_trans = qkv_rows[:, HEAD_DIM:2 * HEAD_DIM].T
        value_rows = qkv_rows[:, 2 * HEAD_DIM:]

        def query_block(query_blk):
            scores = jnp.dot(query_blk, key_trans, preferred_element_type=jnp.float32) * ATTN_SCALE
            row_max = jnp.max(scores, axis=-1, keepdims=True)
            exp_scores = jnp.exp(scores - row_max)
            exp_sum = jnp.sum(exp_scores, axis=-1, keepdims=True)
            block_out = jnp.dot(exp_scores.astype(jnp.bfloat16), value_rows, preferred_element_type=jnp.float32)
            return (block_out / exp_sum).astype(jnp.bfloat16)

        head_out = lax.map(query_block, query_rows.reshape(N_BLOCKS, BLOCK_ROWS, HEAD_DIM)).reshape(SEQ_LEN, HEAD_DIM)
        return attn_acc + jnp.dot(head_out, wout_head, preferred_element_type=jnp.float32), None

    attn_init = jnp.zeros((SEQ_LEN, MODEL_DIM), jnp.float32)
    attn_sum = lax.scan(head_step, attn_init, (jnp.moveaxis(w_qkv, 1, 0), w_out))[0]

    def mlp_block(row_blk):
        pre_act = jnp.dot(row_blk, w_up, preferred_element_type=jnp.float32)
        hidden = jax.nn.gelu(pre_act, approximate=True).astype(jnp.bfloat16)
        return jnp.dot(hidden, w_down, preferred_element_type=jnp.float32)

    mlp_sum = lax.map(mlp_block, normed.reshape(N_BLOCKS, BLOCK_ROWS, MODEL_DIM)).reshape(SEQ_LEN, MODEL_DIM)
    return (residual + attn_sum + mlp_sum).astype(jnp.bfloat16)
```

```python
import functools
import math
import jax
import jax.numpy as jnp
from jax import lax
from jax.experimental import pallas as pl
from jax.experimental.pallas import tpu as pltpu
from jax.sharding import Mesh, PartitionSpec as P

LN_EPS = 1e-6
BF = jnp.bfloat16
F32 = jnp.float32

def split3(x):
    hi = x.astype(BF)
    r = x - hi.astype(F32)
    mid = r.astype(BF)
    lo = (r - mid.astype(F32)).astype(BF)
    return hi, mid, lo

TK = 256

def attn_kernel(hd, bq, qkv_ref, o_ref, kaug_ref, qaug_ref, sums_ref, acc_ref):
    groups, _, toks = qkv_ref.shape
    keys = groups * toks
    i = pl.program_id(0)
    per = toks // bq
    scale = hd ** -0.5 * math.log2(math.e)
    depth = kaug_ref.shape[1]
    pad = depth - 3 * hd

    @pl.when(i == 0)
    def _():
        ones = jnp.where(lax.broadcasted_iota(jnp.int32, (pad, TK), 0) < 3, 1.0, 0.0).astype(BF)
        for g in range(groups):
            for t in range(toks // TK):
                kt = qkv_ref[g, hd:2 * hd, t * TK:(t + 1) * TK]
                aug = jnp.concatenate([kt, kt, kt, ones], axis=0)
                kaug_ref[pl.ds(g * toks + t * TK, TK), :] = aug.T

    qt = qkv_ref[i // per, 0:hd, pl.ds(pl.multiple_of((i % per) * bq, bq), bq)]
    hi, mid, lo = split3(qt.astype(F32) * scale)
    qaug_ref[0:hd, :] = hi
    qaug_ref[hd:2 * hd, :] = mid
    qaug_ref[2 * hd:3 * hd, :] = lo
    qaug_ref[3 * hd:, :] = jnp.zeros((pad, bq), BF)

    def set_shift(c):
        chi, cmid, clo = split3(-c)
        row = lax.broadcasted_iota(jnp.int32, (pad, bq), 0)
        z = jnp.where(row == 0, chi.astype(F32), jnp.where(row == 1, cmid.astype(F32), jnp.where(row == 2, clo.astype(F32), 0.0)))
        qaug_ref[3 * hd:, :] = z.astype(BF)

    def scores(t):
        return jnp.dot(kaug_ref[pl.ds(t * TK, TK), :], qaug_ref[...], preferred_element_type=F32)

    def main():
        l8 = jnp.zeros((8, bq), F32)
        acc = None
        U = 4
        for u in range(keys // (TK * U)):
            ps = []
            for j in range(U):
                t = u * U + j
                p = jnp.exp2(scores(t))
                l8 = l8 + p.reshape(TK // 8, 8, bq).sum(axis=0)
                ps.append(p.astype(BF))
            k0 = u * U * TK
            vt = qkv_ref[k0 // toks, 2 * hd:3 * hd, k0 % toks:k0 % toks + U * TK]
            d = jnp.dot(vt, jnp.concatenate(ps, axis=0), preferred_element_type=F32)
            acc = d if acc is None else acc + d
        sums_ref[...] = l8
        acc_ref[...] = acc

    set_shift(jnp.max(scores(0), axis=0, keepdims=True))
    main()
    l = jnp.sum(sums_ref[...], axis=0, keepdims=True)
    ok = jnp.logical_and(jnp.max(l) < 2.0 ** 64, jnp.max(jnp.abs(acc_ref[...])) < 3e38)

    @pl.when(jnp.logical_not(ok))
    def _():
        qaug_ref[3 * hd:, :] = jnp.zeros((pad, bq), BF)
        def step(t, m):
            return jnp.maximum(m, jnp.max(scores(t), axis=0, keepdims=True))
        m = lax.fori_loop(0, keys // TK, step, jnp.full((1, bq), -jnp.inf, F32))
        set_shift(m)
        sums_ref[...] = jnp.zeros_like(sums_ref)
        acc_ref[...] = jnp.zeros_like(acc_ref)
        def again(t, c):
            p = jnp.exp2(scores(t))
            sums_ref[...] += p.reshape(TK // 8, 8, bq).sum(axis=0)
            vt = qkv_ref[t // (toks // TK), 2 * hd:3 * hd, pl.ds(pl.multiple_of((t % (toks // TK)) * TK, TK), TK)]
            acc_ref[...] += jnp.dot(vt, p.astype(BF), preferred_element_type=F32)
            return c
        lax.fori_loop(0, keys // TK, again, 0)

    o_ref[0] = (acc_ref[...] / jnp.sum(sums_ref[...], axis=0, keepdims=True)).astype(BF)

def attention(qkv, bq=512):
    groups, three, toks = qkv.shape
    hd = three // 3
    keys = groups * toks
    per = toks // bq
    return pl.pallas_call(
        functools.partial(attn_kernel, hd, bq),
        grid=(groups * per,),
        in_specs=[pl.BlockSpec((groups, three, toks), lambda i: (0, 0, 0))],
        out_specs=pl.BlockSpec((1, hd, bq), lambda i: (i // per, 0, i % per)),
        out_shape=jax.ShapeDtypeStruct((groups, hd, toks), BF),
        scratch_shapes=[pltpu.VMEM((keys, 256), BF), pltpu.VMEM((256, bq), BF), pltpu.VMEM((8, bq), F32), pltpu.VMEM((hd, bq), F32)],
        cost_estimate=pl.CostEstimate(flops=4 * keys * keys * hd, bytes_accessed=2 * keys * 4 * hd, transcendentals=keys * keys),
        name="attention",
    )(qkv)


def layer_norm(row_vals, ln_gain):
    row_mean = jnp.mean(row_vals, axis=-1, keepdims=True)
    centered = row_vals - row_mean
    row_var = jnp.mean(centered * centered, axis=-1, keepdims=True)
    return (centered * lax.rsqrt(row_var + LN_EPS) * ln_gain).astype(BF)


def solution(mesh):
    data, tp = mesh.devices.shape
    side = math.isqrt(tp // 2)
    grid = Mesh(mesh.devices.reshape(data, side, side, tp // (side * side)), ("data", "y", "x", "core"))
    col = ("y", "core")

    def local_block(x_loc, ln_gamma, w_qkv, w_out, w_up, w_down):
        residual = x_loc.astype(F32)
        normed = layer_norm(residual, ln_gamma)
        rows = lax.all_gather(normed, "x", axis=0, tiled=True)
        wqkv = lax.all_gather(w_qkv[:, 0, :], col, axis=0)
        wup = lax.all_gather(w_up, col, axis=0)
        wdown = lax.all_gather(w_down, col, axis=0, tiled=True)
        wout = lax.all_gather(w_out[0], col, axis=0, tiled=True)
        qkv = jnp.einsum("hdc,td->hct", wqkv, rows, preferred_element_type=F32).astype(BF)
        qkv = lax.all_to_all(qkv, col, split_axis=0, concat_axis=0, tiled=True)
        out = attention(qkv)
        out = lax.all_to_all(out, col, split_axis=0, concat_axis=0, tiled=True)
        pre = jnp.einsum("td,hdf->thf", rows, wup, preferred_element_type=F32)
        hidden = jax.nn.gelu(pre, approximate=True).astype(BF)
        part = jnp.dot(hidden.reshape(rows.shape[0], -1), wdown, preferred_element_type=F32)
        part = part + jnp.einsum("et,ed->td", out.reshape(-1, out.shape[2]), wout, preferred_element_type=F32)
        reduced = lax.psum_scatter(part, "x", scatter_dimension=0, tiled=True)
        return (residual + reduced).astype(BF)

    row_spec = P(("data", "y", "x", "core"), None)
    tp_axes = ("y", "x", "core")
    return jax.shard_map(
        local_block,
        mesh=grid,
        in_specs=(row_spec, P(None), P(None, tp_axes, None), P(tp_axes, None, None), P(None, tp_axes), P(tp_axes, None)),
        out_specs=row_spec,
        check_vma=False,
    )
```

```python
import functools
import math
import jax
import jax.numpy as jnp
from jax import lax
from jax.experimental import pallas as pl
from jax.experimental.pallas import tpu as pltpu
from jax.sharding import Mesh, PartitionSpec as P

LN_EPS = 1e-6
BF = jnp.bfloat16
F32 = jnp.float32
TK = 256
TRIP = 16
ROWS = 64


def attn_kernel(hd, cores, sub, qkv_ref, o_ref, kaug_ref, qaug_ref, m_ref, sa_ref, sb_ref, acc_ref):
    groups, _, toks = qkv_ref.shape
    keys = groups * toks
    bq = sa_ref.shape[1]
    subs = bq // sub
    i = pl.program_id(0)
    scale = hd ** -0.5 * math.log2(math.e)
    pad = kaug_ref.shape[1] - 3 * hd
    chunk = TRIP * TK

    def load_query(b, slot):
        b = jnp.minimum(b, 2 * pl.num_programs(0) - 1)
        dest, part = b // 2, b % 2
        for j in range(subs):
            g = (part * subs + j) * cores + dest % cores
            at = pl.multiple_of((dest // cores) * sub, sub)
            qt = qkv_ref[g, 0:hd, pl.ds(at, sub)].astype(F32) * scale
            hi = qt.astype(BF)
            rest = qt - hi.astype(F32)
            mid = rest.astype(BF)
            cols = slice(j * sub, (j + 1) * sub)
            qaug_ref[slot, 0:hd, cols] = hi
            qaug_ref[slot, hd:2 * hd, cols] = mid
            qaug_ref[slot, 2 * hd:3 * hd, cols] = (rest - mid.astype(F32)).astype(BF)

    def fold(piece, op):
        return op(piece.reshape(piece.shape[0] // 8, 8, bq), axis=0)

    @pl.when(i == 0)
    def _():
        zeros = jnp.zeros((pad, TK), BF)

        def spread(t, c):
            g = t * TK // toks
            t0 = pl.multiple_of(t * TK - g * toks, TK)
            kt = qkv_ref[g, hd:2 * hd, pl.ds(t0, TK)]
            kaug_ref[pl.ds(pl.multiple_of(t * TK, TK), TK), :] = jnp.concatenate([kt, kt, kt, zeros], axis=0).T
            return c

        lax.fori_loop(0, keys // TK, spread, 0, unroll=4)
        qaug_ref[:, 3 * hd:, :] = jnp.zeros((2, pad, bq), BF)
        load_query(0, 0)
        load_query(1, 1)

        def first(c, m8):
            at = pl.ds(pl.multiple_of(c * 4 * TK, 4 * TK), 4 * TK)
            s = jnp.dot(kaug_ref[at, :], qaug_ref[0], preferred_element_type=F32)
            sa_ref[at, :] = s
            return jnp.maximum(m8, fold(s, jnp.max))

        m8 = lax.fori_loop(0, keys // (4 * TK), first, jnp.full((8, bq), -jnp.inf, F32))
        m_ref[...] = jnp.max(m8, axis=0, keepdims=True)

    def half(s_in, s_out, slot, col):
        m = m_ref[...]
        acc_ref[...] = jnp.zeros_like(acc_ref)

        def trip(c, carry):
            m8, l8 = carry
            k0 = pl.multiple_of(c * chunk, chunk)
            total = None
            for u in range(TRIP):
                s_new = jnp.dot(kaug_ref[pl.ds(k0 + u * TK, TK), :], qaug_ref[slot], preferred_element_type=F32)
                ps = []
                for r in range(0, TK, ROWS):
                    p = jnp.exp2(s_in[pl.ds(k0 + u * TK + r, ROWS), :] - m)
                    l8 = l8 + fold(p, jnp.sum)
                    ps.append(p.astype(BF))
                at = u * TK % toks
                vt = qkv_ref[k0 // toks + u * TK // toks, 2 * hd:3 * hd, at:at + TK]
                d = jnp.dot(vt, jnp.concatenate(ps, axis=0), preferred_element_type=F32)
                total = d if total is None else total + d
                for r in range(0, TK, ROWS):
                    piece = s_new[r:r + ROWS]
                    m8 = jnp.maximum(m8, fold(piece, jnp.max))
                    s_out[pl.ds(k0 + u * TK + r, ROWS), :] = piece
            acc_ref[...] += total
            return m8, l8

        m8, l8 = lax.fori_loop(0, keys // chunk, trip, (jnp.full((8, bq), -jnp.inf, F32), jnp.zeros((8, bq), F32)))
        o_ref[0, :, col:col + bq] = (acc_ref[...] / jnp.sum(l8, axis=0, keepdims=True)).astype(BF)
        m_ref[...] = jnp.max(m8, axis=0, keepdims=True)

    half(sa_ref, sb_ref, 1, 0)
    load_query(2 * i + 2, 0)
    half(sb_ref, sa_ref, 0, bq)
    load_query(2 * i + 3, 1)


def attention(qkv, cores, side):
    groups, three, toks = qkv.shape
    hd = three // 3
    keys = groups * toks
    bq = toks // 2
    return pl.pallas_call(
        functools.partial(attn_kernel, hd, cores, toks // side),
        grid=(groups,),
        in_specs=[pl.BlockSpec((groups, three, toks), lambda i: (0, 0, 0))],
        out_specs=pl.BlockSpec((1, hd, toks), lambda i: (i, 0, 0)),
        out_shape=jax.ShapeDtypeStruct((groups, hd, toks), BF),
        scratch_shapes=[
            pltpu.VMEM((keys, 256), BF),
            pltpu.VMEM((2, 256, bq), BF),
            pltpu.VMEM((1, bq), F32),
            pltpu.VMEM((keys, bq), F32),
            pltpu.VMEM((keys, bq), F32),
            pltpu.VMEM((hd, bq), F32),
        ],
        compiler_params=pltpu.CompilerParams(vmem_limit_bytes=58 * 1024 * 1024),
        cost_estimate=pl.CostEstimate(flops=6 * keys * keys * hd, bytes_accessed=8 * keys * hd, transcendentals=keys * keys),
        name="attention",
    )(qkv)


def layer_norm(row_vals, ln_gain):
    row_mean = jnp.mean(row_vals, axis=-1, keepdims=True)
    centered = row_vals - row_mean
    row_var = jnp.mean(centered * centered, axis=-1, keepdims=True)
    return (centered * lax.rsqrt(row_var + LN_EPS) * ln_gain).astype(BF)


def ring_gather(block, axis, side):
    up = [(j, (j + 1) % side) for j in range(side)]
    down = [(j, (j - 1) % side) for j in range(side)]
    rows = block.shape[0]
    half = rows // 2
    before = lax.ppermute(block, axis, up)
    after = lax.ppermute(block, axis, down)
    far_a = lax.ppermute(before[:half], axis, up)
    far_b = lax.ppermute(after[half:], axis, down)
    me = lax.axis_index(axis)
    full = jnp.zeros((side * rows, block.shape[1]), block.dtype)
    place = lambda full, part, pos, off: lax.dynamic_update_slice(full, part, (pos % side * rows + off, 0))
    full = place(full, block, me, 0)
    full = place(full, before, me - 1 + side, 0)
    full = place(full, after, me + 1, 0)
    full = place(full, far_a, me + 2, 0)
    return place(full, far_b, me + 2, half)


def solution(mesh):
    data, tp = mesh.devices.shape
    side = math.isqrt(tp // 2)
    cores = tp // (side * side)
    grid = Mesh(mesh.devices.reshape(data, side, side, cores), ("data", "y", "x", "core"))
    row, col = ("x", "core"), ("y", "core")

    def local_block(x_loc, ln_gamma, w_qkv, w_out, w_up, w_down):
        residual = x_loc.astype(F32)
        normed = layer_norm(residual, ln_gamma)
        wqkv = lax.all_gather(w_qkv[:, 0, :].T, row, axis=0, tiled=True)
        tall = ring_gather(normed, "y", side)
        qkv = lax.dot_general(wqkv, tall, (((1,), (1,)), ((), ())), preferred_element_type=F32).astype(BF)
        qkv = qkv.reshape(side * cores, -1, tall.shape[0])
        qkv = lax.all_to_all(qkv, row, split_axis=0, concat_axis=0, tiled=True)
        qkv, normed = lax.optimization_barrier((qkv, normed))
        wide = ring_gather(normed, "x", side)
        out = attention(qkv, cores, side)
        out = lax.all_to_all(out, col, split_axis=0, concat_axis=0, tiled=True)
        out = out.reshape(-1, out.shape[2])
        wup = lax.all_gather(w_up.T, col, axis=0, tiled=True)
        wout = lax.all_gather(w_out[0], col, axis=0, tiled=True)
        wdown = lax.all_gather(w_down, col, axis=0, tiled=True)
        pre = lax.dot_general(wide, wup, (((1,), (1,)), ((), ())), preferred_element_type=F32)
        hidden = jax.nn.gelu(pre, approximate=True).astype(BF)
        width = wdown.shape[1]
        cuts = [0, width // 5, 3 * width // 5, width]
        reduced = []
        for a, b in zip(cuts[:-1], cuts[1:]):
            part = jnp.dot(hidden, wdown[:, a:b], preferred_element_type=F32)
            part = part + lax.dot_general(out, wout[:, a:b], (((0,), (0,)), ((), ())), preferred_element_type=F32)
            reduced.append(lax.psum_scatter(part, "x", scatter_dimension=0, tiled=True))
        return (residual + jnp.concatenate(reduced, axis=1)).astype(BF)

    row_spec = P(("data", "y", "x", "core"), None)
    tp_axes = ("y", "x", "core")
    return jax.shard_map(
        local_block,
        mesh=grid,
        in_specs=(row_spec, P(None), P(None, tp_axes, None), P(tp_axes, None, None), P(None, tp_axes), P(tp_axes, None)),
        out_specs=row_spec,
        check_vma=False,
    )
```

```python
import functools
import math
import jax
import jax.numpy as jnp
from jax import lax
from jax.experimental import pallas as pl
from jax.experimental.pallas import tpu as pltpu
from jax.sharding import Mesh, PartitionSpec as P

LN_EPS = 1e-6
BF = jnp.bfloat16
MESH = pl.DeviceIdType.MESH
F32 = jnp.float32
TK = 256
TRIP = 16
ROWS = 64


def attn_kernel(hd, side, cores, sub, qkv_ref, x_ref, oin_ref, wide_ref, kaug_ref, qaug_ref, sa_ref, sb_ref, acc_ref, m_ref, o_buf,
                o_send, o_recv, x_send, x_recv):
    groups, _, toks = qkv_ref.shape
    keys = groups * toks
    bq = sa_ref.shape[1]
    subs = bq // sub
    i = pl.program_id(0)
    scale = hd ** -0.5 * math.log2(math.e)
    pad = kaug_ref.shape[1] - 3 * hd
    chunk = TRIP * TK
    y, core, x = lax.axis_index("y"), lax.axis_index("core"), lax.axis_index("x")
    me = y * cores + core
    right, left = (x + 1) % side, (x + side - 1) % side
    rows = x_ref.shape[0]
    top, low = pl.ds(0, rows // 2), pl.ds(rows // 2, rows // 2)

    def x_copy(n):
        src = (x_ref, x_ref, wide_ref.at[3, top], wide_ref.at[1, low])[n]
        dst = (wide_ref.at[3], wide_ref.at[1], wide_ref.at[2, top], wide_ref.at[2, low])[n]
        return pltpu.make_async_remote_copy(
            src_ref=src, dst_ref=dst, send_sem=x_send.at[n], recv_sem=x_recv.at[n],
            device_id={"x": left if n % 2 else right}, device_id_type=MESH)

    def o_copy(step):
        to = (me + 1 + step) % groups
        return pltpu.make_async_remote_copy(
            src_ref=o_buf.at[step % 2], dst_ref=oin_ref.at[me], send_sem=o_send.at[step % 2], recv_sem=o_recv.at[step],
            device_id={"y": to // cores, "core": to % cores}, device_id_type=MESH)

    def load_query(b, slot):
        b = jnp.minimum(b, 2 * groups - 1)
        dest, part = (me + 1 + b // 2) % groups, b % 2
        for j in range(subs):
            g = (part * subs + j) * cores + dest % cores
            at = pl.multiple_of((dest // cores) * sub, sub)
            qt = qkv_ref[g, 0:hd, pl.ds(at, sub)].astype(F32) * scale
            hi = qt.astype(BF)
            rest = qt - hi.astype(F32)
            mid = rest.astype(BF)
            cols = slice(j * sub, (j + 1) * sub)
            qaug_ref[slot, 0:hd, cols] = hi
            qaug_ref[slot, hd:2 * hd, cols] = mid
            qaug_ref[slot, 2 * hd:3 * hd, cols] = (rest - mid.astype(F32)).astype(BF)

    def fold(piece, op):
        return op(piece.reshape(piece.shape[0] // 8, 8, bq), axis=0)

    @pl.when(i == 0)
    def _():
        barrier = pltpu.get_barrier_semaphore()
        for to in (right, left):
            pl.semaphore_signal(barrier, inc=1, device_id={"x": to}, device_id_type=MESH)
        for hop in range(1, groups):
            to = (me + hop) % groups
            pl.semaphore_signal(barrier, inc=1, device_id={"y": to // cores, "core": to % cores}, device_id_type=MESH)
        pl.semaphore_wait(barrier, groups + 1)
        x_copy(0).start()
        x_copy(1).start()
        zeros = jnp.zeros((pad, TK), BF)

        def spread(t, c):
            g = t * TK // toks
            t0 = pl.multiple_of(t * TK - g * toks, TK)
            kt = qkv_ref[g, hd:2 * hd, pl.ds(t0, TK)]
            kaug_ref[pl.ds(pl.multiple_of(t * TK, TK), TK), :] = jnp.concatenate([kt, kt, kt, zeros], axis=0).T
            return c

        lax.fori_loop(0, keys // TK, spread, 0, unroll=4)
        qaug_ref[:, 3 * hd:, :] = jnp.zeros((2, pad, bq), BF)
        load_query(0, 0)
        load_query(1, 1)

        def first(c, m8):
            at = pl.ds(pl.multiple_of(c * 4 * TK, 4 * TK), 4 * TK)
            s = jnp.dot(kaug_ref[at, :], qaug_ref[0], preferred_element_type=F32)
            sa_ref[at, :] = s
            return jnp.maximum(m8, fold(s, jnp.max))

        m8 = lax.fori_loop(0, keys // (4 * TK), first, jnp.full((8, bq), -jnp.inf, F32))
        m_ref[...] = jnp.broadcast_to(jnp.max(m8, axis=0, keepdims=True), (8, bq))

    @pl.when(i == groups // 2)
    def _():
        x_copy(0).wait()
        x_copy(1).wait()
        x_copy(2).start()
        x_copy(3).start()

    @pl.when(i >= 2)
    def _():
        o_copy(i - 2).wait_send()

    def half(s_in, s_out, slot, col):
        m = m_ref[0:1, :]
        acc_ref[...] = jnp.zeros_like(acc_ref)

        def trip(c, carry):
            m8, l8 = carry
            k0 = pl.multiple_of(c * chunk, chunk)
            total = None
            for u in range(TRIP):
                s_new = jnp.dot(kaug_ref[pl.ds(k0 + u * TK, TK), :], qaug_ref[slot], preferred_element_type=F32)
                ps = []
                for r in range(0, TK, ROWS):
                    p = jnp.exp2(s_in[pl.ds(k0 + u * TK + r, ROWS), :] - m)
                    l8 = l8 + fold(p, jnp.sum)
                    ps.append(p.astype(BF))
                at = u * TK % toks
                vt = qkv_ref[k0 // toks + u * TK // toks, 2 * hd:3 * hd, at:at + TK]
                d = jnp.dot(vt, jnp.concatenate(ps, axis=0), preferred_element_type=F32)
                total = d if total is None else total + d
                for r in range(0, TK, ROWS):
                    piece = s_new[r:r + ROWS]
                    m8 = jnp.maximum(m8, fold(piece, jnp.max))
                    s_out[pl.ds(k0 + u * TK + r, ROWS), :] = piece
            acc_ref[...] += total
            return m8, l8

        m8, l8 = lax.fori_loop(0, keys // chunk, trip, (jnp.full((8, bq), -jnp.inf, F32), jnp.zeros((8, bq), F32)))
        o_buf[i % 2, :, col:col + bq] = (acc_ref[...] / jnp.sum(l8, axis=0, keepdims=True)).astype(BF)
        m_ref[...] = jnp.broadcast_to(jnp.max(m8, axis=0, keepdims=True), (8, bq))

    half(sa_ref, sb_ref, 1, 0)
    load_query(2 * i + 2, 0)
    half(sb_ref, sa_ref, 0, bq)
    load_query(2 * i + 3, 1)

    @pl.when(i < groups - 1)
    def _():
        o_copy(i).start()

    @pl.when(i == groups - 1)
    def _():
        own = pltpu.make_async_copy(o_buf.at[i % 2], oin_ref.at[me], o_send.at[i % 2])
        own.start()
        x_copy(2).wait()
        x_copy(3).wait()
        for step in range(groups - 1):
            o_copy(step).wait_recv()
        o_copy(groups - 2).wait_send()
        own.wait()


def attention(qkv, normed, cores, side):
    groups, three, toks = qkv.shape
    hd = three // 3
    keys = groups * toks
    bq = toks // 2
    anywhere = pl.BlockSpec(memory_space=pl.ANY)
    return pl.pallas_call(
        functools.partial(attn_kernel, hd, side, cores, toks // side),
        grid=(groups,),
        in_specs=[pl.BlockSpec((groups, three, toks), lambda i: (0, 0, 0)), anywhere],
        out_specs=[anywhere, anywhere],
        out_shape=[
            jax.ShapeDtypeStruct((groups, hd, toks), BF),
            jax.ShapeDtypeStruct((side,) + normed.shape, BF),
        ],
        scratch_shapes=[
            pltpu.VMEM((keys, 256), BF),
            pltpu.VMEM((2, 256, bq), BF),
            pltpu.VMEM((keys, bq), F32),
            pltpu.VMEM((keys, bq), F32),
            pltpu.VMEM((hd, bq), F32),
            pltpu.VMEM((8, bq), F32),
            pltpu.VMEM((2, hd, toks), BF),
            pltpu.SemaphoreType.DMA((2,)),
            pltpu.SemaphoreType.DMA((groups - 1,)),
            pltpu.SemaphoreType.DMA((4,)),
            pltpu.SemaphoreType.DMA((4,)),
        ],
        compiler_params=pltpu.CompilerParams(vmem_limit_bytes=58 * 1024 * 1024, collective_id=1, has_side_effects=True),
        cost_estimate=pl.CostEstimate(flops=6 * keys * keys * hd, bytes_accessed=8 * keys * hd, transcendentals=keys * keys),
        name="attention",
    )(qkv, normed)


def mlp_kernel(side, x_ref, wide_ref, oin_ref, w1_ref, w2_ref, wo_ref, res_ref, y_ref, w1, w2, xv, xt, ov, hv, part, far, near, res,
               load, send, recv):
    x = lax.axis_index("x")
    right, left = (x + 1) % side, (x + side - 1) % side
    rows, model = x_ref.shape
    width = w1_ref.shape[0]
    heads = wo_ref.shape[0]
    half = rows // 2
    top, low = pl.ds(0, half), pl.ds(half, half)
    order = (2, 1, 3, 0)

    def x_load(n):
        src = x_ref if order[n] == 0 else wide_ref.at[order[n]]
        return pltpu.make_async_copy(src, xv.at[n % 2], load.at[n % 2])

    def w1_load(n):
        cut = pl.ds(n * (width // 2), width // 2)
        return pltpu.make_async_copy(w1_ref.at[cut], w1.at[cut], load.at[2 + n])

    o_load = pltpu.make_async_copy(oin_ref, ov, load.at[4])
    w2_load = pltpu.make_async_copy(w2_ref, w2.at[pl.ds(0, width)], load.at[5])
    wo_load = pltpu.make_async_copy(wo_ref, w2.at[pl.ds(width, heads)], load.at[6])
    res_load = pltpu.make_async_copy(res_ref, res, load.at[7])
    x_load(0).start()
    w1_load(0).start()
    w1_load(1).start()
    o_load.start()
    w2_load.start()
    wo_load.start()
    x_load(1).start()
    res_load.start()

    barrier = pltpu.get_barrier_semaphore()
    for to in (right, left):
        pl.semaphore_signal(barrier, inc=1, device_id={"x": to}, device_id_type=MESH)
    pl.semaphore_wait(barrier, 2)

    def put(n, src, dst, to):
        return pltpu.make_async_remote_copy(src_ref=src, dst_ref=dst, send_sem=send.at[n], recv_sem=recv.at[n],
                                            device_id={"x": to}, device_id_type=MESH)

    puts = (
        put(0, part.at[0, top], far.at[0], right),
        put(1, part.at[0, low], far.at[1], left),
        put(2, part.at[1, low], near.at[0, low], right),
        put(3, part.at[2, top], near.at[1, top], left),
        put(4, part.at[1, top], near.at[0, top], right),
        put(5, part.at[2, low], near.at[1, low], left),
    )

    def compute(n, slot):
        x_load(n).wait()

        def flip(k, c):
            at = pl.ds(pl.multiple_of(k * 256, 256), 256)
            xt[at, :] = xv[n % 2, :, at].T
            return c

        lax.fori_loop(0, model // 256, flip, 0, unroll=2)
        hd, toks = ov.shape[1:]
        col = pl.multiple_of((x + order[n]) % side * rows, rows)
        if n == 0:
            o_load.wait()
        hv[:, width:] = ov[:, :, pl.ds(col, rows)].reshape(heads, rows).T

        def hidden(f, c):
            at = pl.ds(pl.multiple_of(f * 512, 512), 512)
            pre = jnp.dot(w1[at, :], xt[...], preferred_element_type=F32)
            hv[:, at] = jax.nn.gelu(pre, approximate=True).astype(BF).T
            return c

        if n == 0:
            w1_load(0).wait()
            w1_load(1).wait()
        lax.fori_loop(0, width // 512, hidden, 0)
        if n < 2:
            x_load(n + 2).start()
        if n == 0:
            w2_load.wait()
            wo_load.wait()

        def outs(d, c):
            at = pl.ds(pl.multiple_of(d * 512, 512), 512)
            part[slot, :, at] = jnp.dot(hv[...], w2[:, at], preferred_element_type=F32)
            return c

        lax.fori_loop(0, model // 512, outs, 0)

    compute(0, 0)
    puts[0].start()
    puts[1].start()
    compute(1, 1)
    puts[2].start()
    compute(2, 2)
    puts[3].start()
    puts[0].wait()
    part[1, :half, :] += far[0]
    puts[4].start()
    puts[1].wait()
    part[2, half:, :] += far[1]
    puts[5].start()
    compute(3, 0)
    res_load.wait()
    part[0] += res[...].astype(F32)
    puts[2].wait()
    puts[3].wait()
    puts[4].wait()
    puts[5].wait()
    y_ref[...] = (part[0] + near[0] + near[1]).astype(BF)


def mlp(x_loc, normed, wide, oin, w1, w2, wo, side):
    rows, model = normed.shape
    width = w1.shape[0]
    anywhere = pl.BlockSpec(memory_space=pl.ANY)
    flops = 2 * side * rows * model * (2 * width + wo.shape[0])
    return pl.pallas_call(
        functools.partial(mlp_kernel, side),
        in_specs=[anywhere] * 7,
        out_specs=pl.BlockSpec(memory_space=pltpu.VMEM),
        out_shape=jax.ShapeDtypeStruct((rows, model), BF),
        scratch_shapes=[
            pltpu.VMEM(w1.shape, BF),
            pltpu.VMEM((width + wo.shape[0], model), BF),
            pltpu.VMEM((2, rows, model), BF),
            pltpu.VMEM((model, rows), BF),
            pltpu.VMEM(oin.shape, BF),
            pltpu.VMEM((rows, width + wo.shape[0]), BF),
            pltpu.VMEM((3, rows, model), F32),
            pltpu.VMEM((2, rows // 2, model), F32),
            pltpu.VMEM((2, rows, model), F32),
            pltpu.VMEM((rows, model), BF),
            pltpu.SemaphoreType.DMA((8,)),
            pltpu.SemaphoreType.DMA((6,)),
            pltpu.SemaphoreType.DMA((6,)),
        ],
        compiler_params=pltpu.CompilerParams(vmem_limit_bytes=62 * 1024 * 1024, collective_id=2, has_side_effects=True),
        cost_estimate=pl.CostEstimate(flops=flops, bytes_accessed=4 * model * width, transcendentals=side * rows * width),
        name="mlp",
    )(normed, wide, oin, w1, w2, wo, x_loc)


def layer_norm(row_vals, ln_gain):
    row_mean = jnp.mean(row_vals, axis=-1, keepdims=True)
    centered = row_vals - row_mean
    row_var = jnp.mean(centered * centered, axis=-1, keepdims=True)
    return (centered * lax.rsqrt(row_var + LN_EPS) * ln_gain).astype(BF)


def ring_gather(block, axis, side):
    up = [(j, (j + 1) % side) for j in range(side)]
    down = [(j, (j - 1) % side) for j in range(side)]
    rows = block.shape[0]
    half = rows // 2
    before = lax.ppermute(block, axis, up)
    after = lax.ppermute(block, axis, down)
    far_a = lax.ppermute(before[:half], axis, up)
    far_b = lax.ppermute(after[half:], axis, down)
    me = lax.axis_index(axis)
    full = jnp.zeros((side * rows, block.shape[1]), block.dtype)
    place = lambda full, part, pos, off: lax.dynamic_update_slice(full, part, (pos % side * rows + off, 0))
    full = place(full, block, me, 0)
    full = place(full, before, me - 1 + side, 0)
    full = place(full, after, me + 1, 0)
    full = place(full, far_a, me + 2, 0)
    return place(full, far_b, me + 2, half)


def solution(mesh):
    data, tp = mesh.devices.shape
    side = math.isqrt(tp // 2)
    cores = tp // (side * side)
    grid = Mesh(mesh.devices.reshape(data, side, side, cores), ("data", "y", "x", "core"))
    row, col = ("x", "core"), ("y", "core")

    def local_block(x_loc, ln_gamma, w_qkv, w_out, w_up, w_down):
        normed = layer_norm(x_loc.astype(F32), ln_gamma)
        wqkv = lax.all_gather(w_qkv[:, 0, :].T, row, axis=0, tiled=True)
        tall = ring_gather(normed, "y", side)
        qkv = lax.dot_general(wqkv, tall, (((1,), (1,)), ((), ())), preferred_element_type=F32).astype(BF)
        qkv = qkv.reshape(side * cores, -1, tall.shape[0])
        qkv = lax.all_to_all(qkv, row, split_axis=0, concat_axis=0, tiled=True)
        oin, wide = attention(qkv, normed, cores, side)
        wup = lax.all_gather(w_up.T, col, axis=0, tiled=True)
        wout = lax.all_gather(w_out[0], col, axis=0, tiled=True)
        wdown = lax.all_gather(w_down, col, axis=0, tiled=True)
        return mlp(x_loc, normed, wide, oin, wup, wdown, wout, side)

    row_spec = P(("data", "y", "x", "core"), None)
    tp_axes = ("y", "x", "core")
    return jax.shard_map(
        local_block,
        mesh=grid,
        in_specs=(row_spec, P(None), P(None, tp_axes, None), P(tp_axes, None, None), P(None, tp_axes), P(tp_axes, None)),
        out_specs=row_spec,
        check_vma=False,
    )
```

```python
import functools
import math
import jax
import jax.numpy as jnp
from jax import lax
from jax.experimental import pallas as pl
from jax.experimental.pallas import tpu as pltpu
from jax.sharding import Mesh, PartitionSpec as P

LN_EPS = 1e-6
BF = jnp.bfloat16
MESH = pl.DeviceIdType.MESH
F32 = jnp.float32
TK = 256
TRIP = 16
ROWS = 64


def ring(own, full, axis, split, send, recv):
    side, cores = lax.axis_size(axis), lax.axis_size("core")
    at, core = lax.axis_index(axis), lax.axis_index("core")
    other = (core + 1) % cores
    block = lambda hop: full.at[(at + hop) % side * cores + core]
    head, tail = pl.ds(0, split), pl.ds(split, own.shape[0] - split)
    nxt, prv, sib = {axis: (at + 1) % side}, {axis: (at + side - 1) % side}, {"core": other}
    plan = (
        (own, block(0), nxt),
        (own, block(0), prv),
        (own, block(0), sib),
        (block(side - 1).at[head], block(side - 1).at[head], nxt),
        (block(1).at[tail], block(1).at[tail], prv),
        (block(side - 1), block(side - 1), sib),
        (block(1), block(1), sib),
        (block(2), block(2), sib),
    )
    return [
        pltpu.make_async_remote_copy(
            src_ref=src, dst_ref=dst, send_sem=send.at[n], recv_sem=recv.at[n], device_id=to, device_id_type=MESH)
        for n, (src, dst, to) in enumerate(plan)
    ]


def start(copies, *which):
    for n in which:
        copies[n].start()


def arrived(copies, *which):
    for n in which:
        copies[n].wait_recv()


def meet(*places):
    barrier = pltpu.get_barrier_semaphore()
    for place in places:
        pl.semaphore_signal(barrier, inc=1, device_id=place, device_id_type=MESH)
    pl.semaphore_wait(barrier, len(places))


def qkv_kernel(side, cores, x_ref, gain_ref, wq_ref, w1_ref, qkv_ref, normed_ref, w1_full, wv, xv, xt, qk,
               wq_send, wq_recv, x_send, x_recv, w1_send, w1_recv, a_send, a_recv, local):
    y, x, core = lax.axis_index("y"), lax.axis_index("x"), lax.axis_index("core")
    rows, model = x_ref.shape
    low = rows // 2
    me = x * cores + core
    up, down = {"y": (y + 1) % side}, {"y": (y + side - 1) % side}
    meet(up, down, *[
        {"x": (x + dx) % side, "core": (core + dc) % cores} for dx in range(side) for dc in range(cores) if dx or dc])

    wq = ring(wq_ref, wv, "x", wq_ref.shape[0] // 32 * 16, wq_send, wq_recv)
    w1 = ring(w1_ref, w1_full, "y", w1_ref.shape[0] // 2, w1_send, w1_recv)
    own_wq = pltpu.make_async_copy(wq_ref, wv.at[me], local.at[0])
    own_wq.start()
    start(wq, 0, 1, 2)

    def x_copy(n, src, to):
        return pltpu.make_async_remote_copy(
            src_ref=src, dst_ref=src, send_sem=x_send.at[n], recv_sem=x_recv.at[n], device_id=to, device_id_type=MESH)

    before, after, far = (y + side - 1) % side, (y + 1) % side, (y + 2) % side
    xs = [
        x_copy(0, xv.at[y], up),
        x_copy(1, xv.at[y], down),
        x_copy(2, xv.at[before, pl.ds(0, low)], up),
        x_copy(3, xv.at[after, pl.ds(low, low)], down),
    ]

    def norm(r, c):
        at = pl.ds(pl.multiple_of(r * 32, 32), 32)
        row = x_ref[at, :].astype(F32)
        mean = jnp.mean(row, axis=-1, keepdims=True)
        centered = row - mean
        var = jnp.mean(centered * centered, axis=-1, keepdims=True)
        xv[y, at, :] = (centered * lax.rsqrt(var + LN_EPS) * gain_ref[...]).astype(BF)
        return c

    lax.fori_loop(0, rows // 32, norm, 0)

    def cols(part):
        return pl.ds(pl.multiple_of(part * rows, rows), rows)

    def flip(part):
        def piece(k, c):
            at = pl.ds(pl.multiple_of(k * 256, 256), 256)
            xt[at, cols(part)] = xv[part, :, at].T
            return c

        lax.fori_loop(0, model // 256, piece, 0, unroll=2)

    flip(y)
    start(xs, 0, 1)
    start(w1, 2, 0, 1)
    keep = pltpu.make_async_copy(xv.at[y], normed_ref, local.at[1])
    keep.start()

    def unit(head, part):
        qk[head, :, cols(part)] = jnp.dot(wv[head], xt[:, cols(part)], preferred_element_type=F32).astype(BF)

    def send(n, head):
        return pltpu.make_async_remote_copy(
            src_ref=qk.at[head], dst_ref=qkv_ref.at[me], send_sem=a_send.at[n], recv_sem=a_recv.at[n],
            device_id={"x": head // cores, "core": head % cores}, device_id_type=MESH)

    def head_of(n):
        return (x + n // cores) % side * cores + (core + n) % cores

    arrived(wq, 0, 1)
    start(wq, 3, 4, 5, 6)
    arrived(xs, 0, 1)
    start(xs, 2, 3)
    flip(before)
    flip(after)
    own_wq.wait()
    arrived(wq, 2, 5, 6)

    def near(k, c):
        n, p = k // 3, k % 3
        n = n + cores * (n // (2 * cores))
        unit(head_of(n), (y + p + p // 2) % side)
        return c

    lax.fori_loop(0, 3 * 3 * cores, near, 0)
    arrived(wq, 3, 4)
    start(wq, 7)
    arrived(xs, 2, 3)
    flip(far)

    def close(k, c):
        n = cores * (1 + 2 * (k // cores)) + k % cores
        unit(head_of(n), far)
        send(n, head_of(n)).start()
        return c

    lax.fori_loop(0, 2 * cores, close, 0)
    arrived(wq, 7)

    def distant(k, c):
        unit(head_of(2 * cores + k // side), k % side)
        return c

    for k in range(cores):
        lax.fori_loop(k * side, (k + 1) * side, distant, 0)
        send(2 * cores + k, head_of(2 * cores + k)).start()

    def home(k, c):
        unit(head_of(k), far)
        return c

    lax.fori_loop(0, cores, home, 0)
    for n in range(1, cores):
        send(n, head_of(n)).start()
    own = pltpu.make_async_copy(qk.at[me], qkv_ref.at[me], local.at[2])
    own.start()
    arrived(w1, 0, 1)
    start(w1, 3, 4, 5, 6)
    for n in range(1, side * cores):
        send(n, head_of(n)).wait()
    own.wait()
    keep.wait()
    arrived(w1, 3, 4)
    start(w1, 7)
    arrived(w1, 2, 5, 6, 7)
    for copies in (wq, w1, xs):
        for copy in copies:
            copy.wait_send()


def qkv_stage(x_loc, gain, wq, w1, cores, side):
    rows, model = x_loc.shape
    groups = side * cores
    anywhere = pl.BlockSpec(memory_space=pl.ANY)
    vmem = pl.BlockSpec(memory_space=pltpu.VMEM)
    dma = lambda n: pltpu.SemaphoreType.DMA((n,))
    return pl.pallas_call(
        functools.partial(qkv_kernel, side, cores),
        in_specs=[vmem, vmem, anywhere, anywhere],
        out_specs=[anywhere] * 3,
        out_shape=[
            jax.ShapeDtypeStruct((groups, wq.shape[0], side * rows), BF),
            jax.ShapeDtypeStruct((rows, model), BF),
            jax.ShapeDtypeStruct((groups,) + w1.shape, BF),
        ],
        scratch_shapes=[
            pltpu.VMEM((groups,) + wq.shape, BF),
            pltpu.VMEM((side, rows, model), BF),
            pltpu.VMEM((model, side * rows), BF),
            pltpu.VMEM((groups, wq.shape[0], side * rows), BF),
            dma(8), dma(8), dma(4), dma(4), dma(8), dma(8), dma(groups), dma(groups), dma(3),
        ],
        compiler_params=pltpu.CompilerParams(vmem_limit_bytes=48 * 1024 * 1024, collective_id=0, has_side_effects=True),
        cost_estimate=pl.CostEstimate(flops=2 * side * rows * model * groups * wq.shape[0], bytes_accessed=4 * w1.size, transcendentals=0),
        name="qkv",
    )(x_loc, gain, wq, w1)


def attn_kernel(hd, side, cores, sub, qkv_ref, x_ref, w2_ref, wo_ref, oin_ref, wide_ref, w2_full, wo_full, kaug_ref, qaug_ref, sa_ref,
                sb_ref, acc_ref, m_ref, o_buf, o_send, o_recv, x_send, x_recv, w2_send, w2_recv, wo_send, wo_recv):
    groups, _, toks = qkv_ref.shape
    keys = groups * toks
    bq = sa_ref.shape[1]
    subs = bq // sub
    i = pl.program_id(0)
    scale = hd ** -0.5 * math.log2(math.e)
    pad = kaug_ref.shape[1] - 3 * hd
    chunk = TRIP * TK
    y, core, x = lax.axis_index("y"), lax.axis_index("core"), lax.axis_index("x")
    me = y * cores + core
    right, left = (x + 1) % side, (x + side - 1) % side
    rows = x_ref.shape[0]
    top, low = pl.ds(0, rows // 2), pl.ds(rows // 2, rows // 2)

    def x_copy(n):
        src = (x_ref, x_ref, wide_ref.at[3, top], wide_ref.at[1, low])[n]
        dst = (wide_ref.at[3], wide_ref.at[1], wide_ref.at[2, top], wide_ref.at[2, low])[n]
        return pltpu.make_async_remote_copy(
            src_ref=src, dst_ref=dst, send_sem=x_send.at[n], recv_sem=x_recv.at[n],
            device_id={"x": left if n % 2 else right}, device_id_type=MESH)

    def o_copy(step):
        to = (me + 1 + step) % groups
        return pltpu.make_async_remote_copy(
            src_ref=o_buf.at[step % 2], dst_ref=oin_ref.at[me], send_sem=o_send.at[step % 2], recv_sem=o_recv.at[step],
            device_id={"y": to // cores, "core": to % cores}, device_id_type=MESH)

    w2 = ring(w2_ref, w2_full, "y", w2_ref.shape[0] // 2, w2_send, w2_recv)
    wo = ring(wo_ref, wo_full, "y", wo_ref.shape[0] // 32 * 16, wo_send, wo_recv)

    def load_query(b, slot):
        b = jnp.minimum(b, 2 * groups - 1)
        dest, part = (me + 1 + b // 2) % groups, b % 2
        for j in range(subs):
            g = (part * subs + j) * cores + dest % cores
            at = pl.multiple_of((dest // cores) * sub, sub)
            qt = qkv_ref[g, 0:hd, pl.ds(at, sub)].astype(F32) * scale
            hi = qt.astype(BF)
            rest = qt - hi.astype(F32)
            mid = rest.astype(BF)
            cols = slice(j * sub, (j + 1) * sub)
            qaug_ref[slot, 0:hd, cols] = hi
            qaug_ref[slot, hd:2 * hd, cols] = mid
            qaug_ref[slot, 2 * hd:3 * hd, cols] = (rest - mid.astype(F32)).astype(BF)

    def fold(piece, op):
        return op(piece.reshape(piece.shape[0] // 8, 8, bq), axis=0)

    @pl.when(i == 0)
    def _():
        meet({"x": right}, {"x": left}, *[
            {"y": (me + hop) % groups // cores, "core": (me + hop) % cores} for hop in range(1, groups)])
        start(wo, 0, 1, 2)
        start(w2, 0, 1, 2)
        x_copy(0).start()
        x_copy(1).start()
        zeros = jnp.zeros((pad, TK), BF)

        def spread(t, c):
            g = t * TK // toks
            t0 = pl.multiple_of(t * TK - g * toks, TK)
            kt = qkv_ref[g, hd:2 * hd, pl.ds(t0, TK)]
            kaug_ref[pl.ds(pl.multiple_of(t * TK, TK), TK), :] = jnp.concatenate([kt, kt, kt, zeros], axis=0).T
            return c

        lax.fori_loop(0, keys // TK, spread, 0, unroll=4)
        qaug_ref[:, 3 * hd:, :] = jnp.zeros((2, pad, bq), BF)
        load_query(0, 0)
        load_query(1, 1)

        def first(c, m8):
            at = pl.ds(pl.multiple_of(c * 4 * TK, 4 * TK), 4 * TK)
            s = jnp.dot(kaug_ref[at, :], qaug_ref[0], preferred_element_type=F32)
            sa_ref[at, :] = s
            return jnp.maximum(m8, fold(s, jnp.max))

        m8 = lax.fori_loop(0, keys // (4 * TK), first, jnp.full((8, bq), -jnp.inf, F32))
        m_ref[...] = jnp.broadcast_to(jnp.max(m8, axis=0, keepdims=True), (8, bq))

    @pl.when(i == groups // 2)
    def _():
        x_copy(0).wait()
        x_copy(1).wait()
        x_copy(2).start()
        x_copy(3).start()
        for copies in (wo, w2):
            arrived(copies, 0, 1)
            start(copies, 3, 4, 5, 6)

    @pl.when(i == groups - 1)
    def _():
        for copies in (wo, w2):
            arrived(copies, 3, 4)
            start(copies, 7)

    @pl.when(i >= 2)
    def _():
        o_copy(i - 2).wait_send()

    def half(s_in, s_out, slot, col):
        m = m_ref[0:1, :]
        acc_ref[...] = jnp.zeros_like(acc_ref)

        def trip(c, carry):
            m8, l8 = carry
            k0 = pl.multiple_of(c * chunk, chunk)
            total = None
            for u in range(TRIP):
                s_new = jnp.dot(kaug_ref[pl.ds(k0 + u * TK, TK), :], qaug_ref[slot], preferred_element_type=F32)
                ps = []
                for r in range(0, TK, ROWS):
                    p = jnp.exp2(s_in[pl.ds(k0 + u * TK + r, ROWS), :] - m)
                    l8 = l8 + fold(p, jnp.sum)
                    ps.append(p.astype(BF))
                at = u * TK % toks
                vt = qkv_ref[k0 // toks + u * TK // toks, 2 * hd:3 * hd, at:at + TK]
                d = jnp.dot(vt, jnp.concatenate(ps, axis=0), preferred_element_type=F32)
                total = d if total is None else total + d
                for r in range(0, TK, ROWS):
                    piece = s_new[r:r + ROWS]
                    m8 = jnp.maximum(m8, fold(piece, jnp.max))
                    s_out[pl.ds(k0 + u * TK + r, ROWS), :] = piece
            acc_ref[...] += total
            return m8, l8

        m8, l8 = lax.fori_loop(0, keys // chunk, trip, (jnp.full((8, bq), -jnp.inf, F32), jnp.zeros((8, bq), F32)))
        o_buf[i % 2, :, col:col + bq] = (acc_ref[...] / jnp.sum(l8, axis=0, keepdims=True)).astype(BF)
        m_ref[...] = jnp.broadcast_to(jnp.max(m8, axis=0, keepdims=True), (8, bq))

    half(sa_ref, sb_ref, 1, 0)
    load_query(2 * i + 2, 0)
    half(sb_ref, sa_ref, 0, bq)
    load_query(2 * i + 3, 1)

    @pl.when(i < groups - 1)
    def _():
        o_copy(i).start()

    @pl.when(i == groups - 1)
    def _():
        own = pltpu.make_async_copy(o_buf.at[i % 2], oin_ref.at[me], o_send.at[i % 2])
        own.start()
        x_copy(2).wait()
        x_copy(3).wait()
        for step in range(groups - 1):
            o_copy(step).wait_recv()
        o_copy(groups - 2).wait_send()
        own.wait()
        for copies in (wo, w2):
            arrived(copies, 2, 5, 6, 7)
            for copy in copies:
                copy.wait_send()


def attention(qkv, normed, w2, wo, cores, side):
    groups, three, toks = qkv.shape
    hd = three // 3
    keys = groups * toks
    bq = toks // 2
    anywhere = pl.BlockSpec(memory_space=pl.ANY)
    return pl.pallas_call(
        functools.partial(attn_kernel, hd, side, cores, toks // side),
        grid=(groups,),
        in_specs=[pl.BlockSpec((groups, three, toks), lambda i: (0, 0, 0)), anywhere, anywhere, anywhere],
        out_specs=[anywhere] * 4,
        out_shape=[
            jax.ShapeDtypeStruct((groups, hd, toks), BF),
            jax.ShapeDtypeStruct((side,) + normed.shape, BF),
            jax.ShapeDtypeStruct((groups,) + w2.shape, BF),
            jax.ShapeDtypeStruct((groups,) + wo.shape, BF),
        ],
        scratch_shapes=[
            pltpu.VMEM((keys, 256), BF),
            pltpu.VMEM((2, 256, bq), BF),
            pltpu.VMEM((keys, bq), F32),
            pltpu.VMEM((keys, bq), F32),
            pltpu.VMEM((hd, bq), F32),
            pltpu.VMEM((8, bq), F32),
            pltpu.VMEM((2, hd, toks), BF),
            pltpu.SemaphoreType.DMA((2,)),
            pltpu.SemaphoreType.DMA((groups - 1,)),
            pltpu.SemaphoreType.DMA((4,)),
            pltpu.SemaphoreType.DMA((4,)),
            pltpu.SemaphoreType.DMA((8,)),
            pltpu.SemaphoreType.DMA((8,)),
            pltpu.SemaphoreType.DMA((8,)),
            pltpu.SemaphoreType.DMA((8,)),
        ],
        compiler_params=pltpu.CompilerParams(vmem_limit_bytes=58 * 1024 * 1024, collective_id=1, has_side_effects=True),
        cost_estimate=pl.CostEstimate(flops=6 * keys * keys * hd, bytes_accessed=8 * keys * hd, transcendentals=keys * keys),
        name="attention",
    )(qkv, normed, w2, wo)


def mlp_kernel(side, cores, x_ref, wide_ref, oin_ref, w1_own, w2_own, wo_own, w1_ref, w2_ref, wo_ref, res_ref, y_ref, w1, w2, xv, xt, ov,
               hv, part, far, near, res, load, send, recv):
    x = lax.axis_index("x")
    right, left = (x + 1) % side, (x + side - 1) % side
    rows, model = x_ref.shape
    groups = w1_ref.shape[0]
    width = groups * w1_own.shape[0]
    heads = groups * wo_own.shape[0]
    half = rows // 2
    me = lax.axis_index("y") * cores + lax.axis_index("core")
    top, low = pl.ds(0, half), pl.ds(half, half)
    order = (2, 1, 3, 0)

    def x_load(n):
        src = x_ref if order[n] == 0 else wide_ref.at[order[n]]
        return pltpu.make_async_copy(src, xv.at[n % 2], load.at[n % 2])

    def gathered(own, full, into, base, sem):
        size = own.shape[0]
        for hop in range(groups):
            slot = (me + hop) % groups
            to = into.at[pl.ds(pl.multiple_of(base + slot * size, 16), size)]
            pltpu.make_async_copy(full.at[slot] if hop else own, to, sem).start()
        whole = into.at[pl.ds(base, groups * size)]
        return pltpu.make_async_copy(whole, whole, sem)

    o_load = pltpu.make_async_copy(oin_ref, ov, load.at[2])
    res_load = pltpu.make_async_copy(res_ref, res, load.at[3])
    x_load(0).start()
    w1_load = gathered(w1_own, w1_ref, w1, 0, load.at[4])
    o_load.start()
    w2_load = gathered(w2_own, w2_ref, w2, 0, load.at[5])
    wo_load = gathered(wo_own, wo_ref, w2, width, load.at[6])
    x_load(1).start()
    res_load.start()
    meet({"x": right}, {"x": left})

    def put(n, src, dst, to):
        return pltpu.make_async_remote_copy(src_ref=src, dst_ref=dst, send_sem=send.at[n], recv_sem=recv.at[n],
                                            device_id={"x": to}, device_id_type=MESH)

    puts = (
        put(0, part.at[0, top], far.at[0], right),
        put(1, part.at[0, low], far.at[1], left),
        put(2, part.at[1, low], near.at[0, low], right),
        put(3, part.at[2, top], near.at[1, top], left),
        put(4, part.at[1, top], near.at[0, top], right),
        put(5, part.at[2, low], near.at[1, low], left),
    )

    def compute(n, slot):
        x_load(n).wait()

        def flip(k, c):
            at = pl.ds(pl.multiple_of(k * 256, 256), 256)
            xt[at, :] = xv[n % 2, :, at].T
            return c

        lax.fori_loop(0, model // 256, flip, 0, unroll=2)
        hd, toks = ov.shape[1:]
        col = pl.multiple_of((x + order[n]) % side * rows, rows)
        if n == 0:
            o_load.wait()
        hv[:, width:] = ov[:, :, pl.ds(col, rows)].reshape(heads, rows).T

        def hidden(f, c):
            at = pl.ds(pl.multiple_of(f * 512, 512), 512)
            pre = jnp.dot(w1[at, :], xt[...], preferred_element_type=F32)
            hv[:, at] = jax.nn.gelu(pre, approximate=True).astype(BF).T
            return c

        if n == 0:
            w1_load.wait()
        lax.fori_loop(0, width // 512, hidden, 0)
        if n < 2:
            x_load(n + 2).start()
        if n == 0:
            w2_load.wait()
            wo_load.wait()

        def outs(d, c):
            at = pl.ds(pl.multiple_of(d * 512, 512), 512)
            part[slot, :, at] = jnp.dot(hv[...], w2[:, at], preferred_element_type=F32)
            return c

        lax.fori_loop(0, model // 512, outs, 0)

    compute(0, 0)
    puts[0].start()
    puts[1].start()
    compute(1, 1)
    puts[2].start()
    compute(2, 2)
    puts[3].start()
    puts[0].wait()
    part[1, :half, :] += far[0]
    puts[4].start()
    puts[1].wait()
    part[2, half:, :] += far[1]
    puts[5].start()
    compute(3, 0)
    res_load.wait()
    part[0] += res[...].astype(F32)
    puts[2].wait()
    puts[3].wait()
    puts[4].wait()
    puts[5].wait()
    y_ref[...] = (part[0] + near[0] + near[1]).astype(BF)


def mlp(x_loc, normed, wide, oin, own, full, cores, side):
    rows, model = normed.shape
    groups = side * cores
    width, heads = groups * own[0].shape[0], groups * own[2].shape[0]
    anywhere = pl.BlockSpec(memory_space=pl.ANY)
    flops = 2 * side * rows * model * (2 * width + heads)
    return pl.pallas_call(
        functools.partial(mlp_kernel, side, cores),
        in_specs=[anywhere] * 10,
        out_specs=pl.BlockSpec(memory_space=pltpu.VMEM),
        out_shape=jax.ShapeDtypeStruct((rows, model), BF),
        scratch_shapes=[
            pltpu.VMEM((width, model), BF),
            pltpu.VMEM((width + heads, model), BF),
            pltpu.VMEM((2, rows, model), BF),
            pltpu.VMEM((model, rows), BF),
            pltpu.VMEM(oin.shape, BF),
            pltpu.VMEM((rows, width + heads), BF),
            pltpu.VMEM((3, rows, model), F32),
            pltpu.VMEM((2, rows // 2, model), F32),
            pltpu.VMEM((2, rows, model), F32),
            pltpu.VMEM((rows, model), BF),
            pltpu.SemaphoreType.DMA((7,)),
            pltpu.SemaphoreType.DMA((6,)),
            pltpu.SemaphoreType.DMA((6,)),
        ],
        compiler_params=pltpu.CompilerParams(vmem_limit_bytes=62 * 1024 * 1024, collective_id=2, has_side_effects=True),
        cost_estimate=pl.CostEstimate(flops=flops, bytes_accessed=4 * model * width, transcendentals=side * rows * width),
        name="mlp",
    )(normed, wide, oin, *own, *full, x_loc)


def solution(mesh):
    data, tp = mesh.devices.shape
    side = math.isqrt(tp // 2)
    cores = tp // (side * side)
    grid = Mesh(mesh.devices.reshape(data, side, side, cores), ("data", "y", "x", "core"))

    def local_block(x_loc, ln_gamma, w_qkv, w_out, w_up, w_down):
        own = (w_up.T, w_down, w_out[0])
        qkv, normed, w1 = qkv_stage(x_loc, ln_gamma[None], w_qkv[:, 0, :].T, own[0], cores, side)
        oin, wide, w2, wo = attention(qkv, normed, own[1], own[2], cores, side)
        return mlp(x_loc, normed, wide, oin, own, (w1, w2, wo), cores, side)

    row_spec = P(("data", "y", "x", "core"), None)
    tp_axes = ("y", "x", "core")
    return jax.shard_map(
        local_block,
        mesh=grid,
        in_specs=(row_spec, P(None), P(None, tp_axes, None), P(tp_axes, None, None), P(None, tp_axes), P(tp_axes, None)),
        out_specs=row_spec,
        check_vma=False,
    )
```

```python
import functools
import math
import jax
import jax.numpy as jnp
from jax import lax
from jax.experimental import pallas as pl
from jax.experimental.pallas import tpu as pltpu
from jax.sharding import Mesh, PartitionSpec as P

LN_EPS = 1e-6
BF = jnp.bfloat16
MESH = pl.DeviceIdType.MESH
F32 = jnp.float32
TK = 256
TRIP = 16
ROWS = 64


def ring(own, slot, axis, split, send, recv):
    side, cores = lax.axis_size(axis), lax.axis_size("core")
    at, core = lax.axis_index(axis), lax.axis_index("core")
    other = (core + 1) % cores
    block = lambda hop: slot((at + hop) % side * cores + core)
    head, tail = pl.ds(0, split), pl.ds(split, own.shape[0] - split)
    nxt, prv, sib = {axis: (at + 1) % side}, {axis: (at + side - 1) % side}, {"core": other}
    plan = (
        (own, block(0), nxt),
        (own, block(0), prv),
        (own, block(0), sib),
        (block(side - 1).at[head], block(side - 1).at[head], nxt),
        (block(1).at[tail], block(1).at[tail], prv),
        (block(side - 1), block(side - 1), sib),
        (block(1), block(1), sib),
        (block(2), block(2), sib),
    )
    return [
        pltpu.make_async_remote_copy(
            src_ref=src, dst_ref=dst, send_sem=send.at[n], recv_sem=recv.at[n], device_id=to, device_id_type=MESH)
        for n, (src, dst, to) in enumerate(plan)
    ]


def start(copies, *which):
    for n in which:
        copies[n].start()


def arrived(copies, *which):
    for n in which:
        copies[n].wait_recv()


def meet(*places):
    barrier = pltpu.get_barrier_semaphore()
    for place in places:
        pl.semaphore_signal(barrier, inc=1, device_id=place, device_id_type=MESH)
    pl.semaphore_wait(barrier, len(places))


def qkv_kernel(side, cores, x_ref, gain_ref, wq_ref, w1_ref, qkv_ref, normed_ref, w1_full, wv, xv, xt, qk,
               wq_send, wq_recv, x_send, x_recv, w1_send, w1_recv, a_send, a_recv, local):
    y, x, core = lax.axis_index("y"), lax.axis_index("x"), lax.axis_index("core")
    rows, model = x_ref.shape
    low = rows // 2
    me = x * cores + core
    up, down = {"y": (y + 1) % side}, {"y": (y + side - 1) % side}
    meet(up, down, *[
        {"x": (x + dx) % side, "core": (core + dc) % cores} for dx in range(side) for dc in range(cores) if dx or dc])

    wq = ring(wq_ref, lambda n: wv.at[n], "x", wq_ref.shape[0] // 32 * 16, wq_send, wq_recv)
    w1 = ring(w1_ref, lambda n: w1_full.at[n], "y", w1_ref.shape[0] // 2, w1_send, w1_recv)
    own_wq = pltpu.make_async_copy(wq_ref, wv.at[me], local.at[0])
    own_wq.start()
    start(wq, 0, 1, 2)

    def x_copy(n, src, to):
        return pltpu.make_async_remote_copy(
            src_ref=src, dst_ref=src, send_sem=x_send.at[n], recv_sem=x_recv.at[n], device_id=to, device_id_type=MESH)

    before, after, far = (y + side - 1) % side, (y + 1) % side, (y + 2) % side
    xs = [
        x_copy(0, xv.at[y], up),
        x_copy(1, xv.at[y], down),
        x_copy(2, xv.at[before, pl.ds(0, low)], up),
        x_copy(3, xv.at[after, pl.ds(low, low)], down),
    ]

    def norm(r, c):
        at = pl.ds(pl.multiple_of(r * 32, 32), 32)
        row = x_ref[at, :].astype(F32)
        mean = jnp.mean(row, axis=-1, keepdims=True)
        centered = row - mean
        var = jnp.mean(centered * centered, axis=-1, keepdims=True)
        xv[y, at, :] = (centered * lax.rsqrt(var + LN_EPS) * gain_ref[...]).astype(BF)
        return c

    lax.fori_loop(0, rows // 32, norm, 0)

    def cols(part):
        return pl.ds(pl.multiple_of(part * rows, rows), rows)

    def flip(part):
        def piece(k, c):
            at = pl.ds(pl.multiple_of(k * 256, 256), 256)
            xt[at, cols(part)] = xv[part, :, at].T
            return c

        lax.fori_loop(0, model // 256, piece, 0, unroll=2)

    flip(y)
    start(xs, 0, 1)
    start(w1, 2)
    keep = pltpu.make_async_copy(xv.at[y], normed_ref, local.at[1])
    keep.start()

    def unit(head, part):
        qk[head, :, cols(part)] = jnp.dot(wv[head], xt[:, cols(part)], preferred_element_type=F32).astype(BF)

    def send(n, head):
        return pltpu.make_async_remote_copy(
            src_ref=qk.at[head], dst_ref=qkv_ref.at[me], send_sem=a_send.at[n], recv_sem=a_recv.at[n],
            device_id={"x": head // cores, "core": head % cores}, device_id_type=MESH)

    def head_of(n):
        return (x + n // cores) % side * cores + (core + n) % cores

    arrived(wq, 0, 1)
    start(wq, 3, 4, 5, 6)
    arrived(xs, 0, 1)
    start(xs, 2, 3)
    start(w1, 0, 1)
    flip(before)
    flip(after)
    own_wq.wait()
    arrived(wq, 2, 5, 6)

    def near(k, c):
        n, p = k // 3, k % 3
        n = n + cores * (n // (2 * cores))
        unit(head_of(n), (y + p + p // 2) % side)
        return c

    lax.fori_loop(0, 3 * 3 * cores, near, 0)
    arrived(wq, 3, 4)
    start(wq, 7)
    arrived(xs, 2, 3)
    flip(far)

    def close(k, c):
        n = cores * (1 + 2 * (k // cores)) + k % cores
        unit(head_of(n), far)
        send(n, head_of(n)).start()
        return c

    lax.fori_loop(0, 2 * cores, close, 0)
    arrived(wq, 7)

    def distant(k, c):
        unit(head_of(2 * cores + k // side), k % side)
        return c

    for k in range(cores):
        lax.fori_loop(k * side, (k + 1) * side, distant, 0)
        send(2 * cores + k, head_of(2 * cores + k)).start()

    def home(k, c):
        unit(head_of(k), far)
        return c

    lax.fori_loop(0, cores, home, 0)
    for n in range(1, cores):
        send(n, head_of(n)).start()
    own = pltpu.make_async_copy(qk.at[me], qkv_ref.at[me], local.at[2])
    own.start()
    arrived(w1, 0, 1)
    start(w1, 3, 4, 5, 6)
    for n in range(1, side * cores):
        send(n, head_of(n)).wait()
    own.wait()
    keep.wait()
    arrived(w1, 3, 4)
    start(w1, 7)
    arrived(w1, 2, 5, 6, 7)
    for copies in (wq, w1, xs):
        for copy in copies:
            copy.wait_send()


def qkv_stage(x_loc, gain, wq, w1, cores, side):
    rows, model = x_loc.shape
    groups = side * cores
    anywhere = pl.BlockSpec(memory_space=pl.ANY)
    vmem = pl.BlockSpec(memory_space=pltpu.VMEM)
    dma = lambda n: pltpu.SemaphoreType.DMA((n,))
    return pl.pallas_call(
        functools.partial(qkv_kernel, side, cores),
        in_specs=[vmem, vmem, anywhere, anywhere],
        out_specs=[anywhere] * 3,
        out_shape=[
            jax.ShapeDtypeStruct((groups, wq.shape[0], side * rows), BF),
            jax.ShapeDtypeStruct((rows, model), BF),
            jax.ShapeDtypeStruct((groups,) + w1.shape, BF),
        ],
        scratch_shapes=[
            pltpu.VMEM((groups,) + wq.shape, BF),
            pltpu.VMEM((side, rows, model), BF),
            pltpu.VMEM((model, side * rows), BF),
            pltpu.VMEM((groups, wq.shape[0], side * rows), BF),
            dma(8), dma(8), dma(4), dma(4), dma(8), dma(8), dma(groups), dma(groups), dma(3),
        ],
        compiler_params=pltpu.CompilerParams(vmem_limit_bytes=58 * 1024 * 1024, collective_id=0, has_side_effects=True),
        cost_estimate=pl.CostEstimate(flops=2 * side * rows * model * groups * wq.shape[0], bytes_accessed=4 * w1.size, transcendentals=0),
        name="qkv",
    )(x_loc, gain, wq, w1)


def attn_kernel(hd, side, cores, sub, qkv_ref, x_ref, w2_ref, wo_ref, oin_ref, wide_ref, w2_full, wo_full, kaug_ref, qaug_ref, sa_ref,
                sb_ref, acc_ref, m_ref, o_buf, o_send, o_recv, x_send, x_recv, w2_send, w2_recv, wo_send, wo_recv):
    groups, _, toks = qkv_ref.shape
    keys = groups * toks
    bq = sa_ref.shape[1]
    subs = bq // sub
    i = pl.program_id(0)
    scale = hd ** -0.5 * math.log2(math.e)
    pad = kaug_ref.shape[1] - 3 * hd
    chunk = TRIP * TK
    y, core, x = lax.axis_index("y"), lax.axis_index("core"), lax.axis_index("x")
    me = y * cores + core
    right, left = (x + 1) % side, (x + side - 1) % side
    rows = x_ref.shape[0]
    top, low = pl.ds(0, rows // 2), pl.ds(rows // 2, rows // 2)

    def x_copy(n):
        src = (x_ref, x_ref, wide_ref.at[3, top], wide_ref.at[1, low])[n]
        dst = (wide_ref.at[3], wide_ref.at[1], wide_ref.at[2, top], wide_ref.at[2, low])[n]
        return pltpu.make_async_remote_copy(
            src_ref=src, dst_ref=dst, send_sem=x_send.at[n], recv_sem=x_recv.at[n],
            device_id={"x": left if n % 2 else right}, device_id_type=MESH)

    def o_copy(step):
        to = (me + 1 + step) % groups
        return pltpu.make_async_remote_copy(
            src_ref=o_buf.at[step % 2], dst_ref=oin_ref.at[me], send_sem=o_send.at[step % 2], recv_sem=o_recv.at[step],
            device_id={"y": to // cores, "core": to % cores}, device_id_type=MESH)

    w2 = ring(w2_ref.at[:, pl.ds(0, w2_full.shape[2])], lambda n: w2_full.at[n], "y", w2_ref.shape[0] // 2, w2_send, w2_recv)
    wo = ring(wo_ref, lambda n: wo_full.at[n], "y", wo_ref.shape[0] // 32 * 16, wo_send, wo_recv)

    def load_query(b, slot):
        b = jnp.minimum(b, 2 * groups - 1)
        dest, part = (me + 1 + b // 2) % groups, b % 2
        for j in range(subs):
            g = (part * subs + j) * cores + dest % cores
            at = pl.multiple_of((dest // cores) * sub, sub)
            qt = qkv_ref[g, 0:hd, pl.ds(at, sub)].astype(F32) * scale
            hi = qt.astype(BF)
            rest = qt - hi.astype(F32)
            mid = rest.astype(BF)
            cols = slice(j * sub, (j + 1) * sub)
            qaug_ref[slot, 0:hd, cols] = hi
            qaug_ref[slot, hd:2 * hd, cols] = mid
            qaug_ref[slot, 2 * hd:3 * hd, cols] = (rest - mid.astype(F32)).astype(BF)

    def fold(piece, op):
        return op(piece.reshape(piece.shape[0] // 8, 8, bq), axis=0)

    @pl.when(i == 0)
    def _():
        meet({"x": right}, {"x": left}, *[
            {"y": (me + hop) % groups // cores, "core": (me + hop) % cores} for hop in range(1, groups)])
        start(wo, 0, 1, 2)
        start(w2, 0, 1, 2)
        x_copy(0).start()
        x_copy(1).start()
        zeros = jnp.zeros((pad, TK), BF)

        def spread(t, c):
            g = t * TK // toks
            t0 = pl.multiple_of(t * TK - g * toks, TK)
            kt = qkv_ref[g, hd:2 * hd, pl.ds(t0, TK)]
            kaug_ref[pl.ds(pl.multiple_of(t * TK, TK), TK), :] = jnp.concatenate([kt, kt, kt, zeros], axis=0).T
            return c

        lax.fori_loop(0, keys // TK, spread, 0, unroll=4)
        qaug_ref[:, 3 * hd:, :] = jnp.zeros((2, pad, bq), BF)
        load_query(0, 0)
        load_query(1, 1)

        def first(c, m8):
            at = pl.ds(pl.multiple_of(c * 4 * TK, 4 * TK), 4 * TK)
            s = jnp.dot(kaug_ref[at, :], qaug_ref[0], preferred_element_type=F32)
            sa_ref[at, :] = s
            return jnp.maximum(m8, fold(s, jnp.max))

        m8 = lax.fori_loop(0, keys // (4 * TK), first, jnp.full((8, bq), -jnp.inf, F32))
        m_ref[...] = jnp.broadcast_to(jnp.max(m8, axis=0, keepdims=True), (8, bq))

    @pl.when(i == groups // 2)
    def _():
        x_copy(0).wait()
        x_copy(1).wait()
        x_copy(2).start()
        x_copy(3).start()
        for copies in (wo, w2):
            arrived(copies, 0, 1)
            start(copies, 3, 4, 5, 6)

    @pl.when(i == groups - 1)
    def _():
        for copies in (wo, w2):
            arrived(copies, 3, 4)
            start(copies, 7)

    @pl.when(i >= 2)
    def _():
        o_copy(i - 2).wait_send()

    def half(s_in, s_out, slot, col):
        m = m_ref[0:1, :]
        acc_ref[...] = jnp.zeros_like(acc_ref)

        def trip(c, carry):
            m8, l8 = carry
            k0 = pl.multiple_of(c * chunk, chunk)
            total = None
            for u in range(TRIP):
                s_new = jnp.dot(kaug_ref[pl.ds(k0 + u * TK, TK), :], qaug_ref[slot], preferred_element_type=F32)
                ps = []
                for r in range(0, TK, ROWS):
                    p = jnp.exp2(s_in[pl.ds(k0 + u * TK + r, ROWS), :] - m)
                    l8 = l8 + fold(p, jnp.sum)
                    ps.append(p.astype(BF))
                at = u * TK % toks
                vt = qkv_ref[k0 // toks + u * TK // toks, 2 * hd:3 * hd, at:at + TK]
                d = jnp.dot(vt, jnp.concatenate(ps, axis=0), preferred_element_type=F32)
                total = d if total is None else total + d
                for r in range(0, TK, ROWS):
                    piece = s_new[r:r + ROWS]
                    m8 = jnp.maximum(m8, fold(piece, jnp.max))
                    s_out[pl.ds(k0 + u * TK + r, ROWS), :] = piece
            acc_ref[...] += total
            return m8, l8

        m8, l8 = lax.fori_loop(0, keys // chunk, trip, (jnp.full((8, bq), -jnp.inf, F32), jnp.zeros((8, bq), F32)))
        o_buf[i % 2, :, col:col + bq] = (acc_ref[...] / jnp.sum(l8, axis=0, keepdims=True)).astype(BF)
        m_ref[...] = jnp.broadcast_to(jnp.max(m8, axis=0, keepdims=True), (8, bq))

    half(sa_ref, sb_ref, 1, 0)
    load_query(2 * i + 2, 0)
    half(sb_ref, sa_ref, 0, bq)
    load_query(2 * i + 3, 1)

    @pl.when(i < groups - 1)
    def _():
        o_copy(i).start()

    @pl.when(i == groups - 1)
    def _():
        own = pltpu.make_async_copy(o_buf.at[i % 2], oin_ref.at[me], o_send.at[i % 2])
        own.start()
        x_copy(2).wait()
        x_copy(3).wait()
        for step in range(groups - 1):
            o_copy(step).wait_recv()
        o_copy(groups - 2).wait_send()
        own.wait()
        for copies in (wo, w2):
            arrived(copies, 2, 5, 6, 7)
            for copy in copies:
                copy.wait_send()


def first_columns(model):
    return model * 2 // 5 // 256 * 256


def attention(qkv, normed, w2, wo, cores, side):
    groups, three, toks = qkv.shape
    hd = three // 3
    keys = groups * toks
    bq = toks // 2
    anywhere = pl.BlockSpec(memory_space=pl.ANY)
    return pl.pallas_call(
        functools.partial(attn_kernel, hd, side, cores, toks // side),
        grid=(groups,),
        in_specs=[pl.BlockSpec((groups, three, toks), lambda i: (0, 0, 0)), anywhere, anywhere, anywhere],
        out_specs=[anywhere] * 4,
        out_shape=[
            jax.ShapeDtypeStruct((groups, hd, toks), BF),
            jax.ShapeDtypeStruct((side,) + normed.shape, BF),
            jax.ShapeDtypeStruct((groups, w2.shape[0], first_columns(w2.shape[1])), BF),
            jax.ShapeDtypeStruct((groups,) + wo.shape, BF),
        ],
        scratch_shapes=[
            pltpu.VMEM((keys, 256), BF),
            pltpu.VMEM((2, 256, bq), BF),
            pltpu.VMEM((keys, bq), F32),
            pltpu.VMEM((keys, bq), F32),
            pltpu.VMEM((hd, bq), F32),
            pltpu.VMEM((8, bq), F32),
            pltpu.VMEM((2, hd, toks), BF),
            pltpu.SemaphoreType.DMA((2,)),
            pltpu.SemaphoreType.DMA((groups - 1,)),
            pltpu.SemaphoreType.DMA((4,)),
            pltpu.SemaphoreType.DMA((4,)),
            pltpu.SemaphoreType.DMA((8,)),
            pltpu.SemaphoreType.DMA((8,)),
            pltpu.SemaphoreType.DMA((8,)),
            pltpu.SemaphoreType.DMA((8,)),
        ],
        compiler_params=pltpu.CompilerParams(vmem_limit_bytes=58 * 1024 * 1024, collective_id=1, has_side_effects=True),
        cost_estimate=pl.CostEstimate(flops=6 * keys * keys * hd, bytes_accessed=8 * keys * hd, transcendentals=keys * keys),
        name="attention",
    )(qkv, normed, w2, wo)


def mlp_kernel(side, cores, x_ref, wide_ref, oin_ref, w1_own, w2_own, wo_own, w1_ref, w2_ref, wo_ref, res_ref, y_ref, w1, w2, xv, xt, ov,
               hv, part, far, near, res, load, send, recv, w2_send, w2_recv):
    x, y = lax.axis_index("x"), lax.axis_index("y")
    right, left = {"x": (x + 1) % side}, {"x": (x + side - 1) % side}
    rows, model = x_ref.shape
    groups = w1_ref.shape[0]
    width = groups * w1_own.shape[0]
    heads = groups * wo_own.shape[0]
    cut = w2_ref.shape[2]
    step = math.gcd(cut, model - cut, 512)
    half = rows // 2
    me = y * cores + lax.axis_index("core")
    top, low = pl.ds(0, half), pl.ds(half, half)
    order = (2, 1, 3, 0)

    def x_load(n):
        src = x_ref if order[n] == 0 else wide_ref.at[order[n]]
        return pltpu.make_async_copy(src, xv.at[n % 2], load.at[n % 2])

    def shard(into, base, size, n, columns):
        return into.at[pl.ds(pl.multiple_of(base + n * size, 16), size), columns]

    def gathered(own, full, into, base, sem):
        size, columns = full.shape[1], pl.ds(0, full.shape[2])
        for hop in range(groups):
            n = (me + hop) % groups
            pltpu.make_async_copy(full.at[n] if hop else own.at[:, columns], shard(into, base, size, n, columns), sem).start()
        whole = into.at[pl.ds(base, groups * size), columns]
        return pltpu.make_async_copy(whole, whole, sem)

    o_load = pltpu.make_async_copy(oin_ref, ov, load.at[2])
    res_load = pltpu.make_async_copy(res_ref, res, load.at[3])
    rest = pl.ds(cut, model - cut)
    rest_own = pltpu.make_async_copy(w2_own.at[:, rest], shard(w2, 0, width // groups, me, rest), load.at[7])
    x_load(0).start()
    w1_load = gathered(w1_own, w1_ref, w1, 0, load.at[4])
    o_load.start()
    w2_load = gathered(w2_own, w2_ref, w2, 0, load.at[5])
    wo_load = gathered(wo_own, wo_ref, w2, width, load.at[6])
    rest_own.start()
    x_load(1).start()
    res_load.start()
    meet(right, left, {"y": (y + 1) % side}, {"y": (y + side - 1) % side}, {"core": (lax.axis_index("core") + 1) % cores})
    w2_rest = ring(w2_own.at[:, rest], lambda n: shard(w2, 0, width // groups, n, rest), "y", width // groups // 2, w2_send, w2_recv)
    start(w2_rest, 0, 1, 2)

    def hidden(n):
        x_load(n).wait()

        def flip(k, c):
            at = pl.ds(pl.multiple_of(k * 256, 256), 256)
            xt[at, :] = xv[n % 2, :, at].T
            return c

        lax.fori_loop(0, model // 256, flip, 0, unroll=2)
        if n < 2:
            x_load(n + 2).start()
        col = pl.multiple_of((x + order[n]) % side * rows, rows)
        if n == 0:
            o_load.wait()
        hv[n, :, width:] = ov[:, :, pl.ds(col, rows)].reshape(heads, rows).T
        if n == 0:
            w1_load.wait()

        def piece(f, c):
            at = pl.ds(pl.multiple_of(f * 512, 512), 512)
            pre = jnp.dot(w1[at, :], xt[...], preferred_element_type=F32)
            hv[n, :, at] = jax.nn.gelu(pre, approximate=True).astype(BF).T
            return c

        lax.fori_loop(0, width // 512, piece, 0)

    def outs(n, lo, hi):
        def piece(d, c):
            at = pl.ds(pl.multiple_of(d * step, step), step)
            part[n % 3, :, at] = jnp.dot(hv[n], w2[:, at], preferred_element_type=F32)
            return c

        lax.fori_loop(lo // step, hi // step, piece, 0)

    def phase(lo, hi, first, prepare, between):
        cols = pl.ds(lo, hi - lo)
        plan = (
            (part.at[0, top, cols], far.at[0, :, cols], right),
            (part.at[0, low, cols], far.at[1, :, cols], left),
            (part.at[1, low, cols], near.at[0, low, cols], right),
            (part.at[2, top, cols], near.at[1, top, cols], left),
            (part.at[1, top, cols], near.at[0, top, cols], right),
            (part.at[2, low, cols], near.at[1, low, cols], left),
        )
        puts = [
            pltpu.make_async_remote_copy(src_ref=src, dst_ref=dst, send_sem=send.at[first + n], recv_sem=recv.at[first + n],
                                         device_id=to, device_id_type=MESH)
            for n, (src, dst, to) in enumerate(plan)
        ]
        prepare(0)
        outs(0, lo, hi)
        start(puts, 0, 1)
        prepare(1)
        outs(1, lo, hi)
        start(puts, 2)
        prepare(2)
        outs(2, lo, hi)
        start(puts, 3)
        between()
        puts[0].wait()
        part[1, :half, lo:hi] += far[0, :, lo:hi]
        start(puts, 4)
        puts[1].wait()
        part[2, half:, lo:hi] += far[1, :, lo:hi]
        start(puts, 5)
        prepare(3)
        outs(3, lo, hi)
        return puts[2:]

    def ready(n):
        hidden(n)
        if n == 0:
            w2_load.wait()
            wo_load.wait()

    def pass_on():
        arrived(w2_rest, 0, 1)
        start(w2_rest, 3, 4, 5, 6)

    waits = phase(0, cut, 0, ready, pass_on)
    arrived(w2_rest, 3, 4)
    start(w2_rest, 7)
    rest_own.wait()
    arrived(w2_rest, 2, 5, 6, 7)
    waits += phase(cut, model, 6, lambda n: None, lambda: None)
    res_load.wait()
    part[0] += res[...].astype(F32)
    for put in waits:
        put.wait()
    for copy in w2_rest:
        copy.wait_send()
    y_ref[...] = (part[0] + near[0] + near[1]).astype(BF)


def mlp(x_loc, normed, wide, oin, own, full, cores, side):
    rows, model = normed.shape
    groups = side * cores
    width, heads = groups * own[0].shape[0], groups * own[2].shape[0]
    anywhere = pl.BlockSpec(memory_space=pl.ANY)
    flops = 2 * side * rows * model * (2 * width + heads)
    return pl.pallas_call(
        functools.partial(mlp_kernel, side, cores),
        in_specs=[anywhere] * 10,
        out_specs=pl.BlockSpec(memory_space=pltpu.VMEM),
        out_shape=jax.ShapeDtypeStruct((rows, model), BF),
        scratch_shapes=[
            pltpu.VMEM((width, model), BF),
            pltpu.VMEM((width + heads, model), BF),
            pltpu.VMEM((2, rows, model), BF),
            pltpu.VMEM((model, rows), BF),
            pltpu.VMEM(oin.shape, BF),
            pltpu.VMEM((side, rows, width + heads), BF),
            pltpu.VMEM((3, rows, model), F32),
            pltpu.VMEM((2, rows // 2, model), F32),
            pltpu.VMEM((2, rows, model), F32),
            pltpu.VMEM((rows, model), BF),
            pltpu.SemaphoreType.DMA((8,)),
            pltpu.SemaphoreType.DMA((12,)),
            pltpu.SemaphoreType.DMA((12,)),
            pltpu.SemaphoreType.DMA((8,)),
            pltpu.SemaphoreType.DMA((8,)),
        ],
        compiler_params=pltpu.CompilerParams(vmem_limit_bytes=67043328, collective_id=2, has_side_effects=True),
        cost_estimate=pl.CostEstimate(flops=flops, bytes_accessed=4 * model * width, transcendentals=side * rows * width),
        name="mlp",
    )(normed, wide, oin, *own, *full, x_loc)


def solution(mesh):
    data, tp = mesh.devices.shape
    side = math.isqrt(tp // 2)
    cores = tp // (side * side)
    grid = Mesh(mesh.devices.reshape(data, side, side, cores), ("data", "y", "x", "core"))

    def local_block(x_loc, ln_gamma, w_qkv, w_out, w_up, w_down):
        own = (w_up.T, w_down, w_out[0])
        qkv, normed, w1 = qkv_stage(x_loc, ln_gamma[None], w_qkv[:, 0, :].T, own[0], cores, side)
        oin, wide, w2, wo = attention(qkv, normed, own[1], own[2], cores, side)
        return mlp(x_loc, normed, wide, oin, own, (w1, w2, wo), cores, side)

    row_spec = P(("data", "y", "x", "core"), None)
    tp_axes = ("y", "x", "core")
    return jax.shard_map(
        local_block,
        mesh=grid,
        in_specs=(row_spec, P(None), P(None, tp_axes, None), P(tp_axes, None, None), P(None, tp_axes), P(tp_axes, None)),
        out_specs=row_spec,
        check_vma=False,
    )
```

```python
import functools
import math
import jax
import jax.numpy as jnp
from jax import lax
from jax.experimental import pallas as pl
from jax.experimental.pallas import tpu as pltpu
from jax.sharding import Mesh, PartitionSpec as P

LN_EPS = 1e-6
BF = jnp.bfloat16
MESH = pl.DeviceIdType.MESH
F32 = jnp.float32
TK = 256
TRIP = 16
ROWS = 64


def ring(own, slot, axis, split, send, recv):
    side, cores = lax.axis_size(axis), lax.axis_size("core")
    at, core = lax.axis_index(axis), lax.axis_index("core")
    other = (core + 1) % cores
    block = lambda hop: slot((at + hop) % side * cores + core)
    head, tail = pl.ds(0, split), pl.ds(split, own.shape[0] - split)
    nxt, prv, sib = {axis: (at + 1) % side}, {axis: (at + side - 1) % side}, {"core": other}
    plan = (
        (own, block(0), nxt),
        (own, block(0), prv),
        (own, block(0), sib),
        (block(side - 1).at[head], block(side - 1).at[head], nxt),
        (block(1).at[tail], block(1).at[tail], prv),
        (block(side - 1), block(side - 1), sib),
        (block(1), block(1), sib),
        (block(2), block(2), sib),
    )
    return [
        pltpu.make_async_remote_copy(
            src_ref=src, dst_ref=dst, send_sem=send.at[n], recv_sem=recv.at[n], device_id=to, device_id_type=MESH)
        for n, (src, dst, to) in enumerate(plan)
    ]


def start(copies, *which):
    for n in which:
        copies[n].start()


def arrived(copies, *which):
    for n in which:
        copies[n].wait_recv()


def meet(*places):
    barrier = pltpu.get_barrier_semaphore()
    for place in places:
        pl.semaphore_signal(barrier, inc=1, device_id=place, device_id_type=MESH)
    pl.semaphore_wait(barrier, len(places))


def qkv_kernel(side, cores, x_ref, gain_ref, wq_ref, w1_ref, qkv_ref, normed_ref, w1_full, wv, xv, xt, qk,
               wq_send, wq_recv, x_send, x_recv, w1_send, w1_recv, a_send, a_recv, local):
    y, x, core = lax.axis_index("y"), lax.axis_index("x"), lax.axis_index("core")
    rows, model = x_ref.shape
    low = rows // 2
    me = x * cores + core
    up, down = {"y": (y + 1) % side}, {"y": (y + side - 1) % side}
    meet(up, down, *[
        {"x": (x + dx) % side, "core": (core + dc) % cores} for dx in range(side) for dc in range(cores) if dx or dc])

    wq = ring(wq_ref, lambda n: wv.at[n], "x", wq_ref.shape[0] // 32 * 16, wq_send, wq_recv)
    w1 = ring(w1_ref, lambda n: w1_full.at[n], "y", w1_ref.shape[0] // 2, w1_send, w1_recv)
    own_wq = pltpu.make_async_copy(wq_ref, wv.at[me], local.at[0])
    own_wq.start()
    start(wq, 0, 1, 2)

    def x_copy(n, src, to):
        return pltpu.make_async_remote_copy(
            src_ref=src, dst_ref=src, send_sem=x_send.at[n], recv_sem=x_recv.at[n], device_id=to, device_id_type=MESH)

    before, after, far = (y + side - 1) % side, (y + 1) % side, (y + 2) % side
    xs = [
        x_copy(0, xv.at[y], up),
        x_copy(1, xv.at[y], down),
        x_copy(2, xv.at[before, pl.ds(0, low)], up),
        x_copy(3, xv.at[after, pl.ds(low, low)], down),
    ]

    def norm(r, c):
        at = pl.ds(pl.multiple_of(r * 32, 32), 32)
        row = x_ref[at, :].astype(F32)
        mean = jnp.mean(row, axis=-1, keepdims=True)
        centered = row - mean
        var = jnp.mean(centered * centered, axis=-1, keepdims=True)
        xv[y, at, :] = (centered * lax.rsqrt(var + LN_EPS) * gain_ref[...].reshape(1, model)).astype(BF)
        return c

    lax.fori_loop(0, rows // 32, norm, 0)

    def cols(part):
        return pl.ds(pl.multiple_of(part * rows, rows), rows)

    def flip(part):
        def piece(k, c):
            at = pl.ds(pl.multiple_of(k * 256, 256), 256)
            xt[at, cols(part)] = xv[part, :, at].T
            return c

        lax.fori_loop(0, model // 256, piece, 0, unroll=2)

    flip(y)
    start(xs, 0, 1)
    start(w1, 2)
    keep = pltpu.make_async_copy(xv.at[y], normed_ref, local.at[1])
    keep.start()

    def unit(head, part):
        qk[head, :, cols(part)] = jnp.dot(wv[head], xt[:, cols(part)], preferred_element_type=F32).astype(BF)

    def send(n, head):
        return pltpu.make_async_remote_copy(
            src_ref=qk.at[head], dst_ref=qkv_ref.at[me], send_sem=a_send.at[n], recv_sem=a_recv.at[n],
            device_id={"x": head // cores, "core": head % cores}, device_id_type=MESH)

    def head_of(n):
        return (x + n // cores) % side * cores + (core + n) % cores

    arrived(wq, 0, 1)
    start(wq, 3, 4, 5, 6)
    arrived(xs, 0, 1)
    start(xs, 2, 3)
    start(w1, 0, 1)
    flip(before)
    flip(after)
    own_wq.wait()
    arrived(wq, 2, 5, 6)

    def near(k, c):
        n, p = k // 3, k % 3
        n = n + cores * (n // (2 * cores))
        unit(head_of(n), (y + p + p // 2) % side)
        return c

    lax.fori_loop(0, 3 * 3 * cores, near, 0)
    arrived(wq, 3, 4)
    start(wq, 7)
    arrived(xs, 2, 3)
    flip(far)

    def close(k, c):
        n = cores * (1 + 2 * (k // cores)) + k % cores
        unit(head_of(n), far)
        send(n, head_of(n)).start()
        return c

    lax.fori_loop(0, 2 * cores, close, 0)
    arrived(wq, 7)

    def distant(k, c):
        unit(head_of(2 * cores + k // side), k % side)
        return c

    for k in range(cores):
        lax.fori_loop(k * side, (k + 1) * side, distant, 0)
        send(2 * cores + k, head_of(2 * cores + k)).start()

    def home(k, c):
        unit(head_of(k), far)
        return c

    lax.fori_loop(0, cores, home, 0)
    for n in range(1, cores):
        send(n, head_of(n)).start()
    own = pltpu.make_async_copy(qk.at[me], qkv_ref.at[me], local.at[2])
    own.start()
    for n in range(1, side * cores):
        send(n, head_of(n)).wait()
    own.wait()
    keep.wait()
    arrived(w1, 0, 1, 2)
    for copies in (wq, w1[:3], xs):
        for copy in copies:
            copy.wait_send()


def qkv_stage(x_loc, gain, wq, w1, cores, side):
    rows, model = x_loc.shape
    groups = side * cores
    anywhere = pl.BlockSpec(memory_space=pl.ANY)
    vmem = pl.BlockSpec(memory_space=pltpu.VMEM)
    dma = lambda n: pltpu.SemaphoreType.DMA((n,))
    return pl.pallas_call(
        functools.partial(qkv_kernel, side, cores),
        in_specs=[vmem, vmem, anywhere, anywhere],
        out_specs=[anywhere] * 3,
        out_shape=[
            jax.ShapeDtypeStruct((groups, wq.shape[0], side * rows), BF),
            jax.ShapeDtypeStruct((rows, model), BF),
            jax.ShapeDtypeStruct((groups,) + w1.shape, BF),
        ],
        scratch_shapes=[
            pltpu.VMEM((groups,) + wq.shape, BF),
            pltpu.VMEM((side, rows, model), BF),
            pltpu.VMEM((model, side * rows), BF),
            pltpu.VMEM((groups, wq.shape[0], side * rows), BF),
            dma(8), dma(8), dma(4), dma(4), dma(8), dma(8), dma(groups), dma(groups), dma(3),
        ],
        compiler_params=pltpu.CompilerParams(vmem_limit_bytes=58 * 1024 * 1024, collective_id=0, has_side_effects=True),
        cost_estimate=pl.CostEstimate(flops=2 * side * rows * model * groups * wq.shape[0], bytes_accessed=4 * w1.size, transcendentals=0),
        name="qkv",
    )(x_loc, gain, wq, w1)


def attn_kernel(hd, side, cores, sub, qkv_ref, x_ref, w1_own, w2_ref, wo_ref, w1_part, oin_ref, wide_ref, w2_full, wo_full, w1_full, kaug_ref, qaug_ref, sa_ref,
                sb_ref, acc_ref, m_ref, o_buf, o_send, o_recv, x_send, x_recv, w2_send, w2_recv, wo_send, wo_recv, w1_send, w1_recv):
    groups, _, toks = qkv_ref.shape
    keys = groups * toks
    bq = sa_ref.shape[1]
    subs = bq // sub
    i = pl.program_id(0)
    scale = hd ** -0.5 * math.log2(math.e)
    pad = kaug_ref.shape[1] - 3 * hd
    chunk = TRIP * TK
    y, core, x = lax.axis_index("y"), lax.axis_index("core"), lax.axis_index("x")
    me = y * cores + core
    right, left = (x + 1) % side, (x + side - 1) % side
    rows = x_ref.shape[0]
    top, low = pl.ds(0, rows // 2), pl.ds(rows // 2, rows // 2)

    def x_copy(n):
        src = (x_ref, x_ref, wide_ref.at[3, top], wide_ref.at[1, low])[n]
        dst = (wide_ref.at[3], wide_ref.at[1], wide_ref.at[2, top], wide_ref.at[2, low])[n]
        return pltpu.make_async_remote_copy(
            src_ref=src, dst_ref=dst, send_sem=x_send.at[n], recv_sem=x_recv.at[n],
            device_id={"x": left if n % 2 else right}, device_id_type=MESH)

    def o_copy(step):
        to = (me + 1 + step) % groups
        return pltpu.make_async_remote_copy(
            src_ref=o_buf.at[step % 2], dst_ref=oin_ref.at[me], send_sem=o_send.at[step % 2], recv_sem=o_recv.at[step],
            device_id={"y": to // cores, "core": to % cores}, device_id_type=MESH)

    w2 = ring(w2_ref.at[:, pl.ds(0, w2_full.shape[2])], lambda n: w2_full.at[n], "y", w2_ref.shape[0] // 2, w2_send, w2_recv)
    w1 = ring(w1_own, lambda n: w1_full.at[n], "y", w1_own.shape[0] // 2, w1_send, w1_recv)
    wo = ring(wo_ref, lambda n: wo_full.at[n], "y", wo_ref.shape[0] // 32 * 16, wo_send, wo_recv)

    def load_query(b, slot):
        b = jnp.minimum(b, 2 * groups - 1)
        dest, part = (me + 1 + b // 2) % groups, b % 2
        for j in range(subs):
            g = (part * subs + j) * cores + dest % cores
            at = pl.multiple_of((dest // cores) * sub, sub)
            qt = qkv_ref[g, 0:hd, pl.ds(at, sub)].astype(F32) * scale
            hi = qt.astype(BF)
            rest = qt - hi.astype(F32)
            mid = rest.astype(BF)
            cols = slice(j * sub, (j + 1) * sub)
            qaug_ref[slot, 0:hd, cols] = hi
            qaug_ref[slot, hd:2 * hd, cols] = mid
            qaug_ref[slot, 2 * hd:3 * hd, cols] = (rest - mid.astype(F32)).astype(BF)

    def fold(piece, op):
        return op(piece.reshape(piece.shape[0] // 8, 8, bq), axis=0)

    @pl.when(i == 0)
    def _():
        meet({"x": right}, {"x": left}, *[
            {"y": (me + hop) % groups // cores, "core": (me + hop) % cores} for hop in range(1, groups)])
        start(w1, 3, 4, 5, 6)
        start(wo, 0, 1, 2)
        start(w2, 0, 1, 2)
        x_copy(0).start()
        x_copy(1).start()
        zeros = jnp.zeros((pad, TK), BF)

        def spread(t, c):
            g = t * TK // toks
            t0 = pl.multiple_of(t * TK - g * toks, TK)
            kt = qkv_ref[g, hd:2 * hd, pl.ds(t0, TK)]
            kaug_ref[pl.ds(pl.multiple_of(t * TK, TK), TK), :] = jnp.concatenate([kt, kt, kt, zeros], axis=0).T
            return c

        lax.fori_loop(0, keys // TK, spread, 0, unroll=4)
        qaug_ref[:, 3 * hd:, :] = jnp.zeros((2, pad, bq), BF)
        load_query(0, 0)
        load_query(1, 1)

        def first(c, m8):
            at = pl.ds(pl.multiple_of(c * 4 * TK, 4 * TK), 4 * TK)
            s = jnp.dot(kaug_ref[at, :], qaug_ref[0], preferred_element_type=F32)
            sa_ref[at, :] = s
            return jnp.maximum(m8, fold(s, jnp.max))

        m8 = lax.fori_loop(0, keys // (4 * TK), first, jnp.full((8, bq), -jnp.inf, F32))
        m_ref[...] = jnp.broadcast_to(jnp.max(m8, axis=0, keepdims=True), (8, bq))

    @pl.when(i == groups // 2)
    def _():
        x_copy(0).wait()
        x_copy(1).wait()
        x_copy(2).start()
        x_copy(3).start()
        arrived(w1, 3, 4)
        start(w1, 7)

    @pl.when(i == groups // 2 + 1)
    def _():
        for copies in (wo, w2):
            arrived(copies, 0, 1)
            start(copies, 3, 4, 5, 6)

    @pl.when(i == groups - 1)
    def _():
        for copies in (wo, w2):
            arrived(copies, 3, 4)
            start(copies, 7)

    @pl.when(i >= 2)
    def _():
        o_copy(i - 2).wait_send()

    def half(s_in, s_out, slot, col):
        m = m_ref[0:1, :]
        acc_ref[...] = jnp.zeros_like(acc_ref)

        def trip(c, carry):
            m8, l8 = carry
            k0 = pl.multiple_of(c * chunk, chunk)
            total = None
            for u in range(TRIP):
                s_new = jnp.dot(kaug_ref[pl.ds(k0 + u * TK, TK), :], qaug_ref[slot], preferred_element_type=F32)
                ps = []
                for r in range(0, TK, ROWS):
                    p = jnp.exp2(s_in[pl.ds(k0 + u * TK + r, ROWS), :] - m)
                    l8 = l8 + fold(p, jnp.sum)
                    ps.append(p.astype(BF))
                at = u * TK % toks
                vt = qkv_ref[k0 // toks + u * TK // toks, 2 * hd:3 * hd, at:at + TK]
                d = jnp.dot(vt, jnp.concatenate(ps, axis=0), preferred_element_type=F32)
                total = d if total is None else total + d
                for r in range(0, TK, ROWS):
                    piece = s_new[r:r + ROWS]
                    m8 = jnp.maximum(m8, fold(piece, jnp.max))
                    s_out[pl.ds(k0 + u * TK + r, ROWS), :] = piece
            acc_ref[...] += total
            return m8, l8

        m8, l8 = lax.fori_loop(0, keys // chunk, trip, (jnp.full((8, bq), -jnp.inf, F32), jnp.zeros((8, bq), F32)))
        o_buf[i % 2, :, col:col + bq] = (acc_ref[...] / jnp.sum(l8, axis=0, keepdims=True)).astype(BF)
        m_ref[...] = jnp.broadcast_to(jnp.max(m8, axis=0, keepdims=True), (8, bq))

    half(sa_ref, sb_ref, 1, 0)
    load_query(2 * i + 2, 0)
    half(sb_ref, sa_ref, 0, bq)
    load_query(2 * i + 3, 1)

    @pl.when(i < groups - 1)
    def _():
        o_copy(i).start()

    @pl.when(i == groups - 1)
    def _():
        own = pltpu.make_async_copy(o_buf.at[i % 2], oin_ref.at[me], o_send.at[i % 2])
        own.start()
        x_copy(2).wait()
        x_copy(3).wait()
        for step in range(groups - 1):
            o_copy(step).wait_recv()
        o_copy(groups - 2).wait_send()
        own.wait()
        for copies in (wo, w2):
            arrived(copies, 2, 5, 6, 7)
            for copy in copies:
                copy.wait_send()
        arrived(w1, 5, 6, 7)
        for copy in w1[3:]:
            copy.wait_send()


def first_columns(model):
    return model * 2 // 5 // 256 * 256


def attention(qkv, normed, own, w1, cores, side):
    groups, three, toks = qkv.shape
    w1_own, w2, wo = own
    hd = three // 3
    keys = groups * toks
    bq = toks // 2
    anywhere = pl.BlockSpec(memory_space=pl.ANY)
    return pl.pallas_call(
        functools.partial(attn_kernel, hd, side, cores, toks // side),
        grid=(groups,),
        in_specs=[pl.BlockSpec((groups, three, toks), lambda i: (0, 0, 0))] + [anywhere] * 5,
        out_specs=[anywhere] * 5,
        input_output_aliases={5: 4},
        out_shape=[
            jax.ShapeDtypeStruct((groups, hd, toks), BF),
            jax.ShapeDtypeStruct((side,) + normed.shape, BF),
            jax.ShapeDtypeStruct((groups, w2.shape[0], first_columns(w2.shape[1])), BF),
            jax.ShapeDtypeStruct((groups,) + wo.shape, BF),
            jax.ShapeDtypeStruct(w1.shape, BF),
        ],
        scratch_shapes=[
            pltpu.VMEM((keys, 256), BF),
            pltpu.VMEM((2, 256, bq), BF),
            pltpu.VMEM((keys, bq), F32),
            pltpu.VMEM((keys, bq), F32),
            pltpu.VMEM((hd, bq), F32),
            pltpu.VMEM((8, bq), F32),
            pltpu.VMEM((2, hd, toks), BF),
            pltpu.SemaphoreType.DMA((2,)),
            pltpu.SemaphoreType.DMA((groups - 1,)),
            pltpu.SemaphoreType.DMA((4,)),
            pltpu.SemaphoreType.DMA((4,)),
            pltpu.SemaphoreType.DMA((8,)),
            pltpu.SemaphoreType.DMA((8,)),
            pltpu.SemaphoreType.DMA((8,)),
            pltpu.SemaphoreType.DMA((8,)),
            pltpu.SemaphoreType.DMA((8,)),
            pltpu.SemaphoreType.DMA((8,)),
        ],
        compiler_params=pltpu.CompilerParams(
            vmem_limit_bytes=58 * 1024 * 1024, collective_id=1, has_side_effects=True),
        cost_estimate=pl.CostEstimate(flops=6 * keys * keys * hd, bytes_accessed=8 * keys * hd, transcendentals=keys * keys),
        name="attention",
    )(qkv, normed, w1_own, w2, wo, w1)


def mlp_kernel(side, cores, x_ref, wide_ref, oin_ref, w1_own, w2_own, wo_own, w1_ref, w2_ref, wo_ref, res_ref, y_ref, w1, w2, xv, xt, ov,
               hv, part, far, near, res, load, w1_sem, send, recv, w2_send, w2_recv):
    x, y = lax.axis_index("x"), lax.axis_index("y")
    right, left = {"x": (x + 1) % side}, {"x": (x + side - 1) % side}
    rows, model = x_ref.shape
    groups = w1_ref.shape[0]
    width = groups * w1_own.shape[0]
    heads = groups * wo_own.shape[0]
    cut = w2_ref.shape[2]
    step = math.gcd(cut, model - cut, 512)
    half = rows // 2
    me = y * cores + lax.axis_index("core")
    top, low = pl.ds(0, half), pl.ds(half, half)
    order = (2, 1, 3, 0)

    def x_load(n):
        src = x_ref if order[n] == 0 else wide_ref.at[order[n]]
        return pltpu.make_async_copy(src, xv.at[n % 2], load.at[n % 2])

    def shard(into, base, size, n, columns):
        return into.at[pl.ds(pl.multiple_of(base + n * size, 16), size), columns]

    def gathered(own, full, into, base, sem):
        size, columns = full.shape[1], pl.ds(0, full.shape[2])
        for hop in range(groups):
            n = (me + hop) % groups
            pltpu.make_async_copy(full.at[n] if hop else own.at[:, columns], shard(into, base, size, n, columns), sem).start()
        whole = into.at[pl.ds(base, groups * size), columns]
        return pltpu.make_async_copy(whole, whole, sem)

    o_load = pltpu.make_async_copy(oin_ref, ov, load.at[2])
    res_load = pltpu.make_async_copy(res_ref, res, load.at[3])
    rest = pl.ds(cut, model - cut)
    rest_own = pltpu.make_async_copy(w2_own.at[:, rest], shard(w2, 0, width // groups, me, rest), load.at[7])
    x_load(0).start()
    pair = 2 * w1_own.shape[0]

    def w1_shard(n):
        to = shard(w1, 0, pair // 2, n, pl.ds(0, model))

        @pl.when(n == me)
        def _():
            pltpu.make_async_copy(w1_own, to, w1_sem.at[n // 2]).start()

        @pl.when(n != me)
        def _():
            pltpu.make_async_copy(w1_ref.at[n], to, w1_sem.at[n // 2]).start()

    for n in range(groups):
        w1_shard(n)
    o_load.start()
    w2_load = gathered(w2_own, w2_ref, w2, 0, load.at[5])
    wo_load = gathered(wo_own, wo_ref, w2, width, load.at[6])
    rest_own.start()
    x_load(1).start()
    res_load.start()
    meet(right, left, {"y": (y + 1) % side}, {"y": (y + side - 1) % side}, {"core": (lax.axis_index("core") + 1) % cores})
    w2_rest = ring(w2_own.at[:, rest], lambda n: shard(w2, 0, width // groups, n, rest), "y", width // groups // 2, w2_send, w2_recv)
    start(w2_rest, 0, 1, 2)

    def hidden(n):
        x_load(n).wait()

        def flip(k, c):
            at = pl.ds(pl.multiple_of(k * 256, 256), 256)
            xt[at, :] = xv[n % 2, :, at].T
            return c

        lax.fori_loop(0, model // 256, flip, 0, unroll=2)
        if n < 2:
            x_load(n + 2).start()
        col = pl.multiple_of((x + order[n]) % side * rows, rows)
        if n == 0:
            o_load.wait()
        hv[n, :, width:] = ov[:, :, pl.ds(col, rows)].reshape(heads, rows).T

        def piece(f, c):
            at = pl.ds(pl.multiple_of(f * pair, pair), pair)
            if n == 0:
                pltpu.make_async_copy(w1.at[at], w1.at[at], w1_sem.at[f]).wait()
            pre = jnp.dot(w1[at, :], xt[...], preferred_element_type=F32)
            hv[n, :, at] = jax.nn.gelu(pre, approximate=True).astype(BF).T
            return c

        lax.fori_loop(0, groups // 2, piece, 0)

    def outs(n, lo, hi):
        def piece(d, c):
            at = pl.ds(pl.multiple_of(d * step, step), step)
            part[n % 3, :, at] = jnp.dot(hv[n], w2[:, at], preferred_element_type=F32)
            return c

        lax.fori_loop(lo // step, hi // step, piece, 0)

    def phase(lo, hi, first, prepare, between):
        cols = pl.ds(lo, hi - lo)
        plan = (
            (part.at[0, top, cols], far.at[0, :, cols], right),
            (part.at[0, low, cols], far.at[1, :, cols], left),
            (part.at[1, low, cols], near.at[0, low, cols], right),
            (part.at[2, top, cols], near.at[1, top, cols], left),
            (part.at[1, top, cols], near.at[0, top, cols], right),
            (part.at[2, low, cols], near.at[1, low, cols], left),
        )
        puts = [
            pltpu.make_async_remote_copy(src_ref=src, dst_ref=dst, send_sem=send.at[first + n], recv_sem=recv.at[first + n],
                                         device_id=to, device_id_type=MESH)
            for n, (src, dst, to) in enumerate(plan)
        ]
        prepare(0)
        outs(0, lo, hi)
        start(puts, 0, 1)
        prepare(1)
        outs(1, lo, hi)
        start(puts, 2)
        prepare(2)
        outs(2, lo, hi)
        start(puts, 3)
        between()
        puts[0].wait()
        part[1, :half, lo:hi] += far[0, :, lo:hi]
        start(puts, 4)
        puts[1].wait()
        part[2, half:, lo:hi] += far[1, :, lo:hi]
        start(puts, 5)
        prepare(3)
        outs(3, lo, hi)
        return puts[2:]

    def ready(n):
        hidden(n)
        if n == 0:
            w2_load.wait()
            wo_load.wait()

    def pass_on():
        arrived(w2_rest, 0, 1)
        start(w2_rest, 3, 4, 5, 6)

    waits = phase(0, cut, 0, ready, pass_on)
    arrived(w2_rest, 3, 4)
    start(w2_rest, 7)
    rest_own.wait()
    arrived(w2_rest, 2, 5, 6, 7)
    waits += phase(cut, model, 6, lambda n: None, lambda: None)
    res_load.wait()
    part[0] += res[...].astype(F32)
    for put in waits:
        put.wait()
    for copy in w2_rest:
        copy.wait_send()
    y_ref[...] = (part[0] + near[0] + near[1]).astype(BF)


def mlp(x_loc, normed, wide, oin, own, full, cores, side):
    rows, model = normed.shape
    groups = side * cores
    width, heads = groups * own[0].shape[0], groups * own[2].shape[0]
    anywhere = pl.BlockSpec(memory_space=pl.ANY)
    flops = 2 * side * rows * model * (2 * width + heads)
    return pl.pallas_call(
        functools.partial(mlp_kernel, side, cores),
        in_specs=[anywhere] * 10,
        out_specs=pl.BlockSpec(memory_space=pltpu.VMEM),
        out_shape=jax.ShapeDtypeStruct((rows, model), BF),
        scratch_shapes=[
            pltpu.VMEM((width, model), BF),
            pltpu.VMEM((width + heads, model), BF),
            pltpu.VMEM((2, rows, model), BF),
            pltpu.VMEM((model, rows), BF),
            pltpu.VMEM(oin.shape, BF),
            pltpu.VMEM((side, rows, width + heads), BF),
            pltpu.VMEM((3, rows, model), F32),
            pltpu.VMEM((2, rows // 2, model), F32),
            pltpu.VMEM((2, rows, model), F32),
            pltpu.VMEM((rows, model), BF),
            pltpu.SemaphoreType.DMA((8,)),
            pltpu.SemaphoreType.DMA((groups // 2,)),
            pltpu.SemaphoreType.DMA((12,)),
            pltpu.SemaphoreType.DMA((12,)),
            pltpu.SemaphoreType.DMA((8,)),
            pltpu.SemaphoreType.DMA((8,)),
        ],
        compiler_params=pltpu.CompilerParams(vmem_limit_bytes=67043328, collective_id=2, has_side_effects=True),
        cost_estimate=pl.CostEstimate(flops=flops, bytes_accessed=4 * model * width, transcendentals=side * rows * width),
        name="mlp",
    )(normed, wide, oin, *own, *full, x_loc)


def solution(mesh):
    data, tp = mesh.devices.shape
    side = math.isqrt(tp // 2)
    cores = tp // (side * side)
    grid = Mesh(mesh.devices.reshape(data, side, side, cores), ("data", "y", "x", "core"))

    def local_block(x_loc, ln_gamma, w_qkv, w_out, w_up, w_down):
        own = (w_up.T, w_down, w_out[0])
        qkv, normed, w1 = qkv_stage(x_loc, ln_gamma, w_qkv[:, 0, :].T, own[0], cores, side)
        oin, wide, w2, wo, w1 = attention(qkv, normed, own, w1, cores, side)
        return mlp(x_loc, normed, wide, oin, own, (w1, w2, wo), cores, side)

    row_spec = P(("data", "y", "x", "core"), None)
    tp_axes = ("y", "x", "core")
    return jax.shard_map(
        local_block,
        mesh=grid,
        in_specs=(row_spec, P(None), P(None, tp_axes, None), P(tp_axes, None, None), P(None, tp_axes), P(tp_axes, None)),
        out_specs=row_spec,
        check_vma=False,
    )
```

```python
import functools
import math
import jax
import jax.numpy as jnp
from jax import lax
from jax.experimental import pallas as pl
from jax.experimental.pallas import tpu as pltpu
from jax.sharding import Mesh, PartitionSpec as P

LN_EPS = 1e-6
BF = jnp.bfloat16
MESH = pl.DeviceIdType.MESH
F32 = jnp.float32
TK = 256
TRIP = 16
ROWS = 64


def ring(own, slot, axis, split, send, recv):
    side, cores = lax.axis_size(axis), lax.axis_size("core")
    at, core = lax.axis_index(axis), lax.axis_index("core")
    other = (core + 1) % cores
    block = lambda hop: slot((at + hop) % side * cores + core)
    head, tail = pl.ds(0, split), pl.ds(split, own.shape[0] - split)
    nxt, prv, sib = {axis: (at + 1) % side}, {axis: (at + side - 1) % side}, {"core": other}
    plan = (
        (own, block(0), nxt),
        (own, block(0), prv),
        (own, block(0), sib),
        (block(side - 1).at[head], block(side - 1).at[head], nxt),
        (block(1).at[tail], block(1).at[tail], prv),
        (block(side - 1), block(side - 1), sib),
        (block(1), block(1), sib),
        (block(2), block(2), sib),
    )
    return [
        pltpu.make_async_remote_copy(
            src_ref=src, dst_ref=dst, send_sem=send.at[n], recv_sem=recv.at[n], device_id=to, device_id_type=MESH)
        for n, (src, dst, to) in enumerate(plan)
    ]


def start(copies, *which):
    for n in which:
        copies[n].start()


def arrived(copies, *which):
    for n in which:
        copies[n].wait_recv()


def hail(*places):
    barrier = pltpu.get_barrier_semaphore()
    for place in places:
        pl.semaphore_signal(barrier, inc=1, device_id=place, device_id_type=MESH)
    return lambda: pl.semaphore_wait(barrier, len(places))


def qkv_kernel(side, cores, x_ref, gain_ref, wq_ref, w1_ref, qkv_ref, normed_ref, w1_full, wv, xv, xt, qk,
               wq_send, wq_recv, x_send, x_recv, w1_send, w1_recv, a_send, a_recv, local):
    y, x, core = lax.axis_index("y"), lax.axis_index("x"), lax.axis_index("core")
    rows, model = x_ref.shape
    low = rows // 2
    me = x * cores + core
    up, down = {"y": (y + 1) % side}, {"y": (y + side - 1) % side}
    met = hail(up, down, *[
        {"x": (x + dx) % side, "core": (core + dc) % cores} for dx in range(side) for dc in range(cores) if dx or dc])

    wq = ring(wq_ref, lambda n: wv.at[n], "x", wq_ref.shape[0] // 32 * 16, wq_send, wq_recv)
    w1 = ring(w1_ref, lambda n: w1_full.at[n], "y", w1_ref.shape[0] // 2, w1_send, w1_recv)
    own_wq = pltpu.make_async_copy(wq_ref, wv.at[me], local.at[0])
    own_wq.start()

    def x_copy(n, src, to):
        return pltpu.make_async_remote_copy(
            src_ref=src, dst_ref=src, send_sem=x_send.at[n], recv_sem=x_recv.at[n], device_id=to, device_id_type=MESH)

    before, after, far = (y + side - 1) % side, (y + 1) % side, (y + 2) % side
    xs = [
        x_copy(0, xv.at[y], up),
        x_copy(1, xv.at[y], down),
        x_copy(2, xv.at[before, pl.ds(0, low)], up),
        x_copy(3, xv.at[after, pl.ds(low, low)], down),
    ]

    def norm(r, c):
        at = pl.ds(pl.multiple_of(r * 32, 32), 32)
        row = x_ref[at, :].astype(F32)
        mean = jnp.mean(row, axis=-1, keepdims=True)
        centered = row - mean
        var = jnp.mean(centered * centered, axis=-1, keepdims=True)
        xv[y, at, :] = (centered * lax.rsqrt(var + LN_EPS) * gain_ref[...].reshape(1, model)).astype(BF)
        return c

    lax.fori_loop(0, rows // 32, norm, 0)

    def cols(part):
        return pl.ds(pl.multiple_of(part * rows, rows), rows)

    def flip(part):
        def piece(k, c):
            at = pl.ds(pl.multiple_of(k * 256, 256), 256)
            xt[at, cols(part)] = xv[part, :, at].T
            return c

        lax.fori_loop(0, model // 256, piece, 0, unroll=2)

    flip(y)
    met()
    start(wq, 0, 1, 2)
    start(xs, 0, 1)
    start(w1, 2)
    keep = pltpu.make_async_copy(xv.at[y], normed_ref, local.at[1])
    keep.start()

    def unit(head, part):
        qk[head, :, cols(part)] = jnp.dot(wv[head], xt[:, cols(part)], preferred_element_type=F32).astype(BF)

    def send(n, head, *at):
        return pltpu.make_async_remote_copy(
            src_ref=qk.at[head, *at], dst_ref=qkv_ref.at[me, *at], send_sem=a_send.at[n], recv_sem=a_recv.at[n],
            device_id={"x": head // cores, "core": head % cores}, device_id_type=MESH)

    def head_of(n):
        return (x + n // cores) % side * cores + (core + n) % cores

    close = lambda k: cores * (1 + 2 * (k // cores)) + k % cores
    distant = lambda k: 2 * cores + k

    def work(count, pick, parts, go=True):
        def body(k, c):
            n = pick(k)
            for part in parts:
                unit(head_of(n), part)
            if go:
                for part in parts:
                    send(n, head_of(n), slice(None), cols(part)).start()
            return c

        lax.fori_loop(0, count, body, 0)

    arrived(wq, 0, 1)
    start(wq, 3, 4, 5, 6)
    arrived(xs, 0, 1)
    start(xs, 2, 3)
    start(w1, 0, 1)
    flip(before)
    flip(after)
    own_wq.wait()
    arrived(wq, 2, 5, 6)
    work(2 * cores, close, (y, after, before))
    arrived(wq, 3, 4)
    start(wq, 7)
    work(cores, lambda k: k, (y, after, before), go=False)
    arrived(wq, 7)
    work(cores, distant, (y, after, before))
    arrived(xs, 2, 3)
    flip(far)
    work(cores, distant, (far,))
    work(2 * cores, close, (far,))
    work(cores, lambda k: k, (far,), go=False)
    for n in range(1, cores):
        send(n, head_of(n)).start()
    own = pltpu.make_async_copy(qk.at[me], qkv_ref.at[me], local.at[2])
    own.start()
    for n in range(1, side * cores):
        send(n, head_of(n)).wait()
    own.wait()
    keep.wait()
    arrived(w1, 0, 1, 2)
    for copies in (wq, w1[:3], xs):
        for copy in copies:
            copy.wait_send()


def qkv_stage(x_loc, gain, wq, w1, cores, side):
    rows, model = x_loc.shape
    groups = side * cores
    anywhere = pl.BlockSpec(memory_space=pl.ANY)
    vmem = pl.BlockSpec(memory_space=pltpu.VMEM)
    dma = lambda n: pltpu.SemaphoreType.DMA((n,))
    return pl.pallas_call(
        functools.partial(qkv_kernel, side, cores),
        in_specs=[vmem, vmem, anywhere, anywhere],
        out_specs=[anywhere] * 3,
        out_shape=[
            jax.ShapeDtypeStruct((groups, wq.shape[0], side * rows), BF),
            jax.ShapeDtypeStruct((rows, model), BF),
            jax.ShapeDtypeStruct((groups,) + w1.shape, BF),
        ],
        scratch_shapes=[
            pltpu.VMEM((groups,) + wq.shape, BF),
            pltpu.VMEM((side, rows, model), BF),
            pltpu.VMEM((model, side * rows), BF),
            pltpu.VMEM((groups, wq.shape[0], side * rows), BF),
            dma(8), dma(8), dma(4), dma(4), dma(8), dma(8), dma(groups), dma(groups), dma(3),
        ],
        compiler_params=pltpu.CompilerParams(vmem_limit_bytes=58 * 1024 * 1024, collective_id=0, has_side_effects=True),
        cost_estimate=pl.CostEstimate(flops=2 * side * rows * model * groups * wq.shape[0], bytes_accessed=4 * w1.size, transcendentals=0),
        name="qkv",
    )(x_loc, gain, wq, w1)


def attn_kernel(hd, side, cores, sub, qkv_ref, x_ref, w1_own, w2_ref, wo_ref, w1_part, oin_ref, wide_ref, w2_full, wo_full, w1_full, kaug_ref, qaug_ref, sa_ref,
                sb_ref, acc_ref, m_ref, o_buf, o_send, o_recv, x_send, x_recv, w2_send, w2_recv, wo_send, wo_recv, w1_send, w1_recv):
    groups, _, toks = qkv_ref.shape
    keys = groups * toks
    bq = sa_ref.shape[1]
    subs = bq // sub
    i = pl.program_id(0)
    scale = hd ** -0.5 * math.log2(math.e)
    pad = kaug_ref.shape[1] - 3 * hd
    chunk = TRIP * TK
    y, core, x = lax.axis_index("y"), lax.axis_index("core"), lax.axis_index("x")
    me = y * cores + core
    right, left = (x + 1) % side, (x + side - 1) % side
    rows = x_ref.shape[0]
    top, low = pl.ds(0, rows // 2), pl.ds(rows // 2, rows // 2)

    def x_copy(n):
        src = (x_ref, x_ref, wide_ref.at[3, top], wide_ref.at[1, low])[n]
        dst = (wide_ref.at[3], wide_ref.at[1], wide_ref.at[2, top], wide_ref.at[2, low])[n]
        return pltpu.make_async_remote_copy(
            src_ref=src, dst_ref=dst, send_sem=x_send.at[n], recv_sem=x_recv.at[n],
            device_id={"x": left if n % 2 else right}, device_id_type=MESH)

    def o_copy(step):
        to = (me + 1 + step) % groups
        return pltpu.make_async_remote_copy(
            src_ref=o_buf.at[step], dst_ref=oin_ref.at[me], send_sem=o_send.at[step], recv_sem=o_recv.at[step],
            device_id={"y": to // cores, "core": to % cores}, device_id_type=MESH)

    w2 = ring(w2_ref.at[:, pl.ds(0, w2_full.shape[2])], lambda n: w2_full.at[n], "y", w2_ref.shape[0] // 2, w2_send, w2_recv)
    w1 = ring(w1_own, lambda n: w1_full.at[n], "y", w1_own.shape[0] // 2, w1_send, w1_recv)
    wo = ring(wo_ref, lambda n: wo_full.at[n], "y", wo_ref.shape[0] // 32 * 16, wo_send, wo_recv)

    def load_query(b, slot):
        b = jnp.minimum(b, 2 * groups - 1)
        dest, part = (me + 1 + b // 2) % groups, b % 2
        for j in range(subs):
            g = (part * subs + j) * cores + dest % cores
            at = pl.multiple_of((dest // cores) * sub, sub)
            qt = qkv_ref[g, 0:hd, pl.ds(at, sub)].astype(F32) * scale
            hi = qt.astype(BF)
            rest = qt - hi.astype(F32)
            mid = rest.astype(BF)
            cols = slice(j * sub, (j + 1) * sub)
            qaug_ref[slot, 0:hd, cols] = hi
            qaug_ref[slot, hd:2 * hd, cols] = mid
            qaug_ref[slot, 2 * hd:3 * hd, cols] = (rest - mid.astype(F32)).astype(BF)

    def fold(piece, op):
        return op(piece.reshape(piece.shape[0] // 8, 8, bq), axis=0)

    @pl.when(i == 0)
    def _():
        met = hail({"x": right}, {"x": left}, *[
            {"y": (me + hop) % groups // cores, "core": (me + hop) % cores} for hop in range(1, groups)])
        zeros = jnp.zeros((pad, TK), BF)

        def spread(t, c):
            g = t * TK // toks
            t0 = pl.multiple_of(t * TK - g * toks, TK)
            kt = qkv_ref[g, hd:2 * hd, pl.ds(t0, TK)]
            kaug_ref[pl.ds(pl.multiple_of(t * TK, TK), TK), :] = jnp.concatenate([kt, kt, kt, zeros], axis=0).T
            return c

        lax.fori_loop(0, keys // TK, spread, 0, unroll=4)
        qaug_ref[:, 3 * hd:, :] = jnp.zeros((2, pad, bq), BF)
        load_query(0, 0)
        load_query(1, 1)

        def first(c, m8):
            at = pl.ds(pl.multiple_of(c * 4 * TK, 4 * TK), 4 * TK)
            s = jnp.dot(kaug_ref[at, :], qaug_ref[0], preferred_element_type=F32)
            sa_ref[at, :] = s
            return jnp.maximum(m8, fold(s, jnp.max))

        m8 = lax.fori_loop(0, keys // (4 * TK), first, jnp.full((8, bq), -jnp.inf, F32))
        m_ref[...] = jnp.broadcast_to(jnp.max(m8, axis=0, keepdims=True), (8, bq))
        met()
        start(w1, 3, 4, 5, 6)
        start(wo, 0, 1, 2)
        start(w2, 0, 1, 2)
        x_copy(0).start()
        x_copy(1).start()

    @pl.when(i == groups // 2)
    def _():
        x_copy(0).wait()
        x_copy(1).wait()
        x_copy(2).start()
        x_copy(3).start()
        arrived(w1, 3, 4)
        start(w1, 7)

    @pl.when(i == groups // 2 + 1)
    def _():
        for copies in (wo, w2):
            arrived(copies, 0, 1)
            start(copies, 3, 4, 5, 6)

    @pl.when(i == groups - 1)
    def _():
        for copies in (wo, w2):
            arrived(copies, 3, 4)
            start(copies, 7)

    def half(s_in, s_out, slot, col):
        m = m_ref[0:1, :]
        acc_ref[...] = jnp.zeros_like(acc_ref)

        def trip(c, carry):
            m8, l8 = carry
            k0 = pl.multiple_of(c * chunk, chunk)
            total = None
            for u in range(TRIP):
                s_new = jnp.dot(kaug_ref[pl.ds(k0 + u * TK, TK), :], qaug_ref[slot], preferred_element_type=F32)
                ps = []
                for r in range(0, TK, ROWS):
                    p = jnp.exp2(s_in[pl.ds(k0 + u * TK + r, ROWS), :] - m)
                    l8 = l8 + fold(p, jnp.sum)
                    ps.append(p.astype(BF))
                at = u * TK % toks
                vt = qkv_ref[k0 // toks + u * TK // toks, 2 * hd:3 * hd, at:at + TK]
                d = jnp.dot(vt, jnp.concatenate(ps, axis=0), preferred_element_type=F32)
                total = d if total is None else total + d
                for r in range(0, TK, ROWS):
                    piece = s_new[r:r + ROWS]
                    m8 = jnp.maximum(m8, fold(piece, jnp.max))
                    s_out[pl.ds(k0 + u * TK + r, ROWS), :] = piece
            acc_ref[...] += total
            return m8, l8

        m8, l8 = lax.fori_loop(0, keys // chunk, trip, (jnp.full((8, bq), -jnp.inf, F32), jnp.zeros((8, bq), F32)))
        o_buf[i, :, col:col + bq] = (acc_ref[...] / jnp.sum(l8, axis=0, keepdims=True)).astype(BF)
        m_ref[...] = jnp.broadcast_to(jnp.max(m8, axis=0, keepdims=True), (8, bq))

    half(sa_ref, sb_ref, 1, 0)
    load_query(2 * i + 2, 0)
    half(sb_ref, sa_ref, 0, bq)
    load_query(2 * i + 3, 1)

    @pl.when(i < groups - 1)
    def _():
        o_copy(i).start()

    @pl.when(i == groups - 1)
    def _():
        own = pltpu.make_async_copy(o_buf.at[i], oin_ref.at[me], o_send.at[groups - 1])
        own.start()
        x_copy(2).wait()
        x_copy(3).wait()
        for step in range(groups - 1):
            o_copy(step).wait()
        own.wait()
        for copies in (wo, w2):
            arrived(copies, 2, 5, 6, 7)
            for copy in copies:
                copy.wait_send()
        arrived(w1, 5, 6, 7)
        for copy in w1[3:]:
            copy.wait_send()


def first_columns(model):
    return model * 2 // 5 // 256 * 256


def attention(qkv, normed, own, w1, cores, side):
    groups, three, toks = qkv.shape
    w1_own, w2, wo = own
    hd = three // 3
    keys = groups * toks
    bq = toks // 2
    anywhere = pl.BlockSpec(memory_space=pl.ANY)
    return pl.pallas_call(
        functools.partial(attn_kernel, hd, side, cores, toks // side),
        grid=(groups,),
        in_specs=[pl.BlockSpec((groups, three, toks), lambda i: (0, 0, 0))] + [anywhere] * 5,
        out_specs=[anywhere] * 5,
        input_output_aliases={5: 4},
        out_shape=[
            jax.ShapeDtypeStruct((groups, hd, toks), BF),
            jax.ShapeDtypeStruct((side,) + normed.shape, BF),
            jax.ShapeDtypeStruct((groups, w2.shape[0], first_columns(w2.shape[1])), BF),
            jax.ShapeDtypeStruct((groups,) + wo.shape, BF),
            jax.ShapeDtypeStruct(w1.shape, BF),
        ],
        scratch_shapes=[
            pltpu.VMEM((keys, 256), BF),
            pltpu.VMEM((2, 256, bq), BF),
            pltpu.VMEM((keys, bq), F32),
            pltpu.VMEM((keys, bq), F32),
            pltpu.VMEM((hd, bq), F32),
            pltpu.VMEM((8, bq), F32),
            pltpu.VMEM((groups, hd, toks), BF),
            pltpu.SemaphoreType.DMA((groups,)),
            pltpu.SemaphoreType.DMA((groups - 1,)),
            pltpu.SemaphoreType.DMA((4,)),
            pltpu.SemaphoreType.DMA((4,)),
            pltpu.SemaphoreType.DMA((8,)),
            pltpu.SemaphoreType.DMA((8,)),
            pltpu.SemaphoreType.DMA((8,)),
            pltpu.SemaphoreType.DMA((8,)),
            pltpu.SemaphoreType.DMA((8,)),
            pltpu.SemaphoreType.DMA((8,)),
        ],
        compiler_params=pltpu.CompilerParams(
            vmem_limit_bytes=58 * 1024 * 1024, collective_id=1, has_side_effects=True),
        cost_estimate=pl.CostEstimate(flops=6 * keys * keys * hd, bytes_accessed=8 * keys * hd, transcendentals=keys * keys),
        name="attention",
    )(qkv, normed, w1_own, w2, wo, w1)


def mlp_kernel(side, cores, x_ref, wide_ref, oin_ref, w1_own, w2_own, wo_own, w1_ref, w2_ref, wo_ref, res_ref, y_ref, w1, w2, xv, xt, ov,
               hv, part, far, near, res, load, w1_sem, send, recv, w2_send, w2_recv):
    x, y = lax.axis_index("x"), lax.axis_index("y")
    right, left = {"x": (x + 1) % side}, {"x": (x + side - 1) % side}
    rows, model = x_ref.shape
    groups = w1_ref.shape[0]
    width = groups * w1_own.shape[0]
    heads = groups * wo_own.shape[0]
    cut = w2_ref.shape[2]
    step = math.gcd(cut, model - cut, 512)
    half = rows // 2
    me = y * cores + lax.axis_index("core")
    top, low = pl.ds(0, half), pl.ds(half, half)
    order = (2, 1, 3, 0)

    def x_load(n):
        src = x_ref if order[n] == 0 else wide_ref.at[order[n]]
        return pltpu.make_async_copy(src, xv.at[n % 2], load.at[n % 2])

    def shard(into, base, size, n, columns):
        return into.at[pl.ds(pl.multiple_of(base + n * size, 16), size), columns]

    def gathered(own, full, into, base, sem):
        size, columns = full.shape[1], pl.ds(0, full.shape[2])
        for hop in range(groups):
            n = (me + hop) % groups
            pltpu.make_async_copy(full.at[n] if hop else own.at[:, columns], shard(into, base, size, n, columns), sem).start()
        whole = into.at[pl.ds(base, groups * size), columns]
        return pltpu.make_async_copy(whole, whole, sem)

    o_load = pltpu.make_async_copy(oin_ref, ov, load.at[2])
    res_load = pltpu.make_async_copy(res_ref, res, load.at[3])
    rest = pl.ds(cut, model - cut)
    rest_own = pltpu.make_async_copy(w2_own.at[:, rest], shard(w2, 0, width // groups, me, rest), load.at[7])
    x_load(0).start()
    pair = 2 * w1_own.shape[0]

    def w1_shard(n):
        to = shard(w1, 0, pair // 2, n, pl.ds(0, model))

        @pl.when(n == me)
        def _():
            pltpu.make_async_copy(w1_own, to, w1_sem.at[n // 2]).start()

        @pl.when(n != me)
        def _():
            pltpu.make_async_copy(w1_ref.at[n], to, w1_sem.at[n // 2]).start()

    for n in range(groups):
        w1_shard(n)
    o_load.start()
    w2_load = gathered(w2_own, w2_ref, w2, 0, load.at[5])
    wo_load = gathered(wo_own, wo_ref, w2, width, load.at[6])
    rest_own.start()
    x_load(1).start()
    res_load.start()
    met = hail(right, left, {"y": (y + 1) % side}, {"y": (y + side - 1) % side}, {"core": (lax.axis_index("core") + 1) % cores})
    w2_rest = ring(w2_own.at[:, rest], lambda n: shard(w2, 0, width // groups, n, rest), "y", width // groups // 2, w2_send, w2_recv)

    def hidden(n):
        x_load(n).wait()

        def flip(k, c):
            at = pl.ds(pl.multiple_of(k * 256, 256), 256)
            xt[at, :] = xv[n % 2, :, at].T
            return c

        lax.fori_loop(0, model // 256, flip, 0, unroll=2)
        if n < 2:
            x_load(n + 2).start()
        col = pl.multiple_of((x + order[n]) % side * rows, rows)
        if n == 0:
            o_load.wait()
        hv[n, :, width:] = ov[:, :, pl.ds(col, rows)].reshape(heads, rows).T

        def piece(f, c):
            at = pl.ds(pl.multiple_of(f * pair, pair), pair)
            if n == 0:
                pltpu.make_async_copy(w1.at[at], w1.at[at], w1_sem.at[f]).wait()
            pre = jnp.dot(w1[at, :], xt[...], preferred_element_type=F32)
            hv[n, :, at] = jax.nn.gelu(pre, approximate=True).astype(BF).T
            return c

        lax.fori_loop(0, groups // 2, piece, 0)

    def outs(n, lo, hi):
        def piece(d, c):
            at = pl.ds(pl.multiple_of(d * step, step), step)
            part[n % 3, :, at] = jnp.dot(hv[n], w2[:, at], preferred_element_type=F32)
            return c

        lax.fori_loop(lo // step, hi // step, piece, 0)

    def phase(lo, hi, first, prepare, between):
        cols = pl.ds(lo, hi - lo)
        plan = (
            (part.at[0, top, cols], far.at[0, :, cols], right),
            (part.at[0, low, cols], far.at[1, :, cols], left),
            (part.at[1, low, cols], near.at[0, low, cols], right),
            (part.at[2, top, cols], near.at[1, top, cols], left),
            (part.at[1, top, cols], near.at[0, top, cols], right),
            (part.at[2, low, cols], near.at[1, low, cols], left),
        )
        puts = [
            pltpu.make_async_remote_copy(src_ref=src, dst_ref=dst, send_sem=send.at[first + n], recv_sem=recv.at[first + n],
                                         device_id=to, device_id_type=MESH)
            for n, (src, dst, to) in enumerate(plan)
        ]
        prepare(0)
        outs(0, lo, hi)
        start(puts, 0, 1)
        prepare(1)
        outs(1, lo, hi)
        start(puts, 2)
        prepare(2)
        outs(2, lo, hi)
        start(puts, 3)
        between()
        puts[0].wait()
        part[1, :half, lo:hi] += far[0, :, lo:hi]
        start(puts, 4)
        puts[1].wait()
        part[2, half:, lo:hi] += far[1, :, lo:hi]
        start(puts, 5)
        prepare(3)
        outs(3, lo, hi)
        return puts[2:]

    def ready(n):
        hidden(n)
        if n == 0:
            met()
            start(w2_rest, 0, 1, 2)
            w2_load.wait()
            wo_load.wait()

    def pass_on():
        arrived(w2_rest, 0, 1)
        start(w2_rest, 3, 4, 5, 6)

    waits = phase(0, cut, 0, ready, pass_on)
    arrived(w2_rest, 3, 4)
    start(w2_rest, 7)
    rest_own.wait()
    arrived(w2_rest, 2, 5, 6, 7)
    waits += phase(cut, model, 6, lambda n: None, lambda: None)
    res_load.wait()
    part[0] += res[...].astype(F32)
    for put in waits:
        put.wait()
    for copy in w2_rest:
        copy.wait_send()
    y_ref[...] = (part[0] + near[0] + near[1]).astype(BF)


def mlp(x_loc, normed, wide, oin, own, full, cores, side):
    rows, model = normed.shape
    groups = side * cores
    width, heads = groups * own[0].shape[0], groups * own[2].shape[0]
    anywhere = pl.BlockSpec(memory_space=pl.ANY)
    flops = 2 * side * rows * model * (2 * width + heads)
    return pl.pallas_call(
        functools.partial(mlp_kernel, side, cores),
        in_specs=[anywhere] * 10,
        out_specs=pl.BlockSpec(memory_space=pltpu.VMEM),
        out_shape=jax.ShapeDtypeStruct((rows, model), BF),
        scratch_shapes=[
            pltpu.VMEM((width, model), BF),
            pltpu.VMEM((width + heads, model), BF),
            pltpu.VMEM((2, rows, model), BF),
            pltpu.VMEM((model, rows), BF),
            pltpu.VMEM(oin.shape, BF),
            pltpu.VMEM((side, rows, width + heads), BF),
            pltpu.VMEM((3, rows, model), F32),
            pltpu.VMEM((2, rows // 2, model), F32),
            pltpu.VMEM((2, rows, model), F32),
            pltpu.VMEM((rows, model), BF),
            pltpu.SemaphoreType.DMA((8,)),
            pltpu.SemaphoreType.DMA((groups // 2,)),
            pltpu.SemaphoreType.DMA((12,)),
            pltpu.SemaphoreType.DMA((12,)),
            pltpu.SemaphoreType.DMA((8,)),
            pltpu.SemaphoreType.DMA((8,)),
        ],
        compiler_params=pltpu.CompilerParams(vmem_limit_bytes=67043328, collective_id=2, has_side_effects=True),
        cost_estimate=pl.CostEstimate(flops=flops, bytes_accessed=4 * model * width, transcendentals=side * rows * width),
        name="mlp",
    )(normed, wide, oin, *own, *full, x_loc)


def solution(mesh):
    data, tp = mesh.devices.shape
    side = math.isqrt(tp // 2)
    cores = tp // (side * side)
    grid = Mesh(mesh.devices.reshape(data, side, side, cores), ("data", "y", "x", "core"))

    def local_block(x_loc, ln_gamma, w_qkv, w_out, w_up, w_down):
        own = (w_up.T, w_down, w_out[0])
        qkv, normed, w1 = qkv_stage(x_loc, ln_gamma, w_qkv[:, 0, :].T, own[0], cores, side)
        oin, wide, w2, wo, w1 = attention(qkv, normed, own, w1, cores, side)
        return mlp(x_loc, normed, wide, oin, own, (w1, w2, wo), cores, side)

    row_spec = P(("data", "y", "x", "core"), None)
    tp_axes = ("y", "x", "core")
    return jax.shard_map(
        local_block,
        mesh=grid,
        in_specs=(row_spec, P(None), P(None, tp_axes, None), P(tp_axes, None, None), P(None, tp_axes), P(tp_axes, None)),
        out_specs=row_spec,
        check_vma=False,
    )
```

```python
import functools
import math
import jax
import jax.numpy as jnp
from jax import lax
from jax.experimental import pallas as pl
from jax.experimental.pallas import tpu as pltpu
from jax.sharding import Mesh, PartitionSpec as P

LN_EPS = 1e-6
BF = jnp.bfloat16
MESH = pl.DeviceIdType.MESH
F32 = jnp.float32
TK = 256
TRIP = 32
ROWS = 64


def ring(own, slot, axis, split, send, recv):
    side, cores = lax.axis_size(axis), lax.axis_size("core")
    at, core = lax.axis_index(axis), lax.axis_index("core")
    other = (core + 1) % cores
    block = lambda hop: slot((at + hop) % side * cores + core)
    head, tail = pl.ds(0, split), pl.ds(split, own.shape[0] - split)
    nxt, prv, sib = {axis: (at + 1) % side}, {axis: (at + side - 1) % side}, {"core": other}
    plan = (
        (own, block(0), nxt),
        (own, block(0), prv),
        (own, block(0), sib),
        (block(side - 1).at[head], block(side - 1).at[head], nxt),
        (block(1).at[tail], block(1).at[tail], prv),
        (block(side - 1), block(side - 1), sib),
        (block(1), block(1), sib),
        (block(2), block(2), sib),
    )
    return [
        pltpu.make_async_remote_copy(
            src_ref=src, dst_ref=dst, send_sem=send.at[n], recv_sem=recv.at[n], device_id=to, device_id_type=MESH)
        for n, (src, dst, to) in enumerate(plan)
    ]


def start(copies, *which):
    for n in which:
        copies[n].start()


def arrived(copies, *which):
    for n in which:
        copies[n].wait_recv()


def hail(*places):
    barrier = pltpu.get_barrier_semaphore()
    for place in places:
        pl.semaphore_signal(barrier, inc=1, device_id=place, device_id_type=MESH)
    return lambda: pl.semaphore_wait(barrier, len(places))


def qkv_kernel(side, cores, x_ref, gain_ref, wq_ref, w1_ref, qkv_ref, normed_ref, w1_full, wv, xv, xt, qk,
               wq_send, wq_recv, x_send, x_recv, w1_send, w1_recv, a_send, a_recv, local):
    y, x, core = lax.axis_index("y"), lax.axis_index("x"), lax.axis_index("core")
    rows, model = x_ref.shape
    low = rows // 2
    me = x * cores + core
    up, down = {"y": (y + 1) % side}, {"y": (y + side - 1) % side}
    met = hail(up, down, *[
        {"x": (x + dx) % side, "core": (core + dc) % cores} for dx in range(side) for dc in range(cores) if dx or dc])

    wq = ring(wq_ref, lambda n: wv.at[n], "x", wq_ref.shape[0] // 32 * 16, wq_send, wq_recv)
    w1 = ring(w1_ref, lambda n: w1_full.at[n], "y", w1_ref.shape[0] // 2, w1_send, w1_recv)
    own_wq = pltpu.make_async_copy(wq_ref, wv.at[me], local.at[0])
    own_wq.start()

    def x_copy(n, src, to):
        return pltpu.make_async_remote_copy(
            src_ref=src, dst_ref=src, send_sem=x_send.at[n], recv_sem=x_recv.at[n], device_id=to, device_id_type=MESH)

    before, after, far = (y + side - 1) % side, (y + 1) % side, (y + 2) % side
    xs = [
        x_copy(0, xv.at[y], up),
        x_copy(1, xv.at[y], down),
        x_copy(2, xv.at[before, pl.ds(0, low)], up),
        x_copy(3, xv.at[after, pl.ds(low, low)], down),
    ]

    def norm(r, c):
        at = pl.ds(pl.multiple_of(r * 32, 32), 32)
        row = x_ref[at, :].astype(F32)
        mean = jnp.mean(row, axis=-1, keepdims=True)
        centered = row - mean
        var = jnp.mean(centered * centered, axis=-1, keepdims=True)
        xv[y, at, :] = (centered * lax.rsqrt(var + LN_EPS) * gain_ref[...].reshape(1, model)).astype(BF)
        return c

    lax.fori_loop(0, rows // 32, norm, 0)

    def cols(part):
        return pl.ds(pl.multiple_of(part * rows, rows), rows)

    def flip(part):
        def piece(k, c):
            at = pl.ds(pl.multiple_of(k * 256, 256), 256)
            xt[at, cols(part)] = xv[part, :, at].T
            return c

        lax.fori_loop(0, model // 256, piece, 0, unroll=2)

    flip(y)
    met()
    start(wq, 0, 1, 2)
    start(xs, 0, 1)
    start(w1, 2)
    keep = pltpu.make_async_copy(xv.at[y], normed_ref, local.at[1])
    keep.start()

    def unit(head, part):
        qk[head, :, cols(part)] = jnp.dot(wv[head], xt[:, cols(part)], preferred_element_type=F32).astype(BF)

    def send(n, head, *at):
        return pltpu.make_async_remote_copy(
            src_ref=qk.at[head, *at], dst_ref=qkv_ref.at[me, *at], send_sem=a_send.at[n], recv_sem=a_recv.at[n],
            device_id={"x": head // cores, "core": head % cores}, device_id_type=MESH)

    def head_of(n):
        return (x + n // cores) % side * cores + (core + n) % cores

    close = lambda k: cores * (1 + 2 * (k // cores)) + k % cores
    distant = lambda k: 2 * cores + k

    def work(count, pick, parts, go=True):
        def body(k, c):
            n = pick(k)
            for part in parts:
                unit(head_of(n), part)
            if go:
                for part in parts:
                    send(n, head_of(n), slice(None), cols(part)).start()
            return c

        lax.fori_loop(0, count, body, 0)

    arrived(wq, 0, 1)
    start(wq, 3, 4, 5, 6)
    arrived(xs, 0, 1)
    start(xs, 2, 3)
    start(w1, 0, 1)
    flip(before)
    flip(after)
    own_wq.wait()
    arrived(wq, 2, 5, 6)
    work(2 * cores, close, (y, after, before))
    arrived(wq, 3, 4)
    start(wq, 7)
    work(cores, lambda k: k, (y, after, before), go=False)
    arrived(wq, 7)
    work(cores, distant, (y, after, before))
    arrived(xs, 2, 3)
    flip(far)
    work(cores, distant, (far,))
    work(2 * cores, close, (far,))
    work(cores, lambda k: k, (far,), go=False)
    for n in range(1, cores):
        send(n, head_of(n)).start()
    own = pltpu.make_async_copy(qk.at[me], qkv_ref.at[me], local.at[2])
    own.start()
    for n in range(1, side * cores):
        send(n, head_of(n)).wait()
    own.wait()
    keep.wait()
    arrived(w1, 0, 1, 2)
    for copies in (wq, w1[:3], xs):
        for copy in copies:
            copy.wait_send()


def qkv_stage(x_loc, gain, wq, w1, cores, side):
    rows, model = x_loc.shape
    groups = side * cores
    anywhere = pl.BlockSpec(memory_space=pl.ANY)
    vmem = pl.BlockSpec(memory_space=pltpu.VMEM)
    dma = lambda n: pltpu.SemaphoreType.DMA((n,))
    return pl.pallas_call(
        functools.partial(qkv_kernel, side, cores),
        in_specs=[vmem, vmem, anywhere, anywhere],
        out_specs=[anywhere] * 3,
        out_shape=[
            jax.ShapeDtypeStruct((groups, wq.shape[0], side * rows), BF),
            jax.ShapeDtypeStruct((rows, model), BF),
            jax.ShapeDtypeStruct((groups,) + w1.shape, BF),
        ],
        scratch_shapes=[
            pltpu.VMEM((groups,) + wq.shape, BF),
            pltpu.VMEM((side, rows, model), BF),
            pltpu.VMEM((model, side * rows), BF),
            pltpu.VMEM((groups, wq.shape[0], side * rows), BF),
            dma(8), dma(8), dma(4), dma(4), dma(8), dma(8), dma(groups), dma(groups), dma(3),
        ],
        compiler_params=pltpu.CompilerParams(vmem_limit_bytes=58 * 1024 * 1024, collective_id=0, has_side_effects=True),
        cost_estimate=pl.CostEstimate(flops=2 * side * rows * model * groups * wq.shape[0], bytes_accessed=4 * w1.size, transcendentals=0),
        name="qkv",
    )(x_loc, gain, wq, w1)


def attn_kernel(hd, side, cores, sub, qkv_ref, x_ref, w1_own, w2_ref, wo_ref, w1_part, oin_ref, wide_ref, w2_full, wo_full, w1_full, kaug_ref, qaug_ref, sa_ref,
                sb_ref, acc_ref, m_ref, o_buf, o_send, o_recv, x_send, x_recv, w2_send, w2_recv, wo_send, wo_recv, w1_send, w1_recv):
    groups, _, toks = qkv_ref.shape
    keys = groups * toks
    bq = sa_ref.shape[1]
    subs = bq // sub
    i = pl.program_id(0)
    scale = hd ** -0.5 * math.log2(math.e)
    pad = kaug_ref.shape[1] - 3 * hd
    chunk = min(TRIP * TK, keys)
    y, core, x = lax.axis_index("y"), lax.axis_index("core"), lax.axis_index("x")
    me = y * cores + core
    right, left = (x + 1) % side, (x + side - 1) % side
    rows = x_ref.shape[0]
    top, low = pl.ds(0, rows // 2), pl.ds(rows // 2, rows // 2)

    def x_copy(n):
        src = (x_ref, x_ref, wide_ref.at[3, top], wide_ref.at[1, low])[n]
        dst = (wide_ref.at[3], wide_ref.at[1], wide_ref.at[2, top], wide_ref.at[2, low])[n]
        return pltpu.make_async_remote_copy(
            src_ref=src, dst_ref=dst, send_sem=x_send.at[n], recv_sem=x_recv.at[n],
            device_id={"x": left if n % 2 else right}, device_id_type=MESH)

    def o_copy(step):
        to = (me + 1 + step) % groups
        return pltpu.make_async_remote_copy(
            src_ref=o_buf.at[step], dst_ref=oin_ref.at[me], send_sem=o_send.at[step], recv_sem=o_recv.at[step],
            device_id={"y": to // cores, "core": to % cores}, device_id_type=MESH)

    w2 = ring(w2_ref.at[:, pl.ds(0, w2_full.shape[2])], lambda n: w2_full.at[n], "y", w2_ref.shape[0] // 2, w2_send, w2_recv)
    w1 = ring(w1_own, lambda n: w1_full.at[n], "y", w1_own.shape[0] // 2, w1_send, w1_recv)
    wo = ring(wo_ref, lambda n: wo_full.at[n], "y", wo_ref.shape[0] // 32 * 16, wo_send, wo_recv)

    def load_query(b, slot):
        b = jnp.minimum(b, 2 * groups - 1)
        dest, part = (me + 1 + b // 2) % groups, b % 2
        for j in range(subs):
            g = (part * subs + j) * cores + dest % cores
            at = pl.multiple_of((dest // cores) * sub, sub)
            qt = qkv_ref[g, 0:hd, pl.ds(at, sub)].astype(F32) * scale
            hi = qt.astype(BF)
            rest = qt - hi.astype(F32)
            mid = rest.astype(BF)
            cols = slice(j * sub, (j + 1) * sub)
            qaug_ref[slot, 0:hd, cols] = hi
            qaug_ref[slot, hd:2 * hd, cols] = mid
            qaug_ref[slot, 2 * hd:3 * hd, cols] = (rest - mid.astype(F32)).astype(BF)

    def fold(piece, op):
        return op(piece.reshape(piece.shape[0] // 8, 8, bq), axis=0)

    @pl.when(i == 0)
    def _():
        met = hail({"x": right}, {"x": left}, *[
            {"y": (me + hop) % groups // cores, "core": (me + hop) % cores} for hop in range(1, groups)])
        zeros = jnp.zeros((pad, TK), BF)

        def spread(t, c):
            g = t * TK // toks
            t0 = pl.multiple_of(t * TK - g * toks, TK)
            kt = qkv_ref[g, hd:2 * hd, pl.ds(t0, TK)]
            kaug_ref[pl.ds(pl.multiple_of(t * TK, TK), TK), :] = jnp.concatenate([kt, kt, kt, zeros], axis=0).T
            return c

        lax.fori_loop(0, keys // TK, spread, 0, unroll=4)
        qaug_ref[:, 3 * hd:, :] = jnp.zeros((2, pad, bq), BF)
        load_query(0, 0)
        load_query(1, 1)
        met()
        start(w1, 3, 4, 5, 6)
        start(wo, 0, 1, 2)
        start(w2, 0, 1, 2)
        x_copy(0).start()
        x_copy(1).start()

        def first(c, m8):
            at = pl.ds(pl.multiple_of(c * 8 * TK, 8 * TK), 8 * TK)
            s = jnp.dot(kaug_ref[at, :], qaug_ref[0], preferred_element_type=F32)
            sa_ref[at, :] = s
            return jnp.maximum(m8, fold(s, jnp.max))

        m8 = lax.fori_loop(0, keys // (8 * TK), first, jnp.full((8, bq), -jnp.inf, F32))
        m_ref[...] = jnp.broadcast_to(jnp.max(m8, axis=0, keepdims=True), (8, bq))

    @pl.when(i == groups // 2)
    def _():
        x_copy(0).wait()
        x_copy(1).wait()
        x_copy(2).start()
        x_copy(3).start()
        arrived(w1, 3, 4)
        start(w1, 7)

    @pl.when(i == groups // 2 + 1)
    def _():
        for copies in (wo, w2):
            arrived(copies, 0, 1)
            start(copies, 3, 4, 5, 6)

    @pl.when(i == groups - 1)
    def _():
        for copies in (wo, w2):
            arrived(copies, 3, 4)
            start(copies, 7)

    def half(s_in, s_out, slot, col):
        m = m_ref[0:1, :]
        acc_ref[...] = jnp.zeros_like(acc_ref)

        def trip(c, carry):
            m8, l8 = carry
            k0 = pl.multiple_of(c * chunk, chunk)
            total = None
            for u in range(chunk // TK):
                s_new = jnp.dot(kaug_ref[pl.ds(k0 + u * TK, TK), :], qaug_ref[slot], preferred_element_type=F32)
                ps = []
                for r in range(0, TK, ROWS):
                    p = jnp.exp2(s_in[pl.ds(k0 + u * TK + r, ROWS), :] - m)
                    l8 = l8 + fold(p, jnp.sum)
                    ps.append(p.astype(BF))
                at = u * TK % toks
                vt = qkv_ref[k0 // toks + u * TK // toks, 2 * hd:3 * hd, at:at + TK]
                d = jnp.dot(vt, jnp.concatenate(ps, axis=0), preferred_element_type=F32)
                total = d if total is None else total + d
                for r in range(0, TK, ROWS):
                    piece = s_new[r:r + ROWS]
                    m8 = jnp.maximum(m8, fold(piece, jnp.max))
                    s_out[pl.ds(k0 + u * TK + r, ROWS), :] = piece
            acc_ref[...] += total
            return m8, l8

        m8, l8 = lax.fori_loop(0, (1 + i // groups) * (keys // chunk), trip, (jnp.full((8, bq), -jnp.inf, F32), jnp.zeros((8, bq), F32)))
        o_buf[i, :, col:col + bq] = (acc_ref[...] / jnp.sum(l8, axis=0, keepdims=True)).astype(BF)
        m_ref[...] = jnp.broadcast_to(jnp.max(m8, axis=0, keepdims=True), (8, bq))

    half(sa_ref, sb_ref, 1, 0)
    load_query(2 * i + 2, 0)
    half(sb_ref, sa_ref, 0, bq)
    load_query(2 * i + 3, 1)

    @pl.when(i < groups - 1)
    def _():
        o_copy(i).start()

    @pl.when(i == groups - 1)
    def _():
        own = pltpu.make_async_copy(o_buf.at[i], oin_ref.at[me], o_send.at[groups - 1])
        own.start()
        x_copy(2).wait()
        x_copy(3).wait()
        for step in range(groups - 1):
            o_copy(step).wait()
        own.wait()
        for copies in (wo, w2):
            arrived(copies, 2, 5, 6, 7)
            for copy in copies:
                copy.wait_send()
        arrived(w1, 5, 6, 7)
        for copy in w1[3:]:
            copy.wait_send()


def first_columns(model):
    return model * 2 // 5 // 256 * 256


def attention(qkv, normed, own, w1, cores, side):
    groups, three, toks = qkv.shape
    w1_own, w2, wo = own
    hd = three // 3
    keys = groups * toks
    bq = toks // 2
    anywhere = pl.BlockSpec(memory_space=pl.ANY)
    return pl.pallas_call(
        functools.partial(attn_kernel, hd, side, cores, toks // side),
        grid=(groups,),
        in_specs=[pl.BlockSpec((groups, three, toks), lambda i: (0, 0, 0))] + [anywhere] * 5,
        out_specs=[anywhere] * 5,
        input_output_aliases={5: 4},
        out_shape=[
            jax.ShapeDtypeStruct((groups, hd, toks), BF),
            jax.ShapeDtypeStruct((side,) + normed.shape, BF),
            jax.ShapeDtypeStruct((groups, w2.shape[0], first_columns(w2.shape[1])), BF),
            jax.ShapeDtypeStruct((groups,) + wo.shape, BF),
            jax.ShapeDtypeStruct(w1.shape, BF),
        ],
        scratch_shapes=[
            pltpu.VMEM((keys, 256), BF),
            pltpu.VMEM((2, 256, bq), BF),
            pltpu.VMEM((keys, bq), F32),
            pltpu.VMEM((keys, bq), F32),
            pltpu.VMEM((hd, bq), F32),
            pltpu.VMEM((8, bq), F32),
            pltpu.VMEM((groups, hd, toks), BF),
            pltpu.SemaphoreType.DMA((groups,)),
            pltpu.SemaphoreType.DMA((groups - 1,)),
            pltpu.SemaphoreType.DMA((4,)),
            pltpu.SemaphoreType.DMA((4,)),
            pltpu.SemaphoreType.DMA((8,)),
            pltpu.SemaphoreType.DMA((8,)),
            pltpu.SemaphoreType.DMA((8,)),
            pltpu.SemaphoreType.DMA((8,)),
            pltpu.SemaphoreType.DMA((8,)),
            pltpu.SemaphoreType.DMA((8,)),
        ],
        compiler_params=pltpu.CompilerParams(
            vmem_limit_bytes=58 * 1024 * 1024, collective_id=1, has_side_effects=True),
        cost_estimate=pl.CostEstimate(flops=6 * keys * keys * hd, bytes_accessed=8 * keys * hd, transcendentals=keys * keys),
        name="attention",
    )(qkv, normed, w1_own, w2, wo, w1)


def mlp_kernel(side, cores, x_ref, wide_ref, oin_ref, w1_own, w2_own, wo_own, w1_ref, w2_ref, wo_ref, res_ref, y_ref, w1, w2, xv, xt, ov,
               hv, part, far, near, res, load, w1_sem, send, recv, w2_send, w2_recv):
    x, y = lax.axis_index("x"), lax.axis_index("y")
    right, left = {"x": (x + 1) % side}, {"x": (x + side - 1) % side}
    rows, model = x_ref.shape
    groups = w1_ref.shape[0]
    width = groups * w1_own.shape[0]
    heads = groups * wo_own.shape[0]
    cut = w2_ref.shape[2]
    step = math.gcd(cut, model - cut, 512)
    half = rows // 2
    me = y * cores + lax.axis_index("core")
    top, low = pl.ds(0, half), pl.ds(half, half)
    order = (2, 1, 3, 0)

    def x_load(n):
        src = x_ref if order[n] == 0 else wide_ref.at[order[n]]
        return pltpu.make_async_copy(src, xv.at[n % 2], load.at[n % 2])

    def shard(into, base, size, n, columns):
        return into.at[pl.ds(pl.multiple_of(base + n * size, 16), size), columns]

    def gathered(own, full, into, base, sem):
        size, columns = full.shape[1], pl.ds(0, full.shape[2])
        for hop in range(groups):
            n = (me + hop) % groups
            pltpu.make_async_copy(full.at[n] if hop else own.at[:, columns], shard(into, base, size, n, columns), sem).start()
        whole = into.at[pl.ds(base, groups * size), columns]
        return pltpu.make_async_copy(whole, whole, sem)

    o_load = pltpu.make_async_copy(oin_ref, ov, load.at[2])
    res_load = pltpu.make_async_copy(res_ref, res, load.at[3])
    rest = pl.ds(cut, model - cut)
    rest_own = pltpu.make_async_copy(w2_own.at[:, rest], shard(w2, 0, width // groups, me, rest), load.at[7])
    x_load(0).start()
    pair = 2 * w1_own.shape[0]

    def w1_shard(n):
        to = shard(w1, 0, pair // 2, n, pl.ds(0, model))

        @pl.when(n == me)
        def _():
            pltpu.make_async_copy(w1_own, to, w1_sem.at[n // 2]).start()

        @pl.when(n != me)
        def _():
            pltpu.make_async_copy(w1_ref.at[n], to, w1_sem.at[n // 2]).start()

    for n in range(groups):
        w1_shard(n)
    o_load.start()
    w2_load = gathered(w2_own, w2_ref, w2, 0, load.at[5])
    wo_load = gathered(wo_own, wo_ref, w2, width, load.at[6])
    rest_own.start()
    x_load(1).start()
    res_load.start()
    met = hail(right, left, {"y": (y + 1) % side}, {"y": (y + side - 1) % side}, {"core": (lax.axis_index("core") + 1) % cores})
    w2_rest = ring(w2_own.at[:, rest], lambda n: shard(w2, 0, width // groups, n, rest), "y", width // groups // 2, w2_send, w2_recv)

    def hidden(n):
        x_load(n).wait()

        def flip(k, c):
            at = pl.ds(pl.multiple_of(k * 256, 256), 256)
            xt[at, :] = xv[n % 2, :, at].T
            return c

        lax.fori_loop(0, model // 256, flip, 0, unroll=2)
        if n < 2:
            x_load(n + 2).start()
        col = pl.multiple_of((x + order[n]) % side * rows, rows)
        if n == 0:
            o_load.wait()
        hv[n, :, width:] = ov[:, :, pl.ds(col, rows)].reshape(heads, rows).T
        if n == 0:
            met()
            start(w2_rest, 0, 1, 2)

        def piece(f, c):
            at = pl.ds(pl.multiple_of(f * pair, pair), pair)
            if n == 0:
                pltpu.make_async_copy(w1.at[at], w1.at[at], w1_sem.at[f]).wait()
            pre = jnp.dot(w1[at, :], xt[...], preferred_element_type=F32)
            hv[n, :, at] = jax.nn.gelu(pre, approximate=True).astype(BF).T
            return c

        lax.fori_loop(0, groups // 2, piece, 0)

    def outs(n, lo, hi):
        def piece(d, c):
            at = pl.ds(pl.multiple_of(d * step, step), step)
            part[n % 3, :, at] = jnp.dot(hv[n], w2[:, at], preferred_element_type=F32)
            return c

        lax.fori_loop(lo // step, hi // step, piece, 0)

    def phase(lo, hi, first, prepare, between):
        cols = pl.ds(lo, hi - lo)
        plan = (
            (part.at[0, top, cols], far.at[0, :, cols], right),
            (part.at[0, low, cols], far.at[1, :, cols], left),
            (part.at[1, low, cols], near.at[0, low, cols], right),
            (part.at[2, top, cols], near.at[1, top, cols], left),
            (part.at[1, top, cols], near.at[0, top, cols], right),
            (part.at[2, low, cols], near.at[1, low, cols], left),
        )
        puts = [
            pltpu.make_async_remote_copy(src_ref=src, dst_ref=dst, send_sem=send.at[first + n], recv_sem=recv.at[first + n],
                                         device_id=to, device_id_type=MESH)
            for n, (src, dst, to) in enumerate(plan)
        ]
        prepare(0)
        outs(0, lo, hi)
        start(puts, 0, 1)
        prepare(1)
        outs(1, lo, hi)
        start(puts, 2)
        prepare(2)
        outs(2, lo, hi)
        start(puts, 3)
        between()
        puts[0].wait()
        part[1, :half, lo:hi] += far[0, :, lo:hi]
        start(puts, 4)
        puts[1].wait()
        part[2, half:, lo:hi] += far[1, :, lo:hi]
        start(puts, 5)
        prepare(3)
        outs(3, lo, hi)
        return puts[2:]

    def ready(n):
        hidden(n)
        if n == 0:
            w2_load.wait()
            wo_load.wait()

    def pass_on():
        arrived(w2_rest, 0, 1)
        start(w2_rest, 3, 4, 5, 6)

    waits = phase(0, cut, 0, ready, pass_on)
    arrived(w2_rest, 3, 4)
    start(w2_rest, 7)
    rest_own.wait()
    arrived(w2_rest, 2, 5, 6, 7)
    waits += phase(cut, model, 6, lambda n: None, lambda: None)
    res_load.wait()
    part[0] += res[...].astype(F32)
    for put in waits:
        put.wait()
    for copy in w2_rest:
        copy.wait_send()
    y_ref[...] = (part[0] + near[0] + near[1]).astype(BF)


def mlp(x_loc, normed, wide, oin, own, full, cores, side):
    rows, model = normed.shape
    groups = side * cores
    width, heads = groups * own[0].shape[0], groups * own[2].shape[0]
    anywhere = pl.BlockSpec(memory_space=pl.ANY)
    flops = 2 * side * rows * model * (2 * width + heads)
    return pl.pallas_call(
        functools.partial(mlp_kernel, side, cores),
        in_specs=[anywhere] * 10,
        out_specs=pl.BlockSpec(memory_space=pltpu.VMEM),
        out_shape=jax.ShapeDtypeStruct((rows, model), BF),
        scratch_shapes=[
            pltpu.VMEM((width, model), BF),
            pltpu.VMEM((width + heads, model), BF),
            pltpu.VMEM((2, rows, model), BF),
            pltpu.VMEM((model, rows), BF),
            pltpu.VMEM(oin.shape, BF),
            pltpu.VMEM((side, rows, width + heads), BF),
            pltpu.VMEM((3, rows, model), F32),
            pltpu.VMEM((2, rows // 2, model), F32),
            pltpu.VMEM((2, rows, model), F32),
            pltpu.VMEM((rows, model), BF),
            pltpu.SemaphoreType.DMA((8,)),
            pltpu.SemaphoreType.DMA((groups // 2,)),
            pltpu.SemaphoreType.DMA((12,)),
            pltpu.SemaphoreType.DMA((12,)),
            pltpu.SemaphoreType.DMA((8,)),
            pltpu.SemaphoreType.DMA((8,)),
        ],
        compiler_params=pltpu.CompilerParams(vmem_limit_bytes=67043328, collective_id=2, has_side_effects=True),
        cost_estimate=pl.CostEstimate(flops=flops, bytes_accessed=4 * model * width, transcendentals=side * rows * width),
        name="mlp",
    )(normed, wide, oin, *own, *full, x_loc)


def solution(mesh):
    data, tp = mesh.devices.shape
    side = math.isqrt(tp // 2)
    cores = tp // (side * side)
    grid = Mesh(mesh.devices.reshape(data, side, side, cores), ("data", "y", "x", "core"))

    def local_block(x_loc, ln_gamma, w_qkv, w_out, w_up, w_down):
        own = (w_up.T, w_down, w_out[0])
        qkv, normed, w1 = qkv_stage(x_loc, ln_gamma, w_qkv[:, 0, :].T, own[0], cores, side)
        oin, wide, w2, wo, w1 = attention(qkv, normed, own, w1, cores, side)
        return mlp(x_loc, normed, wide, oin, own, (w1, w2, wo), cores, side)

    row_spec = P(("data", "y", "x", "core"), None)
    tp_axes = ("y", "x", "core")
    return jax.shard_map(
        local_block,
        mesh=grid,
        in_specs=(row_spec, P(None), P(None, tp_axes, None), P(tp_axes, None, None), P(None, tp_axes), P(tp_axes, None)),
        out_specs=row_spec,
        check_vma=False,
    )
```

```python
import functools
import math
import jax
import jax.numpy as jnp
from jax import lax
from jax.experimental import pallas as pl
from jax.experimental.pallas import tpu as pltpu
from jax.sharding import Mesh, PartitionSpec as P

LN_EPS = 1e-6
BF = jnp.bfloat16
MESH = pl.DeviceIdType.MESH
F32 = jnp.float32
TK = 256
TRIP = 32
ROWS = 64


def ring(own, slot, axis, split, send, recv):
    side, cores = lax.axis_size(axis), lax.axis_size("core")
    at, core = lax.axis_index(axis), lax.axis_index("core")
    other = (core + 1) % cores
    block = lambda hop: slot((at + hop) % side * cores + core)
    head, tail = pl.ds(0, split), pl.ds(split, own.shape[0] - split)
    nxt, prv, sib = {axis: (at + 1) % side}, {axis: (at + side - 1) % side}, {"core": other}
    plan = (
        (own, block(0), nxt),
        (own, block(0), prv),
        (own, block(0), sib),
        (block(side - 1).at[head], block(side - 1).at[head], nxt),
        (block(1).at[tail], block(1).at[tail], prv),
        (block(side - 1), block(side - 1), sib),
        (block(1), block(1), sib),
        (block(2), block(2), sib),
    )
    return [
        pltpu.make_async_remote_copy(
            src_ref=src, dst_ref=dst, send_sem=send.at[n], recv_sem=recv.at[n], device_id=to, device_id_type=MESH)
        for n, (src, dst, to) in enumerate(plan)
    ]


def start(copies, *which):
    for n in which:
        copies[n].start()


def arrived(copies, *which):
    for n in which:
        copies[n].wait_recv()


def hail(*places):
    barrier = pltpu.get_barrier_semaphore()
    for place in places:
        pl.semaphore_signal(barrier, inc=1, device_id=place, device_id_type=MESH)
    return lambda: pl.semaphore_wait(barrier, len(places))


def front_kernel(side, cores, hd, x_ref, gain_ref, wq_ref, w1_ref, w2_ref, wo_ref, oin_ref, wide_ref, w1_full, w2_full, wo_full,
                 wv, xv, qk, qkv, qaug, acc_ref, m_ref, wq_send, wq_recv, xs_send, xs_recv, w1_send, w1_recv, a_send, a_recv, o_send, o_recv,
                 xw_send, xw_recv, w2_send, w2_recv, wo_send, wo_recv, local):
    y, x, core = lax.axis_index("y"), lax.axis_index("x"), lax.axis_index("core")
    rows, model = x_ref.shape
    groups, toks = side * cores, side * rows
    keys = groups * toks
    bq = toks // 2
    subs = bq // rows
    scale = hd ** -0.5 * math.log2(math.e)
    depth = qaug.shape[1]
    pad = depth - 3 * hd
    chunk = min(TRIP * TK, keys)
    row_me, col_me = x * cores + core, y * cores + core
    up, down = {"y": (y + 1) % side}, {"y": (y + side - 1) % side}
    right, left = {"x": (x + 1) % side}, {"x": (x + side - 1) % side}
    top, low = pl.ds(0, rows // 2), pl.ds(rows // 2, rows // 2)
    apart = [(d, dc) for d in range(side) for dc in range(cores) if d or dc]
    met = hail(
        *[{"x": (x + d) % side, "core": (core + dc) % cores} for d, dc in apart],
        *[{"y": (y + d) % side, "core": (core + dc) % cores} for d, dc in apart if d])

    wq = ring(wq_ref, lambda n: wv.at[n], "x", wq_ref.shape[0] // 32 * 16, wq_send, wq_recv)
    w1 = ring(w1_ref, lambda n: w1_full.at[n], "y", w1_ref.shape[0] // 2, w1_send, w1_recv)
    w2 = ring(w2_ref.at[:, pl.ds(0, w2_full.shape[2])], lambda n: w2_full.at[n], "y", w2_ref.shape[0] // 2, w2_send, w2_recv)
    wo = ring(wo_ref, lambda n: wo_full.at[n], "y", wo_ref.shape[0] // 32 * 16, wo_send, wo_recv)

    def put(src, dst, send, recv, n, to):
        return pltpu.make_async_remote_copy(
            src_ref=src, dst_ref=dst, send_sem=send.at[n], recv_sem=recv.at[n], device_id=to, device_id_type=MESH)

    before, after, far = (y + side - 1) % side, (y + 1) % side, (y + 2) % side

    def xs_copy(n):
        part = (xv.at[y], xv.at[y], xv.at[before, top], xv.at[after, low])[n]
        return put(part, part, xs_send, xs_recv, n, down if n % 2 else up)

    def xw_copy(n):
        src = (xv.at[y], xv.at[y], wide_ref.at[3, top], wide_ref.at[1, low])[n]
        dst = (wide_ref.at[3], wide_ref.at[1], wide_ref.at[2, top], wide_ref.at[2, low])[n]
        return put(src, dst, xw_send, xw_recv, n, left if n % 2 else right)

    def o_copy(step):
        to = (col_me + 1 + step) % groups
        return put(qk.at[step, pl.ds(0, hd)], oin_ref.at[col_me], o_send, o_recv, step, {"y": to // cores, "core": to % cores})

    def head_of(n):
        return (x + n // cores) % side * cores + (core + n) % cores

    qk_rows, v_rows = pl.ds(0, 2 * hd), pl.ds(2 * hd, hd)

    def cols(part):
        return pl.ds(pl.multiple_of(part * rows, rows), rows)

    def home(n, kind, at):
        head = head_of(n)
        return put(qk.at[head, (qk_rows, v_rows)[kind], at], qkv.at[row_me, (qk_rows, v_rows)[kind], at],
                   a_send.at[kind], a_recv.at[kind], n, {"x": head // cores, "core": head % cores})

    own_x = pltpu.make_async_copy(x_ref, xv.at[y], local.at[0])
    own_wq = pltpu.make_async_copy(wq_ref, wv.at[row_me], local.at[1])
    own_x.start()
    own_wq.start()

    def project(xt):
        def norm(r, c):
            at = pl.ds(pl.multiple_of(r * 32, 32), 32)
            row = xv[y, at, :].astype(F32)
            mean = jnp.mean(row, axis=-1, keepdims=True)
            centered = row - mean
            var = jnp.mean(centered * centered, axis=-1, keepdims=True)
            xv[y, at, :] = (centered * lax.rsqrt(var + LN_EPS) * gain_ref[...].reshape(1, model)).astype(BF)
            return c

        def flip(part):
            def piece(k, c):
                at = pl.ds(pl.multiple_of(k * 256, 256), 256)
                xt[at, cols(part)] = xv[part, :, at].T
                return c

            lax.fori_loop(0, model // 256, piece, 0, unroll=2)

        def work(count, pick, parts, go=True):
            def body(k, c):
                n = pick(k)
                for part in parts:
                    qk[head_of(n), :, cols(part)] = jnp.dot(
                        wv[head_of(n)], xt[:, cols(part)], preferred_element_type=F32).astype(BF)
                if go:
                    for part in parts:
                        home(n, 0, cols(part)).start()
                return c

            lax.fori_loop(0, count, body, 0)

        close = lambda k: cores * (1 + 2 * (k // cores)) + k % cores
        distant = lambda k: 2 * cores + k
        here = lambda k: k

        own_x.wait()
        lax.fori_loop(0, rows // 32, norm, 0)
        flip(y)
        met()
        start(wq, 0, 1, 2)
        xs_copy(0).start()
        xs_copy(1).start()
        start(w1, 2)
        keep = pltpu.make_async_copy(xv.at[y], wide_ref.at[0], local.at[2])
        keep.start()
        arrived(wq, 0, 1)
        start(wq, 3, 4, 5, 6)
        xs_copy(0).wait_recv()
        xs_copy(1).wait_recv()
        xs_copy(2).start()
        xs_copy(3).start()
        start(w1, 0, 1)
        flip(before)
        flip(after)
        own_wq.wait()
        arrived(wq, 2, 5, 6)
        work(2 * cores, close, (y, after, before))
        arrived(wq, 3, 4)
        start(wq, 7)
        work(cores, here, (y, after, before), go=False)
        arrived(wq, 7)
        work(cores, distant, (y, after, before))
        xs_copy(2).wait_recv()
        xs_copy(3).wait_recv()
        flip(far)
        work(cores, distant, (far,))
        work(2 * cores, close, (far,))
        work(cores, here, (far,), go=False)
        everything = pl.ds(0, toks)
        for n in range(1, cores):
            home(n, 0, everything).start()
            home(n, 1, everything).start()
        for k in range(cores):
            home(distant(k), 1, everything).start()
        for k in range(2 * cores):
            home(close(k), 1, everything).start()
        qkv[row_me] = qk[row_me]
        keep.wait()
        for n in range(4):
            xs_copy(n).wait_send()
        for copy in wq:
            copy.wait_send()

    pl.run_scoped(project, pltpu.VMEM((model, toks), BF))
    arrived(w1, 0, 1)
    start(w1, 3, 4, 5, 6)
    start(wo, 0, 1, 2)
    start(w2, 0, 1, 2)
    xw_copy(0).start()
    xw_copy(1).start()
    everything = pl.ds(0, toks)

    def attend(kaug, s_a, s_b):
        def load_query(b, slot):
            b = jnp.minimum(b, 2 * groups - 1)
            dest, part = (col_me + 1 + b // 2) % groups, b % 2
            for j in range(subs):
                g = (part * subs + j) * cores + dest % cores
                qt = qkv[g, 0:hd, cols(dest // cores)].astype(F32) * scale
                hi = qt.astype(BF)
                rest = qt - hi.astype(F32)
                mid = rest.astype(BF)
                at = slice(j * rows, (j + 1) * rows)
                qaug[slot, 0:hd, at] = hi
                qaug[slot, hd:2 * hd, at] = mid
                qaug[slot, 2 * hd:3 * hd, at] = (rest - mid.astype(F32)).astype(BF)

        def fold(piece, op):
            return op(piece.reshape(piece.shape[0] // 8, 8, bq), axis=0)

        def spread(t, c):
            g = t * TK // toks
            t0 = pl.multiple_of(t * TK - g * toks, TK)
            kt = qkv[g, hd:2 * hd, pl.ds(t0, TK)]
            kaug[pl.ds(pl.multiple_of(t * TK, TK), TK), :] = jnp.concatenate([kt, kt, kt, jnp.zeros((pad, TK), BF)], axis=0).T
            return c

        def first(c, m8):
            at = pl.ds(pl.multiple_of(c * 8 * TK, 8 * TK), 8 * TK)
            s = jnp.dot(kaug[at, :], qaug[0], preferred_element_type=F32)
            s_a[at, :] = s
            return jnp.maximum(m8, fold(s, jnp.max))

        def half(i, s_in, s_out, slot, col):
            m = m_ref[0:1, :]
            acc_ref[...] = jnp.zeros_like(acc_ref)

            def trip(c, carry):
                m8, l8 = carry
                k0 = pl.multiple_of(c * chunk, chunk)
                total = None
                for u in range(chunk // TK):
                    s_new = jnp.dot(kaug[pl.ds(k0 + u * TK, TK), :], qaug[slot], preferred_element_type=F32)
                    ps = []
                    for r in range(0, TK, ROWS):
                        p = jnp.exp2(s_in[pl.ds(k0 + u * TK + r, ROWS), :] - m)
                        l8 = l8 + fold(p, jnp.sum)
                        ps.append(p.astype(BF))
                    at = u * TK % toks
                    vt = qkv[k0 // toks + u * TK // toks, 2 * hd:3 * hd, at:at + TK]
                    d = jnp.dot(vt, jnp.concatenate(ps, axis=0), preferred_element_type=F32)
                    total = d if total is None else total + d
                    for r in range(0, TK, ROWS):
                        piece = s_new[r:r + ROWS]
                        m8 = jnp.maximum(m8, fold(piece, jnp.max))
                        s_out[pl.ds(k0 + u * TK + r, ROWS), :] = piece
                acc_ref[...] += total
                return m8, l8

            m8, l8 = lax.fori_loop(0, (1 + x // side) * (keys // chunk), trip,
                                   (jnp.full((8, bq), -jnp.inf, F32), jnp.zeros((8, bq), F32)))
            qk[i, 0:hd, col:col + bq] = (acc_ref[...] / jnp.sum(l8, axis=0, keepdims=True)).astype(BF)
            m_ref[...] = jnp.broadcast_to(jnp.max(m8, axis=0, keepdims=True), (8, bq))

        for n in range(1, groups):
            home(n, 0, everything).wait()
        lax.fori_loop(0, keys // TK, spread, 0, unroll=4)
        qaug[:, 3 * hd:, :] = jnp.zeros((2, pad, bq), BF)
        load_query(0, 0)
        load_query(1, 1)
        m8 = lax.fori_loop(0, keys // (8 * TK), first, jnp.full((8, bq), -jnp.inf, F32))
        m_ref[...] = jnp.broadcast_to(jnp.max(m8, axis=0, keepdims=True), (8, bq))
        for n in range(1, groups):
            home(n, 1, everything).wait()

        def step(i, c):
            @pl.when(i == groups // 2)
            def _():
                xw_copy(0).wait()
                xw_copy(1).wait()
                xw_copy(2).start()
                xw_copy(3).start()
                arrived(w1, 3, 4)
                start(w1, 7)
                for copies in (wo, w2):
                    arrived(copies, 0, 1)
                    start(copies, 3, 4, 5, 6)

            @pl.when(i == groups - 1)
            def _():
                for copies in (wo, w2):
                    arrived(copies, 3, 4)
                    start(copies, 7)

            half(i, s_a, s_b, 1, 0)
            load_query(2 * i + 2, 0)
            half(i, s_b, s_a, 0, bq)
            load_query(2 * i + 3, 1)

            @pl.when(i < groups - 1)
            def _():
                o_copy(i).start()

            return c

        lax.fori_loop(0, groups, step, 0)

    pl.run_scoped(attend, pltpu.VMEM((keys, depth), BF), pltpu.VMEM((keys, bq), F32), pltpu.VMEM((keys, bq), F32))
    own_o = pltpu.make_async_copy(qk.at[groups - 1, pl.ds(0, hd)], oin_ref.at[col_me], local.at[3])
    own_o.start()
    xw_copy(2).wait()
    xw_copy(3).wait()
    for step in range(groups - 1):
        o_copy(step).wait()
    own_o.wait()
    arrived(w1, 2, 5, 6, 7)
    for copies in (wo, w2):
        arrived(copies, 2, 5, 6, 7)
    for copies in (wo, w2, w1):
        for copy in copies:
            copy.wait_send()


def front(x_loc, gain, wq, own, cores, side):
    rows, model = x_loc.shape
    w1, w2, wo = own
    groups, toks = side * cores, side * rows
    hd = wq.shape[0] // 3
    keys, bq = groups * toks, toks // 2
    anywhere = pl.BlockSpec(memory_space=pl.ANY)
    dma = lambda *n: pltpu.SemaphoreType.DMA(n)
    flops = 2 * toks * model * groups * wq.shape[0] + 6 * keys * keys * hd
    return pl.pallas_call(
        functools.partial(front_kernel, side, cores, hd),
        in_specs=[anywhere, pl.BlockSpec(memory_space=pltpu.VMEM)] + [anywhere] * 4,
        out_specs=[anywhere] * 5,
        out_shape=[
            jax.ShapeDtypeStruct((groups, hd, toks), BF),
            jax.ShapeDtypeStruct((side, rows, model), BF),
            jax.ShapeDtypeStruct((groups,) + w1.shape, BF),
            jax.ShapeDtypeStruct((groups, w2.shape[0], first_columns(model)), BF),
            jax.ShapeDtypeStruct((groups,) + wo.shape, BF),
        ],
        scratch_shapes=[
            pltpu.VMEM((groups,) + wq.shape, BF),
            pltpu.VMEM((side, rows, model), BF),
            pltpu.VMEM((groups, 3 * hd, toks), BF),
            pltpu.VMEM((groups, 3 * hd, toks), BF),
            pltpu.VMEM((2, 256, bq), BF),
            pltpu.VMEM((hd, bq), F32),
            pltpu.VMEM((8, bq), F32),
            dma(8), dma(8), dma(4), dma(4), dma(8), dma(8), dma(2, groups), dma(2, groups), dma(groups - 1), dma(groups - 1),
            dma(4), dma(4), dma(8), dma(8), dma(8), dma(8), dma(4),
        ],
        compiler_params=pltpu.CompilerParams(
            vmem_limit_bytes=67043328, collective_id=0, has_side_effects=True),
        cost_estimate=pl.CostEstimate(flops=flops, bytes_accessed=4 * w1.size, transcendentals=keys * keys),
        name="front",
    )(x_loc, gain, wq, w1, w2, wo)


def first_columns(model):
    return model * 2 // 5 // 256 * 256


def mlp_kernel(side, cores, wide_ref, oin_ref, w1_own, w2_own, wo_own, w1_ref, w2_ref, wo_ref, res_ref, y_ref, w1, w2, xv, xt, ov,
               hv, part, far, near, res, load, w1_sem, send, recv, w2_send, w2_recv):
    x, y = lax.axis_index("x"), lax.axis_index("y")
    right, left = {"x": (x + 1) % side}, {"x": (x + side - 1) % side}
    _, rows, model = wide_ref.shape
    groups = w1_ref.shape[0]
    width = groups * w1_own.shape[0]
    heads = groups * wo_own.shape[0]
    cut = w2_ref.shape[2]
    step = math.gcd(cut, model - cut, 512)
    half = rows // 2
    me = y * cores + lax.axis_index("core")
    top, low = pl.ds(0, half), pl.ds(half, half)
    order = (2, 1, 3, 0)

    def x_load(n):
        return pltpu.make_async_copy(wide_ref.at[order[n]], xv.at[n % 2], load.at[n % 2])

    def shard(into, base, size, n, columns):
        return into.at[pl.ds(pl.multiple_of(base + n * size, 16), size), columns]

    def gathered(own, full, into, base, sem):
        size, columns = full.shape[1], pl.ds(0, full.shape[2])
        for hop in range(groups):
            n = (me + hop) % groups
            pltpu.make_async_copy(full.at[n] if hop else own.at[:, columns], shard(into, base, size, n, columns), sem).start()
        whole = into.at[pl.ds(base, groups * size), columns]
        return pltpu.make_async_copy(whole, whole, sem)

    o_load = pltpu.make_async_copy(oin_ref, ov, load.at[2])
    res_load = pltpu.make_async_copy(res_ref, res, load.at[3])
    rest = pl.ds(cut, model - cut)
    rest_own = pltpu.make_async_copy(w2_own.at[:, rest], shard(w2, 0, width // groups, me, rest), load.at[7])
    x_load(0).start()
    pair = 2 * w1_own.shape[0]

    def w1_shard(n):
        to = shard(w1, 0, pair // 2, n, pl.ds(0, model))

        @pl.when(n == me)
        def _():
            pltpu.make_async_copy(w1_own, to, w1_sem.at[n // 2]).start()

        @pl.when(n != me)
        def _():
            pltpu.make_async_copy(w1_ref.at[n], to, w1_sem.at[n // 2]).start()

    for n in range(groups):
        w1_shard(n)
    o_load.start()
    w2_load = gathered(w2_own, w2_ref, w2, 0, load.at[5])
    wo_load = gathered(wo_own, wo_ref, w2, width, load.at[6])
    rest_own.start()
    x_load(1).start()
    res_load.start()
    met = hail(right, left, {"y": (y + 1) % side}, {"y": (y + side - 1) % side}, {"core": (lax.axis_index("core") + 1) % cores})
    w2_rest = ring(w2_own.at[:, rest], lambda n: shard(w2, 0, width // groups, n, rest), "y", width // groups // 2, w2_send, w2_recv)

    def hidden(n):
        x_load(n).wait()

        def flip(k, c):
            at = pl.ds(pl.multiple_of(k * 256, 256), 256)
            xt[at, :] = xv[n % 2, :, at].T
            return c

        lax.fori_loop(0, model // 256, flip, 0, unroll=2)
        if n < 2:
            x_load(n + 2).start()
        col = pl.multiple_of((x + order[n]) % side * rows, rows)
        if n == 0:
            o_load.wait()
        hv[n, :, width:] = ov[:, :, pl.ds(col, rows)].reshape(heads, rows).T
        if n == 0:
            met()
            start(w2_rest, 0, 1, 2)

        def piece(f, c):
            at = pl.ds(pl.multiple_of(f * pair, pair), pair)
            if n == 0:
                pltpu.make_async_copy(w1.at[at], w1.at[at], w1_sem.at[f]).wait()
            pre = jnp.dot(w1[at, :], xt[...], preferred_element_type=F32)
            hv[n, :, at] = jax.nn.gelu(pre, approximate=True).astype(BF).T
            return c

        lax.fori_loop(0, groups // 2, piece, 0)

    def outs(n, lo, hi):
        def piece(d, c):
            at = pl.ds(pl.multiple_of(d * step, step), step)
            part[n % 3, :, at] = jnp.dot(hv[n], w2[:, at], preferred_element_type=F32)
            return c

        lax.fori_loop(lo // step, hi // step, piece, 0)

    def phase(lo, hi, first, prepare, between):
        cols = pl.ds(lo, hi - lo)
        plan = (
            (part.at[0, top, cols], far.at[0, :, cols], right),
            (part.at[0, low, cols], far.at[1, :, cols], left),
            (part.at[1, low, cols], near.at[0, low, cols], right),
            (part.at[2, top, cols], near.at[1, top, cols], left),
            (part.at[1, top, cols], near.at[0, top, cols], right),
            (part.at[2, low, cols], near.at[1, low, cols], left),
        )
        puts = [
            pltpu.make_async_remote_copy(src_ref=src, dst_ref=dst, send_sem=send.at[first + n], recv_sem=recv.at[first + n],
                                         device_id=to, device_id_type=MESH)
            for n, (src, dst, to) in enumerate(plan)
        ]
        prepare(0)
        outs(0, lo, hi)
        start(puts, 0, 1)
        prepare(1)
        outs(1, lo, hi)
        start(puts, 2)
        prepare(2)
        outs(2, lo, hi)
        start(puts, 3)
        between()
        puts[0].wait()
        part[1, :half, lo:hi] += far[0, :, lo:hi]
        start(puts, 4)
        puts[1].wait()
        part[2, half:, lo:hi] += far[1, :, lo:hi]
        start(puts, 5)
        prepare(3)
        outs(3, lo, hi)
        return puts[2:]

    def ready(n):
        hidden(n)
        if n == 0:
            w2_load.wait()
            wo_load.wait()

    def pass_on():
        arrived(w2_rest, 0, 1)
        start(w2_rest, 3, 4, 5, 6)

    waits = phase(0, cut, 0, ready, pass_on)
    arrived(w2_rest, 3, 4)
    start(w2_rest, 7)
    rest_own.wait()
    arrived(w2_rest, 2, 5, 6, 7)
    waits += phase(cut, model, 6, lambda n: None, lambda: None)
    res_load.wait()
    part[0] += res[...].astype(F32)
    for put in waits:
        put.wait()
    for copy in w2_rest:
        copy.wait_send()
    y_ref[...] = (part[0] + near[0] + near[1]).astype(BF)


def mlp(x_loc, wide, oin, own, full, cores, side):
    rows, model = x_loc.shape
    groups = side * cores
    width, heads = groups * own[0].shape[0], groups * own[2].shape[0]
    anywhere = pl.BlockSpec(memory_space=pl.ANY)
    flops = 2 * side * rows * model * (2 * width + heads)
    return pl.pallas_call(
        functools.partial(mlp_kernel, side, cores),
        in_specs=[anywhere] * 9,
        out_specs=pl.BlockSpec(memory_space=pltpu.VMEM),
        out_shape=jax.ShapeDtypeStruct((rows, model), BF),
        scratch_shapes=[
            pltpu.VMEM((width, model), BF),
            pltpu.VMEM((width + heads, model), BF),
            pltpu.VMEM((2, rows, model), BF),
            pltpu.VMEM((model, rows), BF),
            pltpu.VMEM(oin.shape, BF),
            pltpu.VMEM((side, rows, width + heads), BF),
            pltpu.VMEM((3, rows, model), F32),
            pltpu.VMEM((2, rows // 2, model), F32),
            pltpu.VMEM((2, rows, model), F32),
            pltpu.VMEM((rows, model), BF),
            pltpu.SemaphoreType.DMA((8,)),
            pltpu.SemaphoreType.DMA((groups // 2,)),
            pltpu.SemaphoreType.DMA((12,)),
            pltpu.SemaphoreType.DMA((12,)),
            pltpu.SemaphoreType.DMA((8,)),
            pltpu.SemaphoreType.DMA((8,)),
        ],
        compiler_params=pltpu.CompilerParams(vmem_limit_bytes=67043328, collective_id=1, has_side_effects=True),
        cost_estimate=pl.CostEstimate(flops=flops, bytes_accessed=4 * model * width, transcendentals=side * rows * width),
        name="mlp",
    )(wide, oin, *own, *full, x_loc)


def solution(mesh):
    data, tp = mesh.devices.shape
    side = math.isqrt(tp // 2)
    cores = tp // (side * side)
    grid = Mesh(mesh.devices.reshape(data, side, side, cores), ("data", "y", "x", "core"))

    def local_block(x_loc, ln_gamma, w_qkv, w_out, w_up, w_down):
        own = (w_up.T, w_down, w_out[0])
        oin, wide, w1, w2, wo = front(x_loc, ln_gamma, w_qkv[:, 0, :].T, own, cores, side)
        return mlp(x_loc, wide, oin, own, (w1, w2, wo), cores, side)

    row_spec = P(("data", "y", "x", "core"), None)
    tp_axes = ("y", "x", "core")
    return jax.shard_map(
        local_block,
        mesh=grid,
        in_specs=(row_spec, P(None), P(None, tp_axes, None), P(tp_axes, None, None), P(None, tp_axes), P(tp_axes, None)),
        out_specs=row_spec,
        check_vma=False,
    )
```

```python
import functools
import math
import jax
import jax.numpy as jnp
from jax import lax
from jax.experimental import pallas as pl
from jax.experimental.pallas import tpu as pltpu
from jax.sharding import Mesh, PartitionSpec as P

LN_EPS = 1e-6
BF = jnp.bfloat16
MESH = pl.DeviceIdType.MESH
F32 = jnp.float32
TK = 256
TRIP = 32
ROWS = 64


def ring(own, slot, axis, split, send, recv):
    side, cores = lax.axis_size(axis), lax.axis_size("core")
    at, core = lax.axis_index(axis), lax.axis_index("core")
    other = (core + 1) % cores
    block = lambda hop: slot((at + hop) % side * cores + core)
    head, tail = pl.ds(0, split), pl.ds(split, own.shape[0] - split)
    nxt, prv, sib = {axis: (at + 1) % side}, {axis: (at + side - 1) % side}, {"core": other}
    plan = (
        (own, block(0), nxt),
        (own, block(0), prv),
        (own, block(0), sib),
        (block(side - 1).at[head], block(side - 1).at[head], nxt),
        (block(1).at[tail], block(1).at[tail], prv),
        (block(side - 1), block(side - 1), sib),
        (block(1), block(1), sib),
        (block(2), block(2), sib),
    )
    return [
        pltpu.make_async_remote_copy(
            src_ref=src, dst_ref=dst, send_sem=send.at[n], recv_sem=recv.at[n], device_id=to, device_id_type=MESH)
        for n, (src, dst, to) in enumerate(plan)
    ]


def start(copies, *which):
    for n in which:
        copies[n].start()


def arrived(copies, *which):
    for n in which:
        copies[n].wait_recv()


def hail(*places):
    barrier = pltpu.get_barrier_semaphore()
    for place in places:
        pl.semaphore_signal(barrier, inc=1, device_id=place, device_id_type=MESH)
    return lambda: pl.semaphore_wait(barrier, len(places))


def front_kernel(side, cores, hd, x_ref, gain_ref, wq_ref, w1_ref, w2_ref, wo_ref, oin_ref, wide_ref, w1_full, w2_full, wo_full, qkv_ref,
                 wv, xv, qk, qkv, qaug, acc_ref, m_ref, wq_send, wq_recv, xs_send, xs_recv, w1_send, w1_recv, a_send, a_recv, o_send, o_recv,
                 xw_send, xw_recv, w2_send, w2_recv, wo_send, wo_recv, local):
    y, x, core = lax.axis_index("y"), lax.axis_index("x"), lax.axis_index("core")
    rows, model = x_ref.shape
    groups, toks = side * cores, side * rows
    keys = groups * toks
    bq = toks // 2
    subs = bq // rows
    scale = hd ** -0.5 * math.log2(math.e)
    depth = qaug.shape[1]
    pad = depth - 3 * hd
    chunk = min(TRIP * TK, keys)
    row_me, col_me = x * cores + core, y * cores + core
    up, down = {"y": (y + 1) % side}, {"y": (y + side - 1) % side}
    right, left = {"x": (x + 1) % side}, {"x": (x + side - 1) % side}
    top, low = pl.ds(0, rows // 2), pl.ds(rows // 2, rows // 2)
    apart = [(d, dc) for d in range(side) for dc in range(cores) if d or dc]
    met = hail(
        *[{"x": (x + d) % side, "core": (core + dc) % cores} for d, dc in apart],
        *[{"y": (y + d) % side, "core": (core + dc) % cores} for d, dc in apart if d])

    wq = ring(wq_ref, lambda n: wv.at[n], "x", wq_ref.shape[0] // 32 * 16, wq_send, wq_recv)
    w1 = ring(w1_ref, lambda n: w1_full.at[n], "y", w1_ref.shape[0] // 2, w1_send, w1_recv)
    w2 = ring(w2_ref.at[:, pl.ds(0, w2_full.shape[2])], lambda n: w2_full.at[n], "y", w2_ref.shape[0] // 2, w2_send, w2_recv)
    wo = ring(wo_ref, lambda n: wo_full.at[n], "y", wo_ref.shape[0] // 32 * 16, wo_send, wo_recv)

    def put(src, dst, send, recv, n, to):
        return pltpu.make_async_remote_copy(
            src_ref=src, dst_ref=dst, send_sem=send.at[n], recv_sem=recv.at[n], device_id=to, device_id_type=MESH)

    before, after, far = (y + side - 1) % side, (y + 1) % side, (y + 2) % side

    def xs_copy(n):
        part = (xv.at[y], xv.at[y], xv.at[before, top], xv.at[after, low])[n]
        return put(part, part, xs_send, xs_recv, n, down if n % 2 else up)

    def xw_copy(n):
        src = (xv.at[y], xv.at[y], wide_ref.at[3, top], wide_ref.at[1, low])[n]
        dst = (wide_ref.at[3], wide_ref.at[1], wide_ref.at[2, top], wide_ref.at[2, low])[n]
        return put(src, dst, xw_send, xw_recv, n, left if n % 2 else right)

    hops = side - 1

    def place(p):
        return (col_me + 1 + p // hops) % groups, (x + 1 + (p % hops + 1) % hops) % side

    def o_block(p):
        return qk.at[p // 4, pl.ds(0, hd), pl.ds(pl.multiple_of(p % 4 * rows, rows), rows)], oin_ref.at[col_me, :, cols(place(p)[1])]

    def o_copy(p):
        to = place(p)[0]
        return put(*o_block(p), o_send, o_recv, p, {"y": to // cores, "core": to % cores})

    def o_keep(p):
        return pltpu.make_async_copy(*o_block(p), local.at[3])

    def head_of(n):
        return (x + n // cores) % side * cores + (core + n) % cores

    qk_rows, v_rows = pl.ds(0, 2 * hd), pl.ds(2 * hd, hd)

    def cols(part):
        return pl.ds(pl.multiple_of(part * rows, rows), rows)

    def home(n, kind, at):
        head = head_of(n)
        return put(qk.at[head, (qk_rows, v_rows)[kind], at], qkv.at[row_me, (qk_rows, v_rows)[kind], at],
                   a_send.at[kind], a_recv.at[kind], n, {"x": head // cores, "core": head % cores})

    own_x = pltpu.make_async_copy(x_ref, xv.at[y], local.at[0])
    own_wq = pltpu.make_async_copy(wq_ref, wv.at[row_me], local.at[1])
    own_x.start()
    own_wq.start()

    def project(xt):
        def norm(r, c):
            at = pl.ds(pl.multiple_of(r * 32, 32), 32)
            row = xv[y, at, :].astype(F32)
            mean = jnp.mean(row, axis=-1, keepdims=True)
            centered = row - mean
            var = jnp.mean(centered * centered, axis=-1, keepdims=True)
            xv[y, at, :] = (centered * lax.rsqrt(var + LN_EPS) * gain_ref[...].reshape(1, model)).astype(BF)
            return c

        def flip(part):
            def piece(k, c):
                at = pl.ds(pl.multiple_of(k * 256, 256), 256)
                xt[at, cols(part)] = xv[part, :, at].T
                return c

            lax.fori_loop(0, model // 256, piece, 0, unroll=2)

        def work(count, pick, parts, go=True):
            def body(k, c):
                n = pick(k)
                for part in parts:
                    qk[head_of(n), :, cols(part)] = jnp.dot(
                        wv[head_of(n)], xt[:, cols(part)], preferred_element_type=F32).astype(BF)
                if go:
                    for part in parts:
                        home(n, 0, cols(part)).start()
                return c

            lax.fori_loop(0, count, body, 0)

        close = lambda k: cores * (1 + 2 * (k // cores)) + k % cores
        distant = lambda k: 2 * cores + k
        here = lambda k: k

        own_x.wait()
        lax.fori_loop(0, rows // 32, norm, 0)
        flip(y)
        met()
        start(wq, 0, 1, 2)
        xs_copy(0).start()
        xs_copy(1).start()
        start(w1, 2)
        keep = pltpu.make_async_copy(xv.at[y], wide_ref.at[0], local.at[2])
        keep.start()
        arrived(wq, 0, 1)
        start(wq, 3, 4, 5, 6)
        xs_copy(0).wait_recv()
        xs_copy(1).wait_recv()
        xs_copy(2).start()
        xs_copy(3).start()
        start(w1, 0, 1)
        flip(before)
        flip(after)
        own_wq.wait()
        arrived(wq, 2, 5, 6)
        work(2 * cores, close, (y, after, before))
        arrived(wq, 3, 4)
        start(wq, 7)
        work(cores, here, (y, after, before), go=False)
        arrived(wq, 7)
        work(cores, distant, (y, after, before))
        xs_copy(2).wait_recv()
        xs_copy(3).wait_recv()
        flip(far)
        work(cores, distant, (far,))
        work(2 * cores, close, (far,))
        work(cores, here, (far,), go=False)
        everything = pl.ds(0, toks)
        for n in range(1, cores):
            home(n, 0, everything).start()
            home(n, 1, everything).start()
        for k in range(cores):
            home(distant(k), 1, everything).start()
        for k in range(2 * cores):
            home(close(k), 1, everything).start()
        qkv[row_me] = qk[row_me]
        keep.wait()
        for n in range(4):
            xs_copy(n).wait_send()
        for copy in wq:
            copy.wait_send()

    pl.run_scoped(project, pltpu.VMEM((model, toks), BF))
    arrived(w1, 0, 1)
    start(w1, 3, 4, 5, 6)
    start(wo, 0, 1, 2)
    start(w2, 0, 1, 2)
    xw_copy(0).start()
    xw_copy(1).start()
    everything = pl.ds(0, toks)
    kept_qkv = pltpu.make_async_copy(qkv, qkv_ref, local.at[4])

    def attend(kaug, s_a, s_b):
        def load_query(b, slot):
            b = jnp.minimum(b, hops * groups // subs - 1)
            for j in range(subs):
                dest, column = place(b * subs + j)
                g = column * cores + dest % cores
                qt = qkv[g, 0:hd, cols(dest // cores)].astype(F32) * scale
                hi = qt.astype(BF)
                rest = qt - hi.astype(F32)
                mid = rest.astype(BF)
                at = slice(j * rows, (j + 1) * rows)
                qaug[slot, 0:hd, at] = hi
                qaug[slot, hd:2 * hd, at] = mid
                qaug[slot, 2 * hd:3 * hd, at] = (rest - mid.astype(F32)).astype(BF)

        def fold(piece, op):
            return op(piece.reshape(piece.shape[0] // 8, 8, bq), axis=0)

        def spread(t, c):
            g = t * TK // toks
            t0 = pl.multiple_of(t * TK - g * toks, TK)
            kt = qkv[g, hd:2 * hd, pl.ds(t0, TK)]
            kaug[pl.ds(pl.multiple_of(t * TK, TK), TK), :] = jnp.concatenate([kt, kt, kt, jnp.zeros((pad, TK), BF)], axis=0).T
            return c

        def first(c, m8):
            at = pl.ds(pl.multiple_of(c * 8 * TK, 8 * TK), 8 * TK)
            s = jnp.dot(kaug[at, :], qaug[0], preferred_element_type=F32)
            s_a[at, :] = s
            return jnp.maximum(m8, fold(s, jnp.max))

        def half(i, s_in, s_out, slot, col):
            m = m_ref[0:1, :]
            acc_ref[...] = jnp.zeros_like(acc_ref)

            def trip(c, carry):
                m8, l8 = carry
                k0 = pl.multiple_of(c * chunk, chunk)
                total = None
                for u in range(chunk // TK):
                    s_new = jnp.dot(kaug[pl.ds(k0 + u * TK, TK), :], qaug[slot], preferred_element_type=F32)
                    ps = []
                    for r in range(0, TK, ROWS):
                        p = jnp.exp2(s_in[pl.ds(k0 + u * TK + r, ROWS), :] - m)
                        l8 = l8 + fold(p, jnp.sum)
                        ps.append(p.astype(BF))
                    at = u * TK % toks
                    vt = qkv[k0 // toks + u * TK // toks, 2 * hd:3 * hd, at:at + TK]
                    d = jnp.dot(vt, jnp.concatenate(ps, axis=0), preferred_element_type=F32)
                    total = d if total is None else total + d
                    for r in range(0, TK, ROWS):
                        piece = s_new[r:r + ROWS]
                        m8 = jnp.maximum(m8, fold(piece, jnp.max))
                        s_out[pl.ds(k0 + u * TK + r, ROWS), :] = piece
                acc_ref[...] += total
                return m8, l8

            m8, l8 = lax.fori_loop(0, (1 + x // side) * (keys // chunk), trip,
                                   (jnp.full((8, bq), -jnp.inf, F32), jnp.zeros((8, bq), F32)))
            qk[i, 0:hd, col:col + bq] = (acc_ref[...] / jnp.sum(l8, axis=0, keepdims=True)).astype(BF)
            m_ref[...] = jnp.broadcast_to(jnp.max(m8, axis=0, keepdims=True), (8, bq))

        for n in range(1, groups):
            home(n, 0, everything).wait()
        lax.fori_loop(0, keys // TK, spread, 0, unroll=4)
        qaug[:, 3 * hd:, :] = jnp.zeros((2, pad, bq), BF)
        load_query(0, 0)
        load_query(1, 1)
        m8 = lax.fori_loop(0, keys // (8 * TK), first, jnp.full((8, bq), -jnp.inf, F32))
        m_ref[...] = jnp.broadcast_to(jnp.max(m8, axis=0, keepdims=True), (8, bq))
        for n in range(1, groups):
            home(n, 1, everything).wait()
        kept_qkv.start()
        steps = hops * groups // 4

        def step(i, c):
            @pl.when(i == steps // 2)
            def _():
                xw_copy(0).wait()
                xw_copy(1).wait()
                xw_copy(2).start()
                xw_copy(3).start()
                arrived(w1, 3, 4)
                start(w1, 7)
                for copies in (wo, w2):
                    arrived(copies, 0, 1)
                    start(copies, 3, 4, 5, 6)

            half(i, s_a, s_b, 1, 0)
            load_query(2 * i + 2, 0)

            @pl.when(i == steps - 1)
            def _():
                for copies in (wo, w2):
                    arrived(copies, 3, 4)
                    start(copies, 7)

            half(i, s_b, s_a, 0, bq)
            load_query(2 * i + 3, 1)

            def leave(j, c):
                p = 4 * i + j

                @pl.when(p < hops * (groups - 1))
                def _():
                    o_copy(p).start()

                @pl.when(p >= hops * (groups - 1))
                def _():
                    o_keep(p).start()

                return c

            return lax.fori_loop(0, 4, leave, c)

        lax.fori_loop(0, steps, step, 0)

    pl.run_scoped(attend, pltpu.VMEM((keys, depth), BF), pltpu.VMEM((keys, bq), F32), pltpu.VMEM((keys, bq), F32))
    xw_copy(2).wait()
    xw_copy(3).wait()
    for p in range(hops * (groups - 1)):
        o_copy(p).wait()
    all_kept = oin_ref.at[col_me, :, pl.ds(0, hops * rows)]
    pltpu.make_async_copy(all_kept, all_kept, local.at[3]).wait()
    kept_qkv.wait()
    arrived(w1, 2, 5, 6, 7)
    for copies in (wo, w2):
        arrived(copies, 2, 5, 6, 7)
    for copies in (wo, w2, w1):
        for copy in copies:
            copy.wait_send()


def front(x_loc, gain, wq, own, cores, side):
    rows, model = x_loc.shape
    w1, w2, wo = own
    groups, toks = side * cores, side * rows
    hd = wq.shape[0] // 3
    keys, bq = groups * toks, toks // 2
    anywhere = pl.BlockSpec(memory_space=pl.ANY)
    dma = lambda *n: pltpu.SemaphoreType.DMA(n)
    flops = 2 * toks * model * groups * wq.shape[0] + 6 * keys * keys * hd
    return pl.pallas_call(
        functools.partial(front_kernel, side, cores, hd),
        in_specs=[anywhere, pl.BlockSpec(memory_space=pltpu.VMEM)] + [anywhere] * 4,
        out_specs=[anywhere] * 6,
        out_shape=[
            jax.ShapeDtypeStruct((groups, hd, toks), BF),
            jax.ShapeDtypeStruct((side, rows, model), BF),
            jax.ShapeDtypeStruct((groups,) + w1.shape, BF),
            jax.ShapeDtypeStruct((groups, w2.shape[0], first_columns(model)), BF),
            jax.ShapeDtypeStruct((groups,) + wo.shape, BF),
            jax.ShapeDtypeStruct((groups, 3 * hd, toks), BF),
        ],
        scratch_shapes=[
            pltpu.VMEM((groups,) + wq.shape, BF),
            pltpu.VMEM((side, rows, model), BF),
            pltpu.VMEM((groups, 3 * hd, toks), BF),
            pltpu.VMEM((groups, 3 * hd, toks), BF),
            pltpu.VMEM((2, 256, bq), BF),
            pltpu.VMEM((hd, bq), F32),
            pltpu.VMEM((8, bq), F32),
            dma(8), dma(8), dma(4), dma(4), dma(8), dma(8), dma(2, groups), dma(2, groups),
            dma((side - 1) * (groups - 1)), dma((side - 1) * (groups - 1)), dma(4), dma(4), dma(8), dma(8), dma(8), dma(8), dma(5),
        ],
        compiler_params=pltpu.CompilerParams(
            vmem_limit_bytes=67043328, collective_id=0, has_side_effects=True),
        cost_estimate=pl.CostEstimate(flops=flops, bytes_accessed=4 * w1.size, transcendentals=keys * keys),
        name="front",
    )(x_loc, gain, wq, w1, w2, wo)


def first_columns(model):
    return model * 2 // 5 // 256 * 256


def mlp_kernel(side, cores, wide_ref, oin_ref, qkv_ref, w1_own, w2_own, wo_own, w1_ref, w2_ref, wo_ref, res_ref, y_ref, w2, ov, oo, made, hv,
               part, far, near, res, load, w1_sem, send, recv, w2_send, w2_recv, o_send, o_recv):
    x, y, core = lax.axis_index("x"), lax.axis_index("y"), lax.axis_index("core")
    right, left = {"x": (x + 1) % side}, {"x": (x + side - 1) % side}
    _, rows, model = wide_ref.shape
    groups, hd, toks = oin_ref.shape
    width = groups * w1_own.shape[0]
    heads = groups * hd
    keys = groups * toks
    cut = w2_ref.shape[2]
    step = math.gcd(cut, model - cut, 512)
    half = rows // 2
    me = y * cores + core
    top, low = pl.ds(0, half), pl.ds(half, half)
    order = (2, 1, 3, 0)
    pair = 2 * w1_own.shape[0]
    met = hail(right, left, *[
        {"y": (me + hop) % groups // cores, "core": (me + hop) % cores} for hop in range(1, groups)])

    def shard(into, base, size, n, columns):
        return into.at[pl.ds(pl.multiple_of(base + n * size, 16), size), columns]

    def gathered(own, full, into, base, sem):
        size, columns = full.shape[1], pl.ds(0, full.shape[2])
        for hop in range(groups):
            n = (me + hop) % groups
            pltpu.make_async_copy(full.at[n] if hop else own.at[:, columns], shard(into, base, size, n, columns), sem).start()
        whole = into.at[pl.ds(base, groups * size), columns]
        return pltpu.make_async_copy(whole, whole, sem)

    rest = pl.ds(cut, model - cut)
    o_load = pltpu.make_async_copy(oin_ref, ov, load.at[2])
    res_load = pltpu.make_async_copy(res_ref, res, load.at[3])
    rest_own = pltpu.make_async_copy(w2_own.at[:, rest], shard(w2, 0, width // groups, me, rest), load.at[4])
    w2_rest = ring(w2_own.at[:, rest], lambda n: shard(w2, 0, width // groups, n, rest), "y", width // groups // 2, w2_send, w2_recv)

    def outs(n, lo, hi):
        def piece(d, c):
            at = pl.ds(pl.multiple_of(d * step, step), step)
            part[n % 3, :, at] = jnp.dot(hv[n], w2[:, at], preferred_element_type=F32)
            return c

        lax.fori_loop(lo // step, hi // step, piece, 0)

    def plan(lo, hi, first):
        cols = pl.ds(lo, hi - lo)
        copies = (
            (part.at[0, top, cols], far.at[0, :, cols], right),
            (part.at[0, low, cols], far.at[1, :, cols], left),
            (part.at[1, low, cols], near.at[0, low, cols], right),
            (part.at[2, top, cols], near.at[1, top, cols], left),
            (part.at[1, top, cols], near.at[0, top, cols], right),
            (part.at[2, low, cols], near.at[1, low, cols], left),
        )
        return [
            pltpu.make_async_remote_copy(src_ref=src, dst_ref=dst, send_sem=send.at[first + n], recv_sem=recv.at[first + n],
                                         device_id=to, device_id_type=MESH)
            for n, (src, dst, to) in enumerate(copies)
        ]

    def add_far(puts, lo, hi):
        puts[0].wait()
        part[1, :half, lo:hi] += far[0, :, lo:hi]
        start(puts, 4)
        puts[1].wait()
        part[2, half:, lo:hi] += far[1, :, lo:hi]
        start(puts, 5)

    first, second = plan(0, cut, 0), plan(cut, model, 6)

    def hidden_layer(w1, xv, xt):
        def x_load(n):
            return pltpu.make_async_copy(wide_ref.at[order[n]], xv.at[n % 2], load.at[n % 2])

        def w1_shard(n):
            to = shard(w1, 0, pair // 2, n, pl.ds(0, model))

            @pl.when(n == me)
            def _():
                pltpu.make_async_copy(w1_own, to, w1_sem.at[n // 2]).start()

            @pl.when(n != me)
            def _():
                pltpu.make_async_copy(w1_ref.at[n], to, w1_sem.at[n // 2]).start()

        x_load(0).start()
        for n in range(groups):
            w1_shard(n)
        o_load.start()
        w2_load = gathered(w2_own, w2_ref, w2, 0, load.at[5])
        wo_load = gathered(wo_own, wo_ref, w2, width, load.at[6])
        rest_own.start()
        x_load(1).start()
        res_load.start()

        def hidden(n):
            x_load(n).wait()

            def flip(k, c):
                at = pl.ds(pl.multiple_of(k * 256, 256), 256)
                xt[at, :] = xv[n % 2, :, at].T
                return c

            lax.fori_loop(0, model // 256, flip, 0, unroll=2)
            if n < 2:
                x_load(n + 2).start()
            if n == 0:
                o_load.wait()
            if n < 3:
                col = pl.multiple_of((x + order[n]) % side * rows, rows)
                hv[n, :, width:] = ov[:, :, pl.ds(col, rows)].reshape(heads, rows).T
            if n == 0:
                met()
                start(w2_rest, 0, 1, 2)

            def piece(f, c):
                at = pl.ds(pl.multiple_of(f * pair, pair), pair)
                if n == 0:
                    pltpu.make_async_copy(w1.at[at], w1.at[at], w1_sem.at[f]).wait()
                pre = jnp.dot(w1[at, :], xt[...], preferred_element_type=F32)
                hv[n, :, at] = jax.nn.gelu(pre, approximate=True).astype(BF).T
                return c

            lax.fori_loop(0, groups // 2, piece, 0)

        hidden(0)
        w2_load.wait()
        wo_load.wait()
        outs(0, 0, cut)
        start(first, 0, 1)
        hidden(1)
        outs(1, 0, cut)
        start(first, 2)
        hidden(2)
        outs(2, 0, cut)
        start(first, 3)
        arrived(w2_rest, 0, 1)
        start(w2_rest, 3, 4, 5, 6)
        add_far(first, 0, cut)
        hidden(3)

    pl.run_scoped(hidden_layer, pltpu.VMEM((width, model), BF), pltpu.VMEM((2, rows, model), BF), pltpu.VMEM((model, rows), BF))

    def o_copy(k):
        to = (me + 1 + k) % groups
        return pltpu.make_async_remote_copy(
            src_ref=made.at[k], dst_ref=oo.at[me], send_sem=o_send.at[k], recv_sem=o_recv.at[k],
            device_id={"y": to // cores, "core": to % cores}, device_id_type=MESH)

    def own_rows(qkv, kaug, qaug, scores):
        depth = kaug.shape[1]
        scale = hd ** -0.5 * math.log2(math.e)
        fetch = pltpu.make_async_copy(qkv_ref, qkv, load.at[7])
        fetch.start()
        fetch.wait()
        pad = jnp.zeros((depth - 3 * hd, TK), BF)

        def spread(t, c):
            g = t * TK // toks
            kt = qkv[g, hd:2 * hd, pl.ds(pl.multiple_of(t * TK - g * toks, TK), TK)]
            kaug[pl.ds(pl.multiple_of(t * TK, TK), TK), :] = jnp.concatenate([kt, kt, kt, pad], axis=0).T
            return c

        lax.fori_loop(0, keys // TK, spread, 0, unroll=4)
        qaug[3 * hd:, :] = jnp.zeros((depth - 3 * hd, rows), BF)

        def fold(piece, op):
            return op(piece.reshape(piece.shape[0] // 8, 8, rows), axis=0)

        def block(k, c):
            dest = (me + 1 + k) % groups
            qt = qkv[x * cores + dest % cores, 0:hd, pl.ds(pl.multiple_of(dest // cores * rows, rows), rows)].astype(F32) * scale
            hi = qt.astype(BF)
            left_over = qt - hi.astype(F32)
            mid = left_over.astype(BF)
            qaug[0:hd, :] = hi
            qaug[hd:2 * hd, :] = mid
            qaug[2 * hd:3 * hd, :] = (left_over - mid.astype(F32)).astype(BF)

            def score(t, m8):
                at = pl.ds(pl.multiple_of(t * 2 * toks, 2 * toks), 2 * toks)
                s = jnp.dot(kaug[at, :], qaug[...], preferred_element_type=F32)
                scores[at, :] = s
                return jnp.maximum(m8, fold(s, jnp.max))

            m8 = lax.fori_loop(0, groups // 2, score, jnp.full((8, rows), -jnp.inf, F32))
            m = jnp.max(m8, axis=0, keepdims=True)

            def weigh(g, carry):
                l8, acc = carry
                ps = []
                for r in range(0, toks, ROWS):
                    p = jnp.exp2(scores[pl.ds(pl.multiple_of(g * toks, toks) + r, ROWS), :] - m)
                    l8 = l8 + fold(p, jnp.sum)
                    ps.append(p.astype(BF))
                return l8, acc + jnp.dot(qkv[g, 2 * hd:3 * hd, :], jnp.concatenate(ps, axis=0), preferred_element_type=F32)

            l8, acc = lax.fori_loop(0, groups, weigh, (jnp.zeros((8, rows), F32), jnp.zeros((hd, rows), F32)))
            made[k] = (acc / jnp.sum(l8, axis=0, keepdims=True)).astype(BF)

            @pl.when(k < groups - 1)
            def _():
                o_copy(k).start()

            return c

        lax.fori_loop(0, 1, block, 0)
        arrived(w2_rest, 3, 4)
        start(w2_rest, 7)
        lax.fori_loop(1, 2, block, 0)
        rest_own.wait()
        arrived(w2_rest, 2, 5, 6, 7)
        outs(0, cut, model)
        start(second, 0, 1)
        outs(1, cut, model)
        start(second, 2)
        outs(2, cut, model)
        start(second, 3)
        lax.fori_loop(2, groups, block, 0)

    pl.run_scoped(own_rows, pltpu.VMEM((groups, 3 * hd, toks), BF), pltpu.VMEM((keys, 256), BF), pltpu.VMEM((256, rows), BF),
                  pltpu.VMEM((keys, rows), F32))
    add_far(second, cut, model)
    oo[me] = made[groups - 1]
    for k in range(groups - 1):
        o_copy(k).wait()
    hv[3, :, width:] = oo[...].reshape(heads, rows).T
    outs(3, 0, model)
    res_load.wait()
    part[0] += res[...].astype(F32)
    for put in first[2:] + second[2:]:
        put.wait()
    for copy in w2_rest:
        copy.wait_send()
    y_ref[...] = (part[0] + near[0] + near[1]).astype(BF)


def mlp(x_loc, wide, oin, qkv, own, full, cores, side):
    rows, model = x_loc.shape
    groups = side * cores
    width, heads = groups * own[0].shape[0], groups * own[2].shape[0]
    anywhere = pl.BlockSpec(memory_space=pl.ANY)
    dma = lambda n: pltpu.SemaphoreType.DMA((n,))
    flops = 2 * side * rows * model * (2 * width + heads)
    return pl.pallas_call(
        functools.partial(mlp_kernel, side, cores),
        in_specs=[anywhere] * 10,
        out_specs=pl.BlockSpec(memory_space=pltpu.VMEM),
        out_shape=jax.ShapeDtypeStruct((rows, model), BF),
        scratch_shapes=[
            pltpu.VMEM((width + heads, model), BF),
            pltpu.VMEM(oin.shape, BF),
            pltpu.VMEM(oin.shape[:2] + (rows,), BF),
            pltpu.VMEM(oin.shape[:2] + (rows,), BF),
            pltpu.VMEM((side, rows, width + heads), BF),
            pltpu.VMEM((3, rows, model), F32),
            pltpu.VMEM((2, rows // 2, model), F32),
            pltpu.VMEM((2, rows, model), F32),
            pltpu.VMEM((rows, model), BF),
            dma(8), dma(groups // 2), dma(12), dma(12), dma(8), dma(8), dma(groups - 1), dma(groups - 1),
        ],
        compiler_params=pltpu.CompilerParams(vmem_limit_bytes=67043328, collective_id=1, has_side_effects=True),
        cost_estimate=pl.CostEstimate(flops=flops, bytes_accessed=4 * model * width, transcendentals=side * rows * width),
        name="mlp",
    )(wide, oin, qkv, *own, *full, x_loc)


def solution(mesh):
    data, tp = mesh.devices.shape
    side = math.isqrt(tp // 2)
    cores = tp // (side * side)
    grid = Mesh(mesh.devices.reshape(data, side, side, cores), ("data", "y", "x", "core"))

    def local_block(x_loc, ln_gamma, w_qkv, w_out, w_up, w_down):
        own = (w_up.T, w_down, w_out[0])
        oin, wide, w1, w2, wo, qkv = front(x_loc, ln_gamma, w_qkv[:, 0, :].T, own, cores, side)
        return mlp(x_loc, wide, oin, qkv, own, (w1, w2, wo), cores, side)

    row_spec = P(("data", "y", "x", "core"), None)
    tp_axes = ("y", "x", "core")
    return jax.shard_map(
        local_block,
        mesh=grid,
        in_specs=(row_spec, P(None), P(None, tp_axes, None), P(tp_axes, None, None), P(None, tp_axes), P(tp_axes, None)),
        out_specs=row_spec,
        check_vma=False,
    )
```

```python
import functools
import math
import jax
import jax.numpy as jnp
from jax import lax
from jax.experimental import pallas as pl
from jax.experimental.pallas import tpu as pltpu
from jax.sharding import Mesh, PartitionSpec as P

LN_EPS = 1e-6
BF = jnp.bfloat16
MESH = pl.DeviceIdType.MESH
F32 = jnp.float32
TK = 256
TRIP = 32
ROWS = 64


def ring(own, slot, axis, split, send, recv):
    side, cores = lax.axis_size(axis), lax.axis_size("core")
    at, core = lax.axis_index(axis), lax.axis_index("core")
    other = (core + 1) % cores
    block = lambda hop: slot((at + hop) % side * cores + core)
    head, tail = pl.ds(0, split), pl.ds(split, own.shape[0] - split)
    nxt, prv, sib = {axis: (at + 1) % side}, {axis: (at + side - 1) % side}, {"core": other}
    plan = (
        (own, block(0), nxt),
        (own, block(0), prv),
        (own, block(0), sib),
        (block(side - 1).at[head], block(side - 1).at[head], nxt),
        (block(1).at[tail], block(1).at[tail], prv),
        (block(side - 1), block(side - 1), sib),
        (block(1), block(1), sib),
        (block(2), block(2), sib),
    )
    return [
        pltpu.make_async_remote_copy(
            src_ref=src, dst_ref=dst, send_sem=send.at[n], recv_sem=recv.at[n], device_id=to, device_id_type=MESH)
        for n, (src, dst, to) in enumerate(plan)
    ]


def start(copies, *which):
    for n in which:
        copies[n].start()


def arrived(copies, *which):
    for n in which:
        copies[n].wait_recv()


def hail(*places):
    barrier = pltpu.get_barrier_semaphore()
    for place in places:
        pl.semaphore_signal(barrier, inc=1, device_id=place, device_id_type=MESH)
    return lambda: pl.semaphore_wait(barrier, len(places))


def front_kernel(side, cores, hd, x_ref, gain_ref, wq_ref, w1_ref, w2_ref, wo_ref, oin_ref, wide_ref, w1_full, w2_full, wo_full, qkv_ref,
                 wv, xv, qk, qkv, qaug, acc_ref, m_ref, wq_send, wq_recv, xs_send, xs_recv, w1_send, w1_recv, a_send, a_recv, o_send, o_recv,
                 xw_send, xw_recv, w2_send, w2_recv, wo_send, wo_recv, local):
    y, x, core = lax.axis_index("y"), lax.axis_index("x"), lax.axis_index("core")
    rows, model = x_ref.shape
    groups, toks = side * cores, side * rows
    keys = groups * toks
    bq = toks // 2
    subs = bq // rows
    scale = hd ** -0.5 * math.log2(math.e)
    depth = qaug.shape[1]
    pad = depth - 3 * hd
    chunk = min(TRIP * TK, keys)
    row_me, col_me = x * cores + core, y * cores + core
    up, down = {"y": (y + 1) % side}, {"y": (y + side - 1) % side}
    right, left = {"x": (x + 1) % side}, {"x": (x + side - 1) % side}
    top, low = pl.ds(0, rows // 2), pl.ds(rows // 2, rows // 2)
    apart = [(d, dc) for d in range(side) for dc in range(cores) if d or dc]
    met = hail(
        *[{"x": (x + d) % side, "core": (core + dc) % cores} for d, dc in apart],
        *[{"y": (y + d) % side, "core": (core + dc) % cores} for d, dc in apart if d])

    wq = ring(wq_ref, lambda n: wv.at[n], "x", wq_ref.shape[0] // 32 * 16, wq_send, wq_recv)
    w1 = ring(w1_ref, lambda n: w1_full.at[n], "y", w1_ref.shape[0] // 2, w1_send, w1_recv)
    w2 = ring(w2_ref.at[:, pl.ds(0, w2_full.shape[2])], lambda n: w2_full.at[n], "y", w2_ref.shape[0] // 2, w2_send, w2_recv)
    wo = ring(wo_ref, lambda n: wo_full.at[n], "y", wo_ref.shape[0] // 32 * 16, wo_send, wo_recv)

    def put(src, dst, send, recv, n, to):
        return pltpu.make_async_remote_copy(
            src_ref=src, dst_ref=dst, send_sem=send.at[n], recv_sem=recv.at[n], device_id=to, device_id_type=MESH)

    before, after, far = (y + side - 1) % side, (y + 1) % side, (y + 2) % side

    def xs_copy(n):
        part = (xv.at[y], xv.at[y], xv.at[before, top], xv.at[after, low])[n]
        return put(part, part, xs_send, xs_recv, n, down if n % 2 else up)

    def xw_copy(n):
        src = (xv.at[y], xv.at[y], wide_ref.at[3, top], wide_ref.at[1, low])[n]
        dst = (wide_ref.at[3], wide_ref.at[1], wide_ref.at[2, top], wide_ref.at[2, low])[n]
        return put(src, dst, xw_send, xw_recv, n, left if n % 2 else right)

    hops = side - 1

    def place(p):
        return (col_me + 1 + p // hops) % groups, (x + 1 + (p % hops + 1) % hops) % side

    def o_block(p):
        return qk.at[p // 4, pl.ds(0, hd), pl.ds(pl.multiple_of(p % 4 * rows, rows), rows)], oin_ref.at[col_me, :, cols(place(p)[1])]

    def o_copy(p):
        to = place(p)[0]
        return put(*o_block(p), o_send, o_recv, p, {"y": to // cores, "core": to % cores})

    def o_keep(p):
        return pltpu.make_async_copy(*o_block(p), local.at[3])

    def head_of(n):
        return (x + n // cores) % side * cores + (core + n) % cores

    qk_rows, v_rows = pl.ds(0, 2 * hd), pl.ds(2 * hd, hd)

    def cols(part):
        return pl.ds(pl.multiple_of(part * rows, rows), rows)

    def home(n, kind, at):
        head = head_of(n)
        return put(qk.at[head, (qk_rows, v_rows)[kind], at], qkv.at[row_me, (qk_rows, v_rows)[kind], at],
                   a_send.at[kind], a_recv.at[kind], n, {"x": head // cores, "core": head % cores})

    own_x = pltpu.make_async_copy(x_ref, xv.at[y], local.at[0])
    own_wq = pltpu.make_async_copy(wq_ref, wv.at[row_me], local.at[1])
    own_x.start()
    own_wq.start()

    def project(xt):
        def norm(r, c):
            at = pl.ds(pl.multiple_of(r * 32, 32), 32)
            row = xv[y, at, :].astype(F32)
            mean = jnp.mean(row, axis=-1, keepdims=True)
            centered = row - mean
            var = jnp.mean(centered * centered, axis=-1, keepdims=True)
            xv[y, at, :] = (centered * lax.rsqrt(var + LN_EPS) * gain_ref[...].reshape(1, model)).astype(BF)
            return c

        def flip(part):
            def piece(k, c):
                at = pl.ds(pl.multiple_of(k * 256, 256), 256)
                xt[at, cols(part)] = xv[part, :, at].T
                return c

            lax.fori_loop(0, model // 256, piece, 0, unroll=2)

        def work(count, pick, parts, go=True):
            def body(k, c):
                n = pick(k)
                for part in parts:
                    qk[head_of(n), :, cols(part)] = jnp.dot(
                        wv[head_of(n)], xt[:, cols(part)], preferred_element_type=F32).astype(BF)
                if go:
                    for part in parts:
                        home(n, 0, cols(part)).start()
                return c

            lax.fori_loop(0, count, body, 0)

        close = lambda k: cores * (1 + 2 * (k // cores)) + k % cores
        distant = lambda k: 2 * cores + k
        here = lambda k: k

        own_x.wait()
        lax.fori_loop(0, rows // 32, norm, 0)
        flip(y)
        met()
        start(wq, 0, 1, 2)
        xs_copy(0).start()
        xs_copy(1).start()
        start(w1, 2)
        keep = pltpu.make_async_copy(xv.at[y], wide_ref.at[0], local.at[2])
        keep.start()
        arrived(wq, 0, 1)
        start(wq, 3, 4, 5, 6)
        xs_copy(0).wait_recv()
        xs_copy(1).wait_recv()
        xs_copy(2).start()
        xs_copy(3).start()
        start(w1, 0, 1)
        flip(before)
        flip(after)
        own_wq.wait()
        arrived(wq, 2, 5, 6)
        work(2 * cores, close, (y, after, before))
        arrived(wq, 3, 4)
        start(wq, 7)
        work(cores, here, (y, after, before), go=False)
        arrived(wq, 7)
        work(cores, distant, (y, after, before))
        xs_copy(2).wait_recv()
        xs_copy(3).wait_recv()
        flip(far)
        work(cores, distant, (far,))
        work(2 * cores, close, (far,))
        work(cores, here, (far,), go=False)
        everything = pl.ds(0, toks)
        for n in range(1, cores):
            home(n, 0, everything).start()
            home(n, 1, everything).start()
        for k in range(cores):
            home(distant(k), 1, everything).start()
        for k in range(2 * cores):
            home(close(k), 1, everything).start()
        qkv[row_me] = qk[row_me]
        keep.wait()
        for n in range(4):
            xs_copy(n).wait_send()
        for copy in wq:
            copy.wait_send()

    pl.run_scoped(project, pltpu.VMEM((model, toks), BF))
    xw_copy(0).start()
    xw_copy(1).start()
    everything = pl.ds(0, toks)
    kept_qkv = pltpu.make_async_copy(qkv, qkv_ref, local.at[4])

    def attend(kaug, s_a, s_b):
        def load_query(b, slot):
            b = jnp.minimum(b, hops * groups // subs - 1)
            for j in range(subs):
                dest, column = place(b * subs + j)
                g = column * cores + dest % cores
                qt = qkv[g, 0:hd, cols(dest // cores)].astype(F32) * scale
                hi = qt.astype(BF)
                rest = qt - hi.astype(F32)
                mid = rest.astype(BF)
                at = slice(j * rows, (j + 1) * rows)
                qaug[slot, 0:hd, at] = hi
                qaug[slot, hd:2 * hd, at] = mid
                qaug[slot, 2 * hd:3 * hd, at] = (rest - mid.astype(F32)).astype(BF)

        def fold(piece, op):
            return op(piece.reshape(piece.shape[0] // 8, 8, bq), axis=0)

        def spread(t, c):
            g = t * TK // toks
            t0 = pl.multiple_of(t * TK - g * toks, TK)
            kt = qkv[g, hd:2 * hd, pl.ds(t0, TK)]
            kaug[pl.ds(pl.multiple_of(t * TK, TK), TK), :] = jnp.concatenate([kt, kt, kt, jnp.zeros((pad, TK), BF)], axis=0).T
            return c

        def first(c, m8):
            at = pl.ds(pl.multiple_of(c * 8 * TK, 8 * TK), 8 * TK)
            s = jnp.dot(kaug[at, :], qaug[0], preferred_element_type=F32)
            s_a[at, :] = s
            return jnp.maximum(m8, fold(s, jnp.max))

        def half(i, s_in, s_out, slot, col):
            m = m_ref[0:1, :]
            acc_ref[...] = jnp.zeros_like(acc_ref)

            def trip(c, carry):
                m8, l8 = carry
                k0 = pl.multiple_of(c * chunk, chunk)
                total = None
                for u in range(chunk // TK):
                    s_new = jnp.dot(kaug[pl.ds(k0 + u * TK, TK), :], qaug[slot], preferred_element_type=F32)
                    ps = []
                    for r in range(0, TK, ROWS):
                        p = jnp.exp2(s_in[pl.ds(k0 + u * TK + r, ROWS), :] - m)
                        l8 = l8 + fold(p, jnp.sum)
                        ps.append(p.astype(BF))
                    at = u * TK % toks
                    vt = qkv[k0 // toks + u * TK // toks, 2 * hd:3 * hd, at:at + TK]
                    d = jnp.dot(vt, jnp.concatenate(ps, axis=0), preferred_element_type=F32)
                    total = d if total is None else total + d
                    for r in range(0, TK, ROWS):
                        piece = s_new[r:r + ROWS]
                        m8 = jnp.maximum(m8, fold(piece, jnp.max))
                        s_out[pl.ds(k0 + u * TK + r, ROWS), :] = piece
                acc_ref[...] += total
                return m8, l8

            m8, l8 = lax.fori_loop(0, (1 + x // side) * (keys // chunk), trip,
                                   (jnp.full((8, bq), -jnp.inf, F32), jnp.zeros((8, bq), F32)))
            qk[i, 0:hd, col:col + bq] = (acc_ref[...] / jnp.sum(l8, axis=0, keepdims=True)).astype(BF)
            m_ref[...] = jnp.broadcast_to(jnp.max(m8, axis=0, keepdims=True), (8, bq))

        for n in range(1, groups):
            home(n, 0, everything).wait()
        lax.fori_loop(0, keys // TK, spread, 0, unroll=4)
        qaug[:, 3 * hd:, :] = jnp.zeros((2, pad, bq), BF)
        load_query(0, 0)
        load_query(1, 1)
        m8 = lax.fori_loop(0, keys // (8 * TK), first, jnp.full((8, bq), -jnp.inf, F32))
        m_ref[...] = jnp.broadcast_to(jnp.max(m8, axis=0, keepdims=True), (8, bq))
        arrived(w1, 0, 1)
        start(w1, 3, 4, 5, 6)
        start(wo, 0, 1, 2)
        start(w2, 0, 1, 2)
        for n in range(1, groups):
            home(n, 1, everything).wait()
        kept_qkv.start()
        steps = hops * groups // 4

        def step(i, c):
            @pl.when(i == steps // 2)
            def _():
                xw_copy(0).wait()
                xw_copy(1).wait()
                xw_copy(2).start()
                xw_copy(3).start()
                arrived(w1, 3, 4)
                start(w1, 7)

            half(i, s_a, s_b, 1, 0)
            load_query(2 * i + 2, 0)

            @pl.when(i == steps // 2 + 1)
            def _():
                for copies in (wo, w2):
                    arrived(copies, 0, 1)
                    start(copies, 3, 4, 5, 6)

            half(i, s_b, s_a, 0, bq)
            load_query(2 * i + 3, 1)

            def leave(j, c):
                p = 4 * i + j

                @pl.when(p < hops * (groups - 1))
                def _():
                    o_copy(p).start()

                @pl.when(p >= hops * (groups - 1))
                def _():
                    o_keep(p).start()

                return c

            return lax.fori_loop(0, 4, leave, c)

        lax.fori_loop(0, steps, step, 0)

    pl.run_scoped(attend, pltpu.VMEM((keys, depth), BF), pltpu.VMEM((keys, bq), F32), pltpu.VMEM((keys, bq), F32))
    for copies in (wo, w2):
        arrived(copies, 3, 4)
        start(copies, 7)
    xw_copy(2).wait()
    xw_copy(3).wait()
    for p in range(hops * (groups - 1)):
        o_copy(p).wait()
    all_kept = oin_ref.at[col_me, :, pl.ds(0, hops * rows)]
    pltpu.make_async_copy(all_kept, all_kept, local.at[3]).wait()
    kept_qkv.wait()
    arrived(w1, 2, 5, 6, 7)
    for copies in (wo, w2):
        arrived(copies, 2, 5, 6, 7)
    for copies in (wo, w2, w1):
        for copy in copies:
            copy.wait_send()


def front(x_loc, gain, wq, own, cores, side):
    rows, model = x_loc.shape
    w1, w2, wo = own
    groups, toks = side * cores, side * rows
    hd = wq.shape[0] // 3
    keys, bq = groups * toks, toks // 2
    anywhere = pl.BlockSpec(memory_space=pl.ANY)
    dma = lambda *n: pltpu.SemaphoreType.DMA(n)
    flops = 2 * toks * model * groups * wq.shape[0] + 6 * keys * keys * hd
    return pl.pallas_call(
        functools.partial(front_kernel, side, cores, hd),
        in_specs=[anywhere, pl.BlockSpec(memory_space=pltpu.VMEM)] + [anywhere] * 4,
        out_specs=[anywhere] * 6,
        out_shape=[
            jax.ShapeDtypeStruct((groups, hd, toks), BF),
            jax.ShapeDtypeStruct((side, rows, model), BF),
            jax.ShapeDtypeStruct((groups,) + w1.shape, BF),
            jax.ShapeDtypeStruct((groups, w2.shape[0], first_columns(model)), BF),
            jax.ShapeDtypeStruct((groups,) + wo.shape, BF),
            jax.ShapeDtypeStruct((groups, 3 * hd, toks), BF),
        ],
        scratch_shapes=[
            pltpu.VMEM((groups,) + wq.shape, BF),
            pltpu.VMEM((side, rows, model), BF),
            pltpu.VMEM((groups, 3 * hd, toks), BF),
            pltpu.VMEM((groups, 3 * hd, toks), BF),
            pltpu.VMEM((2, 256, bq), BF),
            pltpu.VMEM((hd, bq), F32),
            pltpu.VMEM((8, bq), F32),
            dma(8), dma(8), dma(4), dma(4), dma(8), dma(8), dma(2, groups), dma(2, groups),
            dma((side - 1) * (groups - 1)), dma((side - 1) * (groups - 1)), dma(4), dma(4), dma(8), dma(8), dma(8), dma(8), dma(5),
        ],
        compiler_params=pltpu.CompilerParams(
            vmem_limit_bytes=67043328, collective_id=0, has_side_effects=True),
        cost_estimate=pl.CostEstimate(flops=flops, bytes_accessed=4 * w1.size, transcendentals=keys * keys),
        name="front",
    )(x_loc, gain, wq, w1, w2, wo)


def first_columns(model):
    return model * 2 // 5 // 256 * 256


def mlp_kernel(side, cores, wide_ref, oin_ref, qkv_ref, w1_own, w2_own, wo_own, w1_ref, w2_ref, wo_ref, res_ref, y_ref, w2, ov, oo, made, hv,
               part, far, near, res, load, w1_sem, send, recv, w2_send, w2_recv, o_send, o_recv):
    x, y, core = lax.axis_index("x"), lax.axis_index("y"), lax.axis_index("core")
    right, left = {"x": (x + 1) % side}, {"x": (x + side - 1) % side}
    _, rows, model = wide_ref.shape
    groups, hd, toks = oin_ref.shape
    width = groups * w1_own.shape[0]
    heads = groups * hd
    keys = groups * toks
    cut = w2_ref.shape[2]
    step = math.gcd(cut, model - cut, 512)
    half = rows // 2
    me = y * cores + core
    top, low = pl.ds(0, half), pl.ds(half, half)
    order = (2, 1, 3, 0)
    pair = 2 * w1_own.shape[0]
    met = hail(right, left, *[
        {"y": (me + hop) % groups // cores, "core": (me + hop) % cores} for hop in range(1, groups)])

    def shard(into, base, size, n, columns):
        return into.at[pl.ds(pl.multiple_of(base + n * size, 16), size), columns]

    def gathered(own, full, into, base, sem):
        size, columns = full.shape[1], pl.ds(0, full.shape[2])
        for hop in range(groups):
            n = (me + hop) % groups
            pltpu.make_async_copy(full.at[n] if hop else own.at[:, columns], shard(into, base, size, n, columns), sem).start()
        whole = into.at[pl.ds(base, groups * size), columns]
        return pltpu.make_async_copy(whole, whole, sem)

    rest = pl.ds(cut, model - cut)
    o_load = pltpu.make_async_copy(oin_ref, ov, load.at[2])
    res_load = pltpu.make_async_copy(res_ref, res, load.at[3])
    rest_own = pltpu.make_async_copy(w2_own.at[:, rest], shard(w2, 0, width // groups, me, rest), load.at[4])
    w2_rest = ring(w2_own.at[:, rest], lambda n: shard(w2, 0, width // groups, n, rest), "y", width // groups // 2, w2_send, w2_recv)

    def outs(n, lo, hi):
        def piece(d, c):
            at = pl.ds(pl.multiple_of(d * step, step), step)
            part[n % 3, :, at] = jnp.dot(hv[n], w2[:, at], preferred_element_type=F32)
            return c

        lax.fori_loop(lo // step, hi // step, piece, 0)

    def plan(lo, hi, first):
        cols = pl.ds(lo, hi - lo)
        copies = (
            (part.at[0, top, cols], far.at[0, :, cols], right),
            (part.at[0, low, cols], far.at[1, :, cols], left),
            (part.at[1, low, cols], near.at[0, low, cols], right),
            (part.at[2, top, cols], near.at[1, top, cols], left),
            (part.at[1, top, cols], near.at[0, top, cols], right),
            (part.at[2, low, cols], near.at[1, low, cols], left),
        )
        return [
            pltpu.make_async_remote_copy(src_ref=src, dst_ref=dst, send_sem=send.at[first + n], recv_sem=recv.at[first + n],
                                         device_id=to, device_id_type=MESH)
            for n, (src, dst, to) in enumerate(copies)
        ]

    def add_far(puts, lo, hi):
        puts[0].wait()
        part[1, :half, lo:hi] += far[0, :, lo:hi]
        start(puts, 4)
        puts[1].wait()
        part[2, half:, lo:hi] += far[1, :, lo:hi]
        start(puts, 5)

    first, second = plan(0, cut, 0), plan(cut, model, 6)

    def hidden_layer(w1, xv, xt):
        def x_load(n):
            return pltpu.make_async_copy(wide_ref.at[order[n]], xv.at[n % 2], load.at[n % 2])

        def w1_shard(n):
            to = shard(w1, 0, pair // 2, n, pl.ds(0, model))

            @pl.when(n == me)
            def _():
                pltpu.make_async_copy(w1_own, to, w1_sem.at[n // 2]).start()

            @pl.when(n != me)
            def _():
                pltpu.make_async_copy(w1_ref.at[n], to, w1_sem.at[n // 2]).start()

        x_load(0).start()
        for n in range(groups):
            w1_shard(n)
        o_load.start()
        later = []

        def load_others():
            later.append(gathered(w2_own, w2_ref, w2, 0, load.at[5]))
            later.append(gathered(wo_own, wo_ref, w2, width, load.at[6]))
            x_load(1).start()
            rest_own.start()
            res_load.start()

        def hidden(n):
            x_load(n).wait()

            def flip(k, c):
                at = pl.ds(pl.multiple_of(k * 256, 256), 256)
                xt[at, :] = xv[n % 2, :, at].T
                return c

            if n == 0:
                met()
                start(w2_rest, 0, 1, 2)
            lax.fori_loop(0, model // 256, flip, 0, unroll=2)
            if n == 1:
                x_load(3).start()

            def piece(f, c):
                at = pl.ds(pl.multiple_of(f * pair, pair), pair)
                if n == 0:
                    pltpu.make_async_copy(w1.at[at], w1.at[at], w1_sem.at[f]).wait()
                pre = jnp.dot(w1[at, :], xt[...], preferred_element_type=F32)
                hv[n, :, at] = jax.nn.gelu(pre, approximate=True).astype(BF).T
                return c

            if n == 0:
                lax.fori_loop(0, groups // 4, piece, 0)
                load_others()
                lax.fori_loop(groups // 4, groups // 2, piece, 0)
                x_load(2).start()
                o_load.wait()
            else:
                lax.fori_loop(0, groups // 2, piece, 0)
            if n < 3:
                col = pl.multiple_of((x + order[n]) % side * rows, rows)
                hv[n, :, width:] = ov[:, :, pl.ds(col, rows)].reshape(heads, rows).T

        hidden(0)
        for copy in later:
            copy.wait()
        outs(0, 0, cut)
        start(first, 0, 1)
        hidden(1)
        outs(1, 0, cut)
        start(first, 2)
        hidden(2)
        outs(2, 0, cut)
        start(first, 3)
        arrived(w2_rest, 0, 1)
        start(w2_rest, 3, 4, 5, 6)
        add_far(first, 0, cut)
        hidden(3)

    pl.run_scoped(hidden_layer, pltpu.VMEM((width, model), BF), pltpu.VMEM((2, rows, model), BF), pltpu.VMEM((model, rows), BF))

    def o_copy(k):
        to = (me + 1 + k) % groups
        return pltpu.make_async_remote_copy(
            src_ref=made.at[k], dst_ref=oo.at[me], send_sem=o_send.at[k], recv_sem=o_recv.at[k],
            device_id={"y": to // cores, "core": to % cores}, device_id_type=MESH)

    def own_rows(qkv, kaug, qaug, scores):
        depth = kaug.shape[1]
        scale = hd ** -0.5 * math.log2(math.e)
        fetch = pltpu.make_async_copy(qkv_ref, qkv, load.at[7])
        fetch.start()
        fetch.wait()
        pad = jnp.zeros((depth - 3 * hd, TK), BF)

        def spread(t, c):
            g = t * TK // toks
            kt = qkv[g, hd:2 * hd, pl.ds(pl.multiple_of(t * TK - g * toks, TK), TK)]
            kaug[pl.ds(pl.multiple_of(t * TK, TK), TK), :] = jnp.concatenate([kt, kt, kt, pad], axis=0).T
            return c

        lax.fori_loop(0, keys // TK, spread, 0, unroll=4)
        qaug[3 * hd:, :] = jnp.zeros((depth - 3 * hd, rows), BF)

        def fold(piece, op):
            return op(piece.reshape(piece.shape[0] // 8, 8, rows), axis=0)

        def block(k, c):
            dest = (me + 1 + k) % groups
            qt = qkv[x * cores + dest % cores, 0:hd, pl.ds(pl.multiple_of(dest // cores * rows, rows), rows)].astype(F32) * scale
            hi = qt.astype(BF)
            left_over = qt - hi.astype(F32)
            mid = left_over.astype(BF)
            qaug[0:hd, :] = hi
            qaug[hd:2 * hd, :] = mid
            qaug[2 * hd:3 * hd, :] = (left_over - mid.astype(F32)).astype(BF)

            def score(t, m8):
                at = pl.ds(pl.multiple_of(t * 2 * toks, 2 * toks), 2 * toks)
                s = jnp.dot(kaug[at, :], qaug[...], preferred_element_type=F32)
                scores[at, :] = s
                return jnp.maximum(m8, fold(s, jnp.max))

            m8 = lax.fori_loop(0, groups // 2, score, jnp.full((8, rows), -jnp.inf, F32))
            m = jnp.max(m8, axis=0, keepdims=True)

            def weigh(g, carry):
                l8, acc = carry
                ps = []
                for r in range(0, toks, ROWS):
                    p = jnp.exp2(scores[pl.ds(pl.multiple_of(g * toks, toks) + r, ROWS), :] - m)
                    l8 = l8 + fold(p, jnp.sum)
                    ps.append(p.astype(BF))
                return l8, acc + jnp.dot(qkv[g, 2 * hd:3 * hd, :], jnp.concatenate(ps, axis=0), preferred_element_type=F32)

            l8, acc = lax.fori_loop(0, groups, weigh, (jnp.zeros((8, rows), F32), jnp.zeros((hd, rows), F32)))
            made[k] = (acc / jnp.sum(l8, axis=0, keepdims=True)).astype(BF)

            @pl.when(k < groups - 1)
            def _():
                o_copy(k).start()

            return c

        lax.fori_loop(0, 1, block, 0)
        arrived(w2_rest, 3, 4)
        start(w2_rest, 7)
        lax.fori_loop(1, 2, block, 0)
        rest_own.wait()
        arrived(w2_rest, 2, 5, 6, 7)
        outs(0, cut, model)
        start(second, 0, 1)
        outs(1, cut, model)
        start(second, 2)
        outs(2, cut, model)
        start(second, 3)
        lax.fori_loop(2, groups, block, 0)

    pl.run_scoped(own_rows, pltpu.VMEM((groups, 3 * hd, toks), BF), pltpu.VMEM((keys, 256), BF), pltpu.VMEM((256, rows), BF),
                  pltpu.VMEM((keys, rows), F32))
    add_far(second, cut, model)
    oo[me] = made[groups - 1]
    for k in range(groups - 1):
        o_copy(k).wait()
    hv[3, :, width:] = oo[...].reshape(heads, rows).T
    outs(3, 0, model)
    res_load.wait()
    part[0] += res[...].astype(F32)
    for put in first[2:] + second[2:]:
        put.wait()
    for copy in w2_rest:
        copy.wait_send()
    y_ref[...] = (part[0] + near[0] + near[1]).astype(BF)


def mlp(x_loc, wide, oin, qkv, own, full, cores, side):
    rows, model = x_loc.shape
    groups = side * cores
    width, heads = groups * own[0].shape[0], groups * own[2].shape[0]
    anywhere = pl.BlockSpec(memory_space=pl.ANY)
    dma = lambda n: pltpu.SemaphoreType.DMA((n,))
    flops = 2 * side * rows * model * (2 * width + heads)
    return pl.pallas_call(
        functools.partial(mlp_kernel, side, cores),
        in_specs=[anywhere] * 10,
        out_specs=pl.BlockSpec(memory_space=pltpu.VMEM),
        out_shape=jax.ShapeDtypeStruct((rows, model), BF),
        scratch_shapes=[
            pltpu.VMEM((width + heads, model), BF),
            pltpu.VMEM(oin.shape, BF),
            pltpu.VMEM(oin.shape[:2] + (rows,), BF),
            pltpu.VMEM(oin.shape[:2] + (rows,), BF),
            pltpu.VMEM((side, rows, width + heads), BF),
            pltpu.VMEM((3, rows, model), F32),
            pltpu.VMEM((2, rows // 2, model), F32),
            pltpu.VMEM((2, rows, model), F32),
            pltpu.VMEM((rows, model), BF),
            dma(8), dma(groups // 2), dma(12), dma(12), dma(8), dma(8), dma(groups - 1), dma(groups - 1),
        ],
        compiler_params=pltpu.CompilerParams(vmem_limit_bytes=67043328, collective_id=1, has_side_effects=True),
        cost_estimate=pl.CostEstimate(flops=flops, bytes_accessed=4 * model * width, transcendentals=side * rows * width),
        name="mlp",
    )(wide, oin, qkv, *own, *full, x_loc)


def solution(mesh):
    data, tp = mesh.devices.shape
    side = math.isqrt(tp // 2)
    cores = tp // (side * side)
    grid = Mesh(mesh.devices.reshape(data, side, side, cores), ("data", "y", "x", "core"))

    def local_block(x_loc, ln_gamma, w_qkv, w_out, w_up, w_down):
        own = (w_up.T, w_down, w_out[0])
        oin, wide, w1, w2, wo, qkv = front(x_loc, ln_gamma, w_qkv[:, 0, :].T, own, cores, side)
        return mlp(x_loc, wide, oin, qkv, own, (w1, w2, wo), cores, side)

    row_spec = P(("data", "y", "x", "core"), None)
    tp_axes = ("y", "x", "core")
    return jax.shard_map(
        local_block,
        mesh=grid,
        in_specs=(row_spec, P(None), P(None, tp_axes, None), P(tp_axes, None, None), P(None, tp_axes), P(tp_axes, None)),
        out_specs=row_spec,
        check_vma=False,
    )
```

```python
import functools
import math
import jax
import jax.numpy as jnp
from jax import lax
from jax.experimental import pallas as pl
from jax.experimental.pallas import tpu as pltpu
from jax.sharding import Mesh, PartitionSpec as P

LN_EPS = 1e-6
BF = jnp.bfloat16
MESH = pl.DeviceIdType.MESH
F32 = jnp.float32
TK = 256
TRIP = 32
ROWS = 64


def ring(own, slot, axis, split, send, recv):
    side, cores = lax.axis_size(axis), lax.axis_size("core")
    at, core = lax.axis_index(axis), lax.axis_index("core")
    other = (core + 1) % cores
    block = lambda hop: slot((at + hop) % side * cores + core)
    head, tail = pl.ds(0, split), pl.ds(split, own.shape[0] - split)
    nxt, prv, sib = {axis: (at + 1) % side}, {axis: (at + side - 1) % side}, {"core": other}
    plan = (
        (own, block(0), nxt),
        (own, block(0), prv),
        (own, block(0), sib),
        (block(side - 1).at[head], block(side - 1).at[head], nxt),
        (block(1).at[tail], block(1).at[tail], prv),
        (block(side - 1), block(side - 1), sib),
        (block(1), block(1), sib),
        (block(2), block(2), sib),
    )
    return [
        pltpu.make_async_remote_copy(
            src_ref=src, dst_ref=dst, send_sem=send.at[n], recv_sem=recv.at[n], device_id=to, device_id_type=MESH)
        for n, (src, dst, to) in enumerate(plan)
    ]


def start(copies, *which):
    for n in which:
        copies[n].start()


def arrived(copies, *which):
    for n in which:
        copies[n].wait_recv()


def hail(*places):
    barrier = pltpu.get_barrier_semaphore()
    for place in places:
        pl.semaphore_signal(barrier, inc=1, device_id=place, device_id_type=MESH)
    return lambda: pl.semaphore_wait(barrier, len(places))


def front_kernel(side, cores, hd, x_ref, gain_ref, wq_ref, w1_ref, w2_ref, wo_ref, oin_ref, wide_ref, w1_full, w2_full, wo_full, qkv_ref,
                 wv, xv, qk, qkv, qaug, acc_ref, m_ref, wq_send, wq_recv, xs_send, xs_recv, w1_send, w1_recv, a_send, a_recv, o_send, o_recv,
                 xw_send, xw_recv, w2_send, w2_recv, wo_send, wo_recv, local):
    y, x, core = lax.axis_index("y"), lax.axis_index("x"), lax.axis_index("core")
    rows, model = x_ref.shape
    groups, toks = side * cores, side * rows
    keys = groups * toks
    bq = toks // 2
    subs = bq // rows
    scale = hd ** -0.5 * math.log2(math.e)
    depth = qaug.shape[1]
    pad = depth - 3 * hd
    chunk = min(TRIP * TK, keys)
    row_me, col_me = x * cores + core, y * cores + core
    up, down = {"y": (y + 1) % side}, {"y": (y + side - 1) % side}
    right, left = {"x": (x + 1) % side}, {"x": (x + side - 1) % side}
    top, low = pl.ds(0, rows // 2), pl.ds(rows // 2, rows // 2)
    apart = [(d, dc) for d in range(side) for dc in range(cores) if d or dc]
    met = hail(
        *[{"x": (x + d) % side, "core": (core + dc) % cores} for d, dc in apart],
        *[{"y": (y + d) % side, "core": (core + dc) % cores} for d, dc in apart if d])

    wq = ring(wq_ref, lambda n: wv.at[n], "x", wq_ref.shape[0] // 32 * 16, wq_send, wq_recv)
    w1 = ring(w1_ref, lambda n: w1_full.at[n], "y", w1_ref.shape[0] // 2, w1_send, w1_recv)
    w2 = ring(w2_ref.at[:, pl.ds(0, w2_full.shape[2])], lambda n: w2_full.at[n], "y", w2_ref.shape[0] // 2, w2_send, w2_recv)
    wo = ring(wo_ref.at[:, pl.ds(0, wo_full.shape[2])], lambda n: wo_full.at[n], "y", wo_ref.shape[0] // 32 * 16, wo_send, wo_recv)

    def put(src, dst, send, recv, n, to):
        return pltpu.make_async_remote_copy(
            src_ref=src, dst_ref=dst, send_sem=send.at[n], recv_sem=recv.at[n], device_id=to, device_id_type=MESH)

    before, after, far = (y + side - 1) % side, (y + 1) % side, (y + 2) % side

    def xs_copy(n):
        part = (xv.at[y], xv.at[y], xv.at[before, top], xv.at[after, low])[n]
        return put(part, part, xs_send, xs_recv, n, down if n % 2 else up)

    def xw_copy(n):
        src = (xv.at[y], xv.at[y], wide_ref.at[3, top], wide_ref.at[1, low])[n]
        dst = (wide_ref.at[3], wide_ref.at[1], wide_ref.at[2, top], wide_ref.at[2, low])[n]
        return put(src, dst, xw_send, xw_recv, n, left if n % 2 else right)

    hops = side - 1

    def place(p):
        return (col_me + 1 + p // hops) % groups, (x + 1 + (p % hops + 1) % hops) % side

    def o_block(p):
        return qk.at[p // 4, pl.ds(0, hd), pl.ds(pl.multiple_of(p % 4 * rows, rows), rows)], oin_ref.at[col_me, :, cols(place(p)[1])]

    def o_copy(p):
        to = place(p)[0]
        return put(*o_block(p), o_send, o_recv, p, {"y": to // cores, "core": to % cores})

    def o_keep(p):
        return pltpu.make_async_copy(*o_block(p), local.at[3])

    def head_of(n):
        return (x + n // cores) % side * cores + (core + n) % cores

    qk_rows, v_rows = pl.ds(0, 2 * hd), pl.ds(2 * hd, hd)

    def cols(part):
        return pl.ds(pl.multiple_of(part * rows, rows), rows)

    def home(n, kind, at):
        head = head_of(n)
        return put(qk.at[head, (qk_rows, v_rows)[kind], at], qkv.at[row_me, (qk_rows, v_rows)[kind], at],
                   a_send.at[kind], a_recv.at[kind], n, {"x": head // cores, "core": head % cores})

    own_x = pltpu.make_async_copy(x_ref, xv.at[y], local.at[0])
    own_wq = pltpu.make_async_copy(wq_ref, wv.at[row_me], local.at[1])
    own_x.start()
    own_wq.start()

    def project(xt):
        def norm(r, c):
            at = pl.ds(pl.multiple_of(r * 32, 32), 32)
            row = xv[y, at, :].astype(F32)
            mean = jnp.mean(row, axis=-1, keepdims=True)
            centered = row - mean
            var = jnp.mean(centered * centered, axis=-1, keepdims=True)
            xv[y, at, :] = (centered * lax.rsqrt(var + LN_EPS) * gain_ref[...].reshape(1, model)).astype(BF)
            return c

        def flip(part):
            def piece(k, c):
                at = pl.ds(pl.multiple_of(k * 256, 256), 256)
                xt[at, cols(part)] = xv[part, :, at].T
                return c

            lax.fori_loop(0, model // 256, piece, 0, unroll=2)

        def work(count, pick, parts, go=True):
            def body(k, c):
                n = pick(k)
                for part in parts:
                    qk[head_of(n), :, cols(part)] = jnp.dot(
                        wv[head_of(n)], xt[:, cols(part)], preferred_element_type=F32).astype(BF)
                if go:
                    for part in parts:
                        home(n, 0, cols(part)).start()
                return c

            lax.fori_loop(0, count, body, 0)

        close = lambda k: cores * (1 + 2 * (k // cores)) + k % cores
        distant = lambda k: 2 * cores + k
        here = lambda k: k

        own_x.wait()
        lax.fori_loop(0, rows // 32, norm, 0)
        flip(y)
        met()
        start(wq, 0, 1, 2)
        xs_copy(0).start()
        xs_copy(1).start()
        start(w1, 2)
        keep = pltpu.make_async_copy(xv.at[y], wide_ref.at[0], local.at[2])
        keep.start()
        arrived(wq, 0, 1)
        start(wq, 3, 4, 5, 6)
        xs_copy(0).wait_recv()
        xs_copy(1).wait_recv()
        xs_copy(2).start()
        xs_copy(3).start()
        start(w1, 0, 1)
        start(wo, 0, 1, 2)
        start(w2, 0, 1, 2)
        flip(before)
        flip(after)
        own_wq.wait()
        arrived(wq, 2, 5, 6)
        work(2 * cores, close, (y, after, before))
        arrived(wq, 3, 4)
        start(wq, 7)
        work(cores, here, (y, after, before), go=False)
        arrived(wq, 7)
        work(cores, distant, (y, after, before))
        xs_copy(2).wait_recv()
        xs_copy(3).wait_recv()
        flip(far)
        work(cores, distant, (far,))
        work(2 * cores, close, (far,))
        work(cores, here, (far,), go=False)
        everything = pl.ds(0, toks)
        for n in range(1, cores):
            home(n, 0, everything).start()
            home(n, 1, everything).start()
        for k in range(cores):
            home(distant(k), 1, everything).start()
        for k in range(2 * cores):
            home(close(k), 1, everything).start()
        qkv[row_me] = qk[row_me]
        keep.wait()
        for n in range(4):
            xs_copy(n).wait_send()
        for copy in wq:
            copy.wait_send()

    pl.run_scoped(project, pltpu.VMEM((model, toks), BF))
    xw_copy(0).start()
    xw_copy(1).start()
    everything = pl.ds(0, toks)
    kept_qkv = pltpu.make_async_copy(qkv, qkv_ref, local.at[4])

    def attend(kaug, s_a, s_b):
        def load_query(b, slot):
            b = jnp.minimum(b, hops * groups // subs - 1)
            for j in range(subs):
                dest, column = place(b * subs + j)
                g = column * cores + dest % cores
                qt = qkv[g, 0:hd, cols(dest // cores)].astype(F32) * scale
                hi = qt.astype(BF)
                rest = qt - hi.astype(F32)
                mid = rest.astype(BF)
                at = slice(j * rows, (j + 1) * rows)
                qaug[slot, 0:hd, at] = hi
                qaug[slot, hd:2 * hd, at] = mid
                qaug[slot, 2 * hd:3 * hd, at] = (rest - mid.astype(F32)).astype(BF)

        def fold(piece, op):
            return op(piece.reshape(piece.shape[0] // 8, 8, bq), axis=0)

        def spread(t, c):
            g = t * TK // toks
            t0 = pl.multiple_of(t * TK - g * toks, TK)
            kt = qkv[g, hd:2 * hd, pl.ds(t0, TK)]
            kaug[pl.ds(pl.multiple_of(t * TK, TK), TK), :] = jnp.concatenate([kt, kt, kt, jnp.zeros((pad, TK), BF)], axis=0).T
            return c

        def first(c, m8):
            at = pl.ds(pl.multiple_of(c * 8 * TK, 8 * TK), 8 * TK)
            s = jnp.dot(kaug[at, :], qaug[0], preferred_element_type=F32)
            s_a[at, :] = s
            return jnp.maximum(m8, fold(s, jnp.max))

        def half(i, s_in, s_out, slot, col):
            m = m_ref[0:1, :]
            acc_ref[...] = jnp.zeros_like(acc_ref)

            def trip(c, carry):
                m8, l8 = carry
                k0 = pl.multiple_of(c * chunk, chunk)
                total = None
                for u in range(chunk // TK):
                    s_new = jnp.dot(kaug[pl.ds(k0 + u * TK, TK), :], qaug[slot], preferred_element_type=F32)
                    ps = []
                    for r in range(0, TK, ROWS):
                        p = jnp.exp2(s_in[pl.ds(k0 + u * TK + r, ROWS), :] - m)
                        l8 = l8 + fold(p, jnp.sum)
                        ps.append(p.astype(BF))
                    at = u * TK % toks
                    vt = qkv[k0 // toks + u * TK // toks, 2 * hd:3 * hd, at:at + TK]
                    d = jnp.dot(vt, jnp.concatenate(ps, axis=0), preferred_element_type=F32)
                    total = d if total is None else total + d
                    for r in range(0, TK, ROWS):
                        piece = s_new[r:r + ROWS]
                        m8 = jnp.maximum(m8, fold(piece, jnp.max))
                        s_out[pl.ds(k0 + u * TK + r, ROWS), :] = piece
                acc_ref[...] += total
                return m8, l8

            m8, l8 = lax.fori_loop(0, (1 + x // side) * (keys // chunk), trip,
                                   (jnp.full((8, bq), -jnp.inf, F32), jnp.zeros((8, bq), F32)))
            qk[i, 0:hd, col:col + bq] = (acc_ref[...] / jnp.sum(l8, axis=0, keepdims=True)).astype(BF)
            m_ref[...] = jnp.broadcast_to(jnp.max(m8, axis=0, keepdims=True), (8, bq))

        for n in range(1, groups):
            home(n, 0, everything).wait()
        lax.fori_loop(0, keys // TK, spread, 0, unroll=4)
        qaug[:, 3 * hd:, :] = jnp.zeros((2, pad, bq), BF)
        load_query(0, 0)
        load_query(1, 1)
        m8 = lax.fori_loop(0, keys // (8 * TK), first, jnp.full((8, bq), -jnp.inf, F32))
        m_ref[...] = jnp.broadcast_to(jnp.max(m8, axis=0, keepdims=True), (8, bq))
        arrived(w1, 0, 1)
        start(w1, 3, 4, 5, 6)
        for n in range(1, groups):
            home(n, 1, everything).wait()
        kept_qkv.start()
        steps = hops * groups // 4

        def step(i, c):
            @pl.when(i == steps // 2)
            def _():
                xw_copy(0).wait()
                xw_copy(1).wait()
                xw_copy(2).start()
                xw_copy(3).start()
                for copies in (wo, w2):
                    arrived(copies, 0, 1)
                    start(copies, 3, 4, 5, 6)

            half(i, s_a, s_b, 1, 0)
            load_query(2 * i + 2, 0)

            @pl.when(i == steps // 2 + 1)
            def _():
                arrived(w1, 3, 4)
                start(w1, 7)

            half(i, s_b, s_a, 0, bq)
            load_query(2 * i + 3, 1)

            def leave(j, c):
                p = 4 * i + j

                @pl.when(p < hops * (groups - 1))
                def _():
                    o_copy(p).start()

                @pl.when(p >= hops * (groups - 1))
                def _():
                    o_keep(p).start()

                return c

            return lax.fori_loop(0, 4, leave, c)

        lax.fori_loop(0, steps, step, 0)

    pl.run_scoped(attend, pltpu.VMEM((keys, depth), BF), pltpu.VMEM((keys, bq), F32), pltpu.VMEM((keys, bq), F32))
    for copies in (wo, w2):
        arrived(copies, 3, 4)
        start(copies, 7)
    xw_copy(2).wait()
    xw_copy(3).wait()
    for p in range(hops * (groups - 1)):
        o_copy(p).wait()
    all_kept = oin_ref.at[col_me, :, pl.ds(0, hops * rows)]
    pltpu.make_async_copy(all_kept, all_kept, local.at[3]).wait()
    kept_qkv.wait()
    arrived(w1, 2, 5, 6, 7)
    for copies in (wo, w2):
        arrived(copies, 2, 5, 6, 7)
    for copies in (wo, w2, w1):
        for copy in copies:
            copy.wait_send()


def front(x_loc, gain, wq, own, cores, side):
    rows, model = x_loc.shape
    w1, w2, wo = own
    groups, toks = side * cores, side * rows
    hd = wq.shape[0] // 3
    keys, bq = groups * toks, toks // 2
    anywhere = pl.BlockSpec(memory_space=pl.ANY)
    dma = lambda *n: pltpu.SemaphoreType.DMA(n)
    flops = 2 * toks * model * groups * wq.shape[0] + 6 * keys * keys * hd
    return pl.pallas_call(
        functools.partial(front_kernel, side, cores, hd),
        in_specs=[anywhere, pl.BlockSpec(memory_space=pltpu.VMEM)] + [anywhere] * 4,
        out_specs=[anywhere] * 6,
        out_shape=[
            jax.ShapeDtypeStruct((groups, hd, toks), BF),
            jax.ShapeDtypeStruct((side, rows, model), BF),
            jax.ShapeDtypeStruct((groups,) + w1.shape, BF),
            jax.ShapeDtypeStruct((groups, w2.shape[0], first_columns(model)), BF),
            jax.ShapeDtypeStruct((groups, wo.shape[0], first_columns(model)), BF),
            jax.ShapeDtypeStruct((groups, 3 * hd, toks), BF),
        ],
        scratch_shapes=[
            pltpu.VMEM((groups,) + wq.shape, BF),
            pltpu.VMEM((side, rows, model), BF),
            pltpu.VMEM((groups, 3 * hd, toks), BF),
            pltpu.VMEM((groups, 3 * hd, toks), BF),
            pltpu.VMEM((2, 256, bq), BF),
            pltpu.VMEM((hd, bq), F32),
            pltpu.VMEM((8, bq), F32),
            dma(8), dma(8), dma(4), dma(4), dma(8), dma(8), dma(2, groups), dma(2, groups),
            dma((side - 1) * (groups - 1)), dma((side - 1) * (groups - 1)), dma(4), dma(4), dma(8), dma(8), dma(8), dma(8), dma(5),
        ],
        compiler_params=pltpu.CompilerParams(
            vmem_limit_bytes=67043328, collective_id=0, has_side_effects=True),
        cost_estimate=pl.CostEstimate(flops=flops, bytes_accessed=4 * w1.size, transcendentals=keys * keys),
        name="front",
    )(x_loc, gain, wq, w1, w2, wo)


def first_columns(model):
    return model * 2 // 5 // 256 * 256


def mlp_kernel(side, cores, wide_ref, oin_ref, qkv_ref, w1_own, w2_own, wo_own, w1_ref, w2_ref, wo_ref, res_ref, y_ref, w2, ov, oo, made, hv,
               part, far, near, res, load, w1_sem, send, recv, w2_send, w2_recv, wo_send, wo_recv, o_send, o_recv):
    x, y, core = lax.axis_index("x"), lax.axis_index("y"), lax.axis_index("core")
    right, left = {"x": (x + 1) % side}, {"x": (x + side - 1) % side}
    _, rows, model = wide_ref.shape
    groups, hd, toks = oin_ref.shape
    width = groups * w1_own.shape[0]
    heads = groups * hd
    keys = groups * toks
    cut = w2_ref.shape[2]
    step = math.gcd(cut, model - cut, 512)
    half = rows // 2
    me = y * cores + core
    top, low = pl.ds(0, half), pl.ds(half, half)
    order = (2, 1, 3, 0)
    pair = 2 * w1_own.shape[0]
    met = hail(right, left, *[
        {"y": (me + hop) % groups // cores, "core": (me + hop) % cores} for hop in range(1, groups)])

    def shard(into, base, size, n, columns):
        return into.at[pl.ds(pl.multiple_of(base + n * size, 16), size), columns]

    def gathered(own, full, into, base, sem):
        size, columns = full.shape[1], pl.ds(0, full.shape[2])
        for hop in range(groups):
            n = (me + hop) % groups
            pltpu.make_async_copy(full.at[n] if hop else own.at[:, columns], shard(into, base, size, n, columns), sem).start()
        whole = into.at[pl.ds(base, groups * size), columns]
        return pltpu.make_async_copy(whole, whole, sem)

    rest = pl.ds(cut, model - cut)
    o_load = pltpu.make_async_copy(oin_ref, ov, load.at[2])
    res_load = pltpu.make_async_copy(res_ref, res, load.at[3])
    rest_own = pltpu.make_async_copy(w2_own.at[:, rest], shard(w2, 0, width // groups, me, rest), load.at[4])
    wo_rest_own = pltpu.make_async_copy(wo_own.at[:, rest], shard(w2, width, hd, me, rest), load.at[8])
    w2_rest = ring(w2_own.at[:, rest], lambda n: shard(w2, 0, width // groups, n, rest), "y", width // groups // 2, w2_send, w2_recv)
    wo_rest = ring(wo_own.at[:, rest], lambda n: shard(w2, width, hd, n, rest), "y", hd // 32 * 16, wo_send, wo_recv)

    def outs(n, lo, hi):
        def piece(d, c):
            at = pl.ds(pl.multiple_of(d * step, step), step)
            part[n % 3, :, at] = jnp.dot(hv[n], w2[:, at], preferred_element_type=F32)
            return c

        lax.fori_loop(lo // step, hi // step, piece, 0)

    def plan(lo, hi, first):
        cols = pl.ds(lo, hi - lo)
        copies = (
            (part.at[0, top, cols], far.at[0, :, cols], right),
            (part.at[0, low, cols], far.at[1, :, cols], left),
            (part.at[1, low, cols], near.at[0, low, cols], right),
            (part.at[2, top, cols], near.at[1, top, cols], left),
            (part.at[1, top, cols], near.at[0, top, cols], right),
            (part.at[2, low, cols], near.at[1, low, cols], left),
        )
        return [
            pltpu.make_async_remote_copy(src_ref=src, dst_ref=dst, send_sem=send.at[first + n], recv_sem=recv.at[first + n],
                                         device_id=to, device_id_type=MESH)
            for n, (src, dst, to) in enumerate(copies)
        ]

    def add_far(puts, lo, hi):
        puts[0].wait()
        part[1, :half, lo:hi] += far[0, :, lo:hi]
        start(puts, 4)
        puts[1].wait()
        part[2, half:, lo:hi] += far[1, :, lo:hi]
        start(puts, 5)

    first, second = plan(0, cut, 0), plan(cut, model, 6)

    def hidden_layer(w1, xv, xt):
        def x_load(n):
            return pltpu.make_async_copy(wide_ref.at[order[n]], xv.at[n % 2], load.at[n % 2])

        def w1_shard(n):
            to = shard(w1, 0, pair // 2, n, pl.ds(0, model))

            @pl.when(n == me)
            def _():
                pltpu.make_async_copy(w1_own, to, w1_sem.at[n // 2]).start()

            @pl.when(n != me)
            def _():
                pltpu.make_async_copy(w1_ref.at[n], to, w1_sem.at[n // 2]).start()

        x_load(0).start()
        for n in range(groups):
            w1_shard(n)
        o_load.start()
        later = []

        def load_others():
            later.append(gathered(w2_own, w2_ref, w2, 0, load.at[5]))
            later.append(gathered(wo_own, wo_ref, w2, width, load.at[6]))
            x_load(1).start()
            rest_own.start()
            wo_rest_own.start()
            res_load.start()

        def hidden(n):
            x_load(n).wait()

            def flip(k, c):
                at = pl.ds(pl.multiple_of(k * 256, 256), 256)
                xt[at, :] = xv[n % 2, :, at].T
                return c

            if n == 0:
                met()
                start(wo_rest, 0, 1, 2)
                start(w2_rest, 0, 1, 2)
            lax.fori_loop(0, model // 256, flip, 0, unroll=2)
            if n == 1:
                x_load(3).start()

            def piece(f, c):
                at = pl.ds(pl.multiple_of(f * pair, pair), pair)
                if n == 0:
                    pltpu.make_async_copy(w1.at[at], w1.at[at], w1_sem.at[f]).wait()
                pre = jnp.dot(w1[at, :], xt[...], preferred_element_type=F32)
                hv[n, :, at] = jax.nn.gelu(pre, approximate=True).astype(BF).T
                return c

            if n == 0:
                lax.fori_loop(0, groups // 4, piece, 0)
                load_others()
                lax.fori_loop(groups // 4, groups // 2, piece, 0)
                x_load(2).start()
                o_load.wait()
            else:
                lax.fori_loop(0, groups // 2, piece, 0)
            if n < 3:
                col = pl.multiple_of((x + order[n]) % side * rows, rows)
                hv[n, :, width:] = ov[:, :, pl.ds(col, rows)].reshape(heads, rows).T

        hidden(0)
        for copy in later:
            copy.wait()
        outs(0, 0, cut)
        start(first, 0, 1)
        hidden(1)
        outs(1, 0, cut)
        start(first, 2)
        hidden(2)
        outs(2, 0, cut)
        start(first, 3)
        for copies in (wo_rest, w2_rest):
            arrived(copies, 0, 1)
            start(copies, 3, 4, 5, 6)
        add_far(first, 0, cut)
        hidden(3)

    pl.run_scoped(hidden_layer, pltpu.VMEM((width, model), BF), pltpu.VMEM((2, rows, model), BF), pltpu.VMEM((model, rows), BF))

    def o_copy(k):
        to = (me + 1 + k) % groups
        return pltpu.make_async_remote_copy(
            src_ref=made.at[k], dst_ref=oo.at[me], send_sem=o_send.at[k], recv_sem=o_recv.at[k],
            device_id={"y": to // cores, "core": to % cores}, device_id_type=MESH)

    def own_rows(qkv, kaug, qaug, scores):
        depth = kaug.shape[1]
        scale = hd ** -0.5 * math.log2(math.e)
        fetch = pltpu.make_async_copy(qkv_ref, qkv, load.at[7])
        fetch.start()
        fetch.wait()
        pad = jnp.zeros((depth - 3 * hd, TK), BF)

        def spread(t, c):
            g = t * TK // toks
            kt = qkv[g, hd:2 * hd, pl.ds(pl.multiple_of(t * TK - g * toks, TK), TK)]
            kaug[pl.ds(pl.multiple_of(t * TK, TK), TK), :] = jnp.concatenate([kt, kt, kt, pad], axis=0).T
            return c

        lax.fori_loop(0, keys // TK, spread, 0, unroll=4)
        qaug[3 * hd:, :] = jnp.zeros((depth - 3 * hd, rows), BF)

        def fold(piece, op):
            return op(piece.reshape(piece.shape[0] // 8, 8, rows), axis=0)

        def block(k, c):
            dest = (me + 1 + k) % groups
            qt = qkv[x * cores + dest % cores, 0:hd, pl.ds(pl.multiple_of(dest // cores * rows, rows), rows)].astype(F32) * scale
            hi = qt.astype(BF)
            left_over = qt - hi.astype(F32)
            mid = left_over.astype(BF)
            qaug[0:hd, :] = hi
            qaug[hd:2 * hd, :] = mid
            qaug[2 * hd:3 * hd, :] = (left_over - mid.astype(F32)).astype(BF)

            def score(t, m8):
                at = pl.ds(pl.multiple_of(t * 2 * toks, 2 * toks), 2 * toks)
                s = jnp.dot(kaug[at, :], qaug[...], preferred_element_type=F32)
                scores[at, :] = s
                return jnp.maximum(m8, fold(s, jnp.max))

            m8 = lax.fori_loop(0, groups // 2, score, jnp.full((8, rows), -jnp.inf, F32))
            m = jnp.max(m8, axis=0, keepdims=True)

            def weigh(g, carry):
                l8, acc = carry
                ps = []
                for r in range(0, toks, ROWS):
                    p = jnp.exp2(scores[pl.ds(pl.multiple_of(g * toks, toks) + r, ROWS), :] - m)
                    l8 = l8 + fold(p, jnp.sum)
                    ps.append(p.astype(BF))
                return l8, acc + jnp.dot(qkv[g, 2 * hd:3 * hd, :], jnp.concatenate(ps, axis=0), preferred_element_type=F32)

            l8, acc = lax.fori_loop(0, groups, weigh, (jnp.zeros((8, rows), F32), jnp.zeros((hd, rows), F32)))
            made[k] = (acc / jnp.sum(l8, axis=0, keepdims=True)).astype(BF)

            @pl.when(k < groups - 1)
            def _():
                o_copy(k).start()

            return c

        lax.fori_loop(0, 1, block, 0)
        for copies in (wo_rest, w2_rest):
            arrived(copies, 3, 4)
            start(copies, 7)
        lax.fori_loop(1, 2, block, 0)
        rest_own.wait()
        wo_rest_own.wait()
        arrived(wo_rest, 2, 5, 6, 7)
        arrived(w2_rest, 2, 5, 6, 7)
        outs(0, cut, model)
        start(second, 0, 1)
        outs(1, cut, model)
        start(second, 2)
        outs(2, cut, model)
        start(second, 3)
        lax.fori_loop(2, groups, block, 0)

    pl.run_scoped(own_rows, pltpu.VMEM((groups, 3 * hd, toks), BF), pltpu.VMEM((keys, 256), BF), pltpu.VMEM((256, rows), BF),
                  pltpu.VMEM((keys, rows), F32))
    add_far(second, cut, model)
    oo[me] = made[groups - 1]
    for k in range(groups - 1):
        o_copy(k).wait()
    hv[3, :, width:] = oo[...].reshape(heads, rows).T
    outs(3, 0, model)
    res_load.wait()
    part[0] += res[...].astype(F32)
    for put in first[2:] + second[2:]:
        put.wait()
    for copy in w2_rest + wo_rest:
        copy.wait_send()
    y_ref[...] = (part[0] + near[0] + near[1]).astype(BF)


def mlp(x_loc, wide, oin, qkv, own, full, cores, side):
    rows, model = x_loc.shape
    groups = side * cores
    width, heads = groups * own[0].shape[0], groups * own[2].shape[0]
    anywhere = pl.BlockSpec(memory_space=pl.ANY)
    dma = lambda n: pltpu.SemaphoreType.DMA((n,))
    flops = 2 * side * rows * model * (2 * width + heads)
    return pl.pallas_call(
        functools.partial(mlp_kernel, side, cores),
        in_specs=[anywhere] * 10,
        out_specs=pl.BlockSpec(memory_space=pltpu.VMEM),
        out_shape=jax.ShapeDtypeStruct((rows, model), BF),
        scratch_shapes=[
            pltpu.VMEM((width + heads, model), BF),
            pltpu.VMEM(oin.shape, BF),
            pltpu.VMEM(oin.shape[:2] + (rows,), BF),
            pltpu.VMEM(oin.shape[:2] + (rows,), BF),
            pltpu.VMEM((side, rows, width + heads), BF),
            pltpu.VMEM((3, rows, model), F32),
            pltpu.VMEM((2, rows // 2, model), F32),
            pltpu.VMEM((2, rows, model), F32),
            pltpu.VMEM((rows, model), BF),
            dma(9), dma(groups // 2), dma(12), dma(12), dma(8), dma(8), dma(8), dma(8), dma(groups - 1), dma(groups - 1),
        ],
        compiler_params=pltpu.CompilerParams(vmem_limit_bytes=67043328, collective_id=1, has_side_effects=True),
        cost_estimate=pl.CostEstimate(flops=flops, bytes_accessed=4 * model * width, transcendentals=side * rows * width),
        name="mlp",
    )(wide, oin, qkv, *own, *full, x_loc)


def solution(mesh):
    data, tp = mesh.devices.shape
    side = math.isqrt(tp // 2)
    cores = tp // (side * side)
    grid = Mesh(mesh.devices.reshape(data, side, side, cores), ("data", "y", "x", "core"))

    def local_block(x_loc, ln_gamma, w_qkv, w_out, w_up, w_down):
        own = (w_up.T, w_down, w_out[0])
        oin, wide, w1, w2, wo, qkv = front(x_loc, ln_gamma, w_qkv[:, 0, :].T, own, cores, side)
        return mlp(x_loc, wide, oin, qkv, own, (w1, w2, wo), cores, side)

    row_spec = P(("data", "y", "x", "core"), None)
    tp_axes = ("y", "x", "core")
    return jax.shard_map(
        local_block,
        mesh=grid,
        in_specs=(row_spec, P(None), P(None, tp_axes, None), P(tp_axes, None, None), P(None, tp_axes), P(tp_axes, None)),
        out_specs=row_spec,
        check_vma=False,
    )
```

```python
import functools
import math
import jax
import jax.numpy as jnp
from jax import lax
from jax.experimental import pallas as pl
from jax.experimental.pallas import tpu as pltpu
from jax.sharding import Mesh, PartitionSpec as P

LN_EPS = 1e-6
BF = jnp.bfloat16
MESH = pl.DeviceIdType.MESH
F32 = jnp.float32
TK = 256
TRIP = 32
ROWS = 64


def ring(own, slot, axis, split, send, recv):
    side, cores = lax.axis_size(axis), lax.axis_size("core")
    at, core = lax.axis_index(axis), lax.axis_index("core")
    other = (core + 1) % cores
    block = lambda hop: slot((at + hop) % side * cores + core)
    head, tail = pl.ds(0, split), pl.ds(split, own.shape[0] - split)
    nxt, prv, sib = {axis: (at + 1) % side}, {axis: (at + side - 1) % side}, {"core": other}
    plan = (
        (own, block(0), nxt),
        (own, block(0), prv),
        (own, block(0), sib),
        (block(side - 1).at[head], block(side - 1).at[head], nxt),
        (block(1).at[tail], block(1).at[tail], prv),
        (block(side - 1), block(side - 1), sib),
        (block(1), block(1), sib),
        (block(2), block(2), sib),
    )
    return [
        pltpu.make_async_remote_copy(
            src_ref=src, dst_ref=dst, send_sem=send.at[n], recv_sem=recv.at[n], device_id=to, device_id_type=MESH)
        for n, (src, dst, to) in enumerate(plan)
    ]


def start(copies, *which):
    for n in which:
        copies[n].start()


def arrived(copies, *which):
    for n in which:
        copies[n].wait_recv()


def hail(*places):
    barrier = pltpu.get_barrier_semaphore()
    for place in places:
        pl.semaphore_signal(barrier, inc=1, device_id=place, device_id_type=MESH)
    return lambda: pl.semaphore_wait(barrier, len(places))


def front_kernel(side, cores, hd, x_ref, gain_ref, wq_ref, w1_ref, w2_ref, wo_ref, oin_ref, wide_ref, w1_full, w2_full, wo_full, qkv_ref,
                 wv, xv, qk, qkv, qaug, acc_ref, m_ref, wq_send, wq_recv, xs_send, xs_recv, w1_send, w1_recv, a_send, a_recv, o_send, o_recv,
                 xw_send, xw_recv, w2_send, w2_recv, wo_send, wo_recv, local):
    y, x, core = lax.axis_index("y"), lax.axis_index("x"), lax.axis_index("core")
    rows, model = x_ref.shape
    groups, toks = side * cores, side * rows
    keys = groups * toks
    bq = toks // 2
    subs = bq // rows
    scale = hd ** -0.5 * math.log2(math.e)
    depth = qaug.shape[1]
    pad = depth - 3 * hd
    chunk = min(TRIP * TK, keys)
    row_me, col_me = x * cores + core, y * cores + core
    up, down = {"y": (y + 1) % side}, {"y": (y + side - 1) % side}
    right, left = {"x": (x + 1) % side}, {"x": (x + side - 1) % side}
    top, low = pl.ds(0, rows // 2), pl.ds(rows // 2, rows // 2)
    apart = [(d, dc) for d in range(side) for dc in range(cores) if d or dc]
    met = hail(
        *[{"x": (x + d) % side, "core": (core + dc) % cores} for d, dc in apart],
        *[{"y": (y + d) % side, "core": (core + dc) % cores} for d, dc in apart if d])

    wq = ring(wq_ref, lambda n: wv.at[n], "x", wq_ref.shape[0] // 32 * 16, wq_send, wq_recv)
    w1 = ring(w1_ref, lambda n: w1_full.at[n], "y", w1_ref.shape[0] // 2, w1_send, w1_recv)
    w2 = ring(w2_ref.at[:, pl.ds(0, w2_full.shape[2])], lambda n: w2_full.at[n], "y", w2_ref.shape[0] // 2, w2_send, w2_recv)
    wo = ring(wo_ref.at[:, pl.ds(0, wo_full.shape[2])], lambda n: wo_full.at[n], "y", wo_ref.shape[0] // 32 * 16, wo_send, wo_recv)

    def put(src, dst, send, recv, n, to):
        return pltpu.make_async_remote_copy(
            src_ref=src, dst_ref=dst, send_sem=send.at[n], recv_sem=recv.at[n], device_id=to, device_id_type=MESH)

    before, after, far = (y + side - 1) % side, (y + 1) % side, (y + 2) % side

    def xs_copy(n):
        part = (xv.at[y], xv.at[y], xv.at[before, top], xv.at[after, low])[n]
        return put(part, part, xs_send, xs_recv, n, down if n % 2 else up)

    def xw_copy(n):
        src = (xv.at[y], xv.at[y], wide_ref.at[3, top], wide_ref.at[1, low])[n]
        dst = (wide_ref.at[3], wide_ref.at[1], wide_ref.at[2, top], wide_ref.at[2, low])[n]
        return put(src, dst, xw_send, xw_recv, n, left if n % 2 else right)

    hops = side - 1

    def place(p):
        return (col_me + 1 + p // hops) % groups, (x + 1 + (p % hops + 1) % hops) % side

    def o_block(p):
        return qk.at[p // 4, pl.ds(0, hd), pl.ds(pl.multiple_of(p % 4 * rows, rows), rows)], oin_ref.at[col_me, :, cols(place(p)[1])]

    def o_copy(p):
        to = place(p)[0]
        return put(*o_block(p), o_send, o_recv, p, {"y": to // cores, "core": to % cores})

    def o_keep(p):
        return pltpu.make_async_copy(*o_block(p), local.at[3])

    def head_of(n):
        return (x + n // cores) % side * cores + (core + n) % cores

    qk_rows, v_rows = pl.ds(0, 2 * hd), pl.ds(2 * hd, hd)

    def cols(part):
        return pl.ds(pl.multiple_of(part * rows, rows), rows)

    def home(n, kind, at):
        head = head_of(n)
        return put(qk.at[head, (qk_rows, v_rows)[kind], at], qkv.at[row_me, (qk_rows, v_rows)[kind], at],
                   a_send.at[kind], a_recv.at[kind], n, {"x": head // cores, "core": head % cores})

    own_x = pltpu.make_async_copy(x_ref, xv.at[y], local.at[0])
    own_wq = pltpu.make_async_copy(wq_ref, wv.at[row_me], local.at[1])
    own_x.start()
    own_wq.start()

    def project(xt):
        def norm(r, c):
            at = pl.ds(pl.multiple_of(r * 32, 32), 32)
            row = xv[y, at, :].astype(F32)
            mean = jnp.mean(row, axis=-1, keepdims=True)
            centered = row - mean
            var = jnp.mean(centered * centered, axis=-1, keepdims=True)
            xv[y, at, :] = (centered * lax.rsqrt(var + LN_EPS) * gain_ref[...].reshape(1, model)).astype(BF)
            return c

        def flip(part):
            def piece(k, c):
                at = pl.ds(pl.multiple_of(k * 256, 256), 256)
                xt[at, cols(part)] = xv[part, :, at].T
                return c

            lax.fori_loop(0, model // 256, piece, 0, unroll=2)

        def work(count, pick, parts, go=True):
            def body(k, c):
                n = pick(k)
                for part in parts:
                    qk[head_of(n), :, cols(part)] = jnp.dot(
                        wv[head_of(n)], xt[:, cols(part)], preferred_element_type=F32).astype(BF)
                if go:
                    for part in parts:
                        home(n, 0, cols(part)).start()
                return c

            lax.fori_loop(0, count, body, 0)

        close = lambda k: cores * (1 + 2 * (k // cores)) + k % cores
        distant = lambda k: 2 * cores + k
        here = lambda k: k

        own_x.wait()
        lax.fori_loop(0, rows // 32, norm, 0)
        flip(y)
        met()
        start(wq, 0, 1, 2)
        xs_copy(0).start()
        xs_copy(1).start()
        start(w1, 2)
        keep = pltpu.make_async_copy(xv.at[y], wide_ref.at[0], local.at[2])
        keep.start()
        arrived(wq, 0, 1)
        start(wq, 3, 4, 5, 6)
        xs_copy(0).wait_recv()
        xs_copy(1).wait_recv()
        xs_copy(2).start()
        xs_copy(3).start()
        start(w1, 0, 1)
        start(wo, 0, 1, 2)
        start(w2, 0, 1, 2)
        flip(before)
        flip(after)
        own_wq.wait()
        arrived(wq, 2, 5, 6)
        work(2 * cores, close, (y, after, before))
        arrived(wq, 3, 4)
        start(wq, 7)
        work(cores, here, (y, after, before), go=False)
        arrived(wq, 7)
        work(cores, distant, (y, after, before))
        xs_copy(2).wait_recv()
        xs_copy(3).wait_recv()
        flip(far)
        work(cores, distant, (far,))
        work(2 * cores, close, (far,))
        work(cores, here, (far,), go=False)
        everything = pl.ds(0, toks)
        for n in range(1, cores):
            home(n, 0, everything).start()
            home(n, 1, everything).start()
        for k in range(cores):
            home(distant(k), 1, everything).start()
        for k in range(2 * cores):
            home(close(k), 1, everything).start()
        qkv[row_me] = qk[row_me]
        keep.wait()
        for n in range(4):
            xs_copy(n).wait_send()
        for copy in wq:
            copy.wait_send()

    pl.run_scoped(project, pltpu.VMEM((model, toks), BF))
    xw_copy(0).start()
    xw_copy(1).start()
    everything = pl.ds(0, toks)
    kept_qkv = pltpu.make_async_copy(qkv, qkv_ref, local.at[4])

    def attend(kaug, s_a, s_b):
        def load_query(b, slot):
            b = jnp.minimum(b, hops * groups // subs - 1)
            for j in range(subs):
                dest, column = place(b * subs + j)
                g = column * cores + dest % cores
                qt = qkv[g, 0:hd, cols(dest // cores)].astype(F32) * scale
                hi = qt.astype(BF)
                rest = qt - hi.astype(F32)
                mid = rest.astype(BF)
                at = slice(j * rows, (j + 1) * rows)
                qaug[slot, 0:hd, at] = hi
                qaug[slot, hd:2 * hd, at] = mid
                qaug[slot, 2 * hd:3 * hd, at] = (rest - mid.astype(F32)).astype(BF)

        def fold(piece, op):
            return op(piece.reshape(piece.shape[0] // 8, 8, bq), axis=0)

        def spread(t, c):
            g = t * TK // toks
            t0 = pl.multiple_of(t * TK - g * toks, TK)
            kt = qkv[g, hd:2 * hd, pl.ds(t0, TK)]
            kaug[pl.ds(pl.multiple_of(t * TK, TK), TK), :] = jnp.concatenate([kt, kt, kt, jnp.zeros((pad, TK), BF)], axis=0).T
            return c

        def first(c, m8):
            at = pl.ds(pl.multiple_of(c * 8 * TK, 8 * TK), 8 * TK)
            s = jnp.dot(kaug[at, :], qaug[0], preferred_element_type=F32)
            s_a[at, :] = s
            return jnp.maximum(m8, fold(s, jnp.max))

        def half(i, s_in, s_out, slot, col):
            m = m_ref[0:1, :]
            acc_ref[...] = jnp.zeros_like(acc_ref)

            def trip(c, carry):
                m8, l8 = carry
                k0 = pl.multiple_of(c * chunk, chunk)
                total = None
                for u in range(chunk // TK):
                    s_new = jnp.dot(kaug[pl.ds(k0 + u * TK, TK), :], qaug[slot], preferred_element_type=F32)
                    ps = []
                    for r in range(0, TK, ROWS):
                        p = jnp.exp2(s_in[pl.ds(k0 + u * TK + r, ROWS), :] - m)
                        l8 = l8 + fold(p, jnp.sum)
                        ps.append(p.astype(BF))
                    at = u * TK % toks
                    vt = qkv[k0 // toks + u * TK // toks, 2 * hd:3 * hd, at:at + TK]
                    d = jnp.dot(vt, jnp.concatenate(ps, axis=0), preferred_element_type=F32)
                    total = d if total is None else total + d
                    for r in range(0, TK, ROWS):
                        piece = s_new[r:r + ROWS]
                        m8 = jnp.maximum(m8, fold(piece, jnp.max))
                        s_out[pl.ds(k0 + u * TK + r, ROWS), :] = piece
                acc_ref[...] += total
                return m8, l8

            m8, l8 = lax.fori_loop(0, (1 + x // side) * (keys // chunk), trip,
                                   (jnp.full((8, bq), -jnp.inf, F32), jnp.zeros((8, bq), F32)))
            qk[i, 0:hd, col:col + bq] = (acc_ref[...] / jnp.sum(l8, axis=0, keepdims=True)).astype(BF)
            m_ref[...] = jnp.broadcast_to(jnp.max(m8, axis=0, keepdims=True), (8, bq))

        for n in range(1, groups):
            home(n, 0, everything).wait()
        lax.fori_loop(0, keys // TK, spread, 0, unroll=4)
        qaug[:, 3 * hd:, :] = jnp.zeros((2, pad, bq), BF)
        load_query(0, 0)
        load_query(1, 1)
        m8 = lax.fori_loop(0, keys // (8 * TK), first, jnp.full((8, bq), -jnp.inf, F32))
        m_ref[...] = jnp.broadcast_to(jnp.max(m8, axis=0, keepdims=True), (8, bq))
        arrived(w1, 0, 1)
        start(w1, 3, 4, 5, 6)
        for n in range(1, groups):
            home(n, 1, everything).wait()
        kept_qkv.start()
        steps = hops * groups // 4

        def step(i, c):
            @pl.when(i == steps // 2)
            def _():
                xw_copy(0).wait()
                xw_copy(1).wait()
                xw_copy(2).start()
                xw_copy(3).start()
                for copies in (wo, w2):
                    arrived(copies, 0, 1)
                    start(copies, 3, 4, 5, 6)

            half(i, s_a, s_b, 1, 0)
            load_query(2 * i + 2, 0)

            @pl.when(i == steps // 2 + 1)
            def _():
                arrived(w1, 3, 4)
                start(w1, 7)

            half(i, s_b, s_a, 0, bq)
            load_query(2 * i + 3, 1)

            def leave(j, c):
                p = 4 * i + j

                @pl.when(p < hops * (groups - 1))
                def _():
                    o_copy(p).start()

                @pl.when(p >= hops * (groups - 1))
                def _():
                    o_keep(p).start()

                return c

            return lax.fori_loop(0, 4, leave, c)

        lax.fori_loop(0, steps, step, 0)

    pl.run_scoped(attend, pltpu.VMEM((keys, depth), BF), pltpu.VMEM((keys, bq), F32), pltpu.VMEM((keys, bq), F32))
    for copies in (wo, w2):
        arrived(copies, 3, 4)
        start(copies, 7)
    xw_copy(2).wait()
    xw_copy(3).wait()
    for p in range(hops * (groups - 1)):
        o_copy(p).wait()
    all_kept = oin_ref.at[col_me, :, pl.ds(0, hops * rows)]
    pltpu.make_async_copy(all_kept, all_kept, local.at[3]).wait()
    kept_qkv.wait()
    arrived(w1, 2, 5, 6, 7)
    for copies in (wo, w2):
        arrived(copies, 2, 5, 6, 7)
    for copies in (wo, w2, w1):
        for copy in copies:
            copy.wait_send()


def front(x_loc, gain, wq, own, cores, side):
    rows, model = x_loc.shape
    w1, w2, wo = own
    groups, toks = side * cores, side * rows
    hd = wq.shape[0] // 3
    keys, bq = groups * toks, toks // 2
    anywhere = pl.BlockSpec(memory_space=pl.ANY)
    dma = lambda *n: pltpu.SemaphoreType.DMA(n)
    flops = 2 * toks * model * groups * wq.shape[0] + 6 * keys * keys * hd
    return pl.pallas_call(
        functools.partial(front_kernel, side, cores, hd),
        in_specs=[anywhere, pl.BlockSpec(memory_space=pltpu.VMEM)] + [anywhere] * 4,
        out_specs=[anywhere] * 6,
        out_shape=[
            jax.ShapeDtypeStruct((groups, hd, toks), BF),
            jax.ShapeDtypeStruct((side, rows, model), BF),
            jax.ShapeDtypeStruct((groups,) + w1.shape, BF),
            jax.ShapeDtypeStruct((groups, w2.shape[0], first_columns(model)), BF),
            jax.ShapeDtypeStruct((groups, wo.shape[0], first_columns(model)), BF),
            jax.ShapeDtypeStruct((groups, 3 * hd, toks), BF),
        ],
        scratch_shapes=[
            pltpu.VMEM((groups,) + wq.shape, BF),
            pltpu.VMEM((side, rows, model), BF),
            pltpu.VMEM((groups, 3 * hd, toks), BF),
            pltpu.VMEM((groups, 3 * hd, toks), BF),
            pltpu.VMEM((2, 256, bq), BF),
            pltpu.VMEM((hd, bq), F32),
            pltpu.VMEM((8, bq), F32),
            dma(8), dma(8), dma(4), dma(4), dma(8), dma(8), dma(2, groups), dma(2, groups),
            dma((side - 1) * (groups - 1)), dma((side - 1) * (groups - 1)), dma(4), dma(4), dma(8), dma(8), dma(8), dma(8), dma(5),
        ],
        compiler_params=pltpu.CompilerParams(
            vmem_limit_bytes=67043328, collective_id=0, has_side_effects=True),
        cost_estimate=pl.CostEstimate(flops=flops, bytes_accessed=4 * w1.size, transcendentals=keys * keys),
        name="front",
    )(x_loc, gain, wq, w1, w2, wo)


def first_columns(model):
    return model // 2 // 256 * 256


def mlp_kernel(side, cores, wide_ref, oin_ref, qkv_ref, w1_own, w2_own, wo_own, w1_ref, w2_ref, wo_ref, res_ref, y_ref, w2, ov, oo, made, hv,
               part, far, near, res, load, w1_sem, send, recv, w2_send, w2_recv, wo_send, wo_recv, o_send, o_recv):
    x, y, core = lax.axis_index("x"), lax.axis_index("y"), lax.axis_index("core")
    right, left = {"x": (x + 1) % side}, {"x": (x + side - 1) % side}
    _, rows, model = wide_ref.shape
    groups, hd, toks = oin_ref.shape
    width = groups * w1_own.shape[0]
    heads = groups * hd
    keys = groups * toks
    cut = w2_ref.shape[2]
    step = math.gcd(cut, model - cut, 512)
    half = rows // 2
    me = y * cores + core
    top, low = pl.ds(0, half), pl.ds(half, half)
    order = (2, 1, 3, 0)
    pair = 2 * w1_own.shape[0]
    met = hail(right, left, *[
        {"y": (me + hop) % groups // cores, "core": (me + hop) % cores} for hop in range(1, groups)])

    def shard(into, base, size, n, columns):
        return into.at[pl.ds(pl.multiple_of(base + n * size, 16), size), columns]

    def gathered(own, full, into, base, sem):
        size, columns = full.shape[1], pl.ds(0, full.shape[2])
        for hop in range(groups):
            n = (me + hop) % groups
            pltpu.make_async_copy(full.at[n] if hop else own.at[:, columns], shard(into, base, size, n, columns), sem).start()
        whole = into.at[pl.ds(base, groups * size), columns]
        return pltpu.make_async_copy(whole, whole, sem)

    rest = pl.ds(cut, model - cut)
    o_load = pltpu.make_async_copy(oin_ref, ov, load.at[2])
    res_load = pltpu.make_async_copy(res_ref, res, load.at[3])
    rest_own = pltpu.make_async_copy(w2_own.at[:, rest], shard(w2, 0, width // groups, me, rest), load.at[4])
    wo_rest_own = pltpu.make_async_copy(wo_own.at[:, rest], shard(w2, width, hd, me, rest), load.at[8])
    w2_rest = ring(w2_own.at[:, rest], lambda n: shard(w2, 0, width // groups, n, rest), "y", width // groups // 2, w2_send, w2_recv)
    wo_rest = ring(wo_own.at[:, rest], lambda n: shard(w2, width, hd, n, rest), "y", hd // 32 * 16, wo_send, wo_recv)

    def outs(n, lo, hi):
        def piece(d, c):
            at = pl.ds(pl.multiple_of(d * step, step), step)
            part[n % 3, :, at] = jnp.dot(hv[n], w2[:, at], preferred_element_type=F32)
            return c

        lax.fori_loop(lo // step, hi // step, piece, 0)

    def plan(lo, hi, first):
        cols = pl.ds(lo, hi - lo)
        copies = (
            (part.at[0, top, cols], far.at[0, :, cols], right),
            (part.at[0, low, cols], far.at[1, :, cols], left),
            (part.at[1, low, cols], near.at[0, low, cols], right),
            (part.at[2, top, cols], near.at[1, top, cols], left),
            (part.at[1, top, cols], near.at[0, top, cols], right),
            (part.at[2, low, cols], near.at[1, low, cols], left),
        )
        return [
            pltpu.make_async_remote_copy(src_ref=src, dst_ref=dst, send_sem=send.at[first + n], recv_sem=recv.at[first + n],
                                         device_id=to, device_id_type=MESH)
            for n, (src, dst, to) in enumerate(copies)
        ]

    def add_far(puts, lo, hi):
        puts[0].wait()
        part[1, :half, lo:hi] += far[0, :, lo:hi]
        start(puts, 4)
        puts[1].wait()
        part[2, half:, lo:hi] += far[1, :, lo:hi]
        start(puts, 5)

    first, second = plan(0, cut, 0), plan(cut, model, 6)

    def hidden_layer(w1, xv, xt):
        def x_load(n):
            return pltpu.make_async_copy(wide_ref.at[order[n]], xv.at[n % 2], load.at[n % 2])

        def w1_shard(n):
            to = shard(w1, 0, pair // 2, n, pl.ds(0, model))

            @pl.when(n == me)
            def _():
                pltpu.make_async_copy(w1_own, to, w1_sem.at[n // 2]).start()

            @pl.when(n != me)
            def _():
                pltpu.make_async_copy(w1_ref.at[n], to, w1_sem.at[n // 2]).start()

        x_load(0).start()
        for n in range(groups):
            w1_shard(n)
        o_load.start()
        later = []

        def load_others():
            later.append(gathered(w2_own, w2_ref, w2, 0, load.at[5]))
            later.append(gathered(wo_own, wo_ref, w2, width, load.at[6]))
            x_load(1).start()
            rest_own.start()
            wo_rest_own.start()
            res_load.start()

        def hidden(n):
            x_load(n).wait()

            def flip(k, c):
                at = pl.ds(pl.multiple_of(k * 256, 256), 256)
                xt[at, :] = xv[n % 2, :, at].T
                return c

            if n == 0:
                met()
                start(wo_rest, 0, 1, 2)
                start(w2_rest, 0, 1, 2)
            lax.fori_loop(0, model // 256, flip, 0, unroll=2)
            if n == 1:
                x_load(3).start()

            def piece(f, c):
                at = pl.ds(pl.multiple_of(f * pair, pair), pair)
                if n == 0:
                    pltpu.make_async_copy(w1.at[at], w1.at[at], w1_sem.at[f]).wait()
                pre = jnp.dot(w1[at, :], xt[...], preferred_element_type=F32)
                hv[n, :, at] = jax.nn.gelu(pre, approximate=True).astype(BF).T
                return c

            if n == 0:
                lax.fori_loop(0, groups // 4, piece, 0)
                load_others()
                lax.fori_loop(groups // 4, groups // 2, piece, 0)
                x_load(2).start()
                o_load.wait()
            else:
                lax.fori_loop(0, groups // 2, piece, 0)
            if n < 3:
                col = pl.multiple_of((x + order[n]) % side * rows, rows)
                hv[n, :, width:] = ov[:, :, pl.ds(col, rows)].reshape(heads, rows).T

        hidden(0)
        for copy in later:
            copy.wait()
        outs(0, 0, cut)
        start(first, 0, 1)
        hidden(1)
        outs(1, 0, cut)
        start(first, 2)
        hidden(2)
        outs(2, 0, cut)
        start(first, 3)
        for copies in (wo_rest, w2_rest):
            arrived(copies, 0, 1)
            start(copies, 3, 4, 5, 6)
        add_far(first, 0, cut)
        hidden(3)

    pl.run_scoped(hidden_layer, pltpu.VMEM((width, model), BF), pltpu.VMEM((2, rows, model), BF), pltpu.VMEM((model, rows), BF))

    def o_copy(k):
        to = (me + 1 + k) % groups
        return pltpu.make_async_remote_copy(
            src_ref=made.at[k], dst_ref=oo.at[me], send_sem=o_send.at[k], recv_sem=o_recv.at[k],
            device_id={"y": to // cores, "core": to % cores}, device_id_type=MESH)

    def own_rows(qkv, kaug, qaug, scores):
        depth = kaug.shape[1]
        scale = hd ** -0.5 * math.log2(math.e)
        fetch = pltpu.make_async_copy(qkv_ref, qkv, load.at[7])
        fetch.start()
        fetch.wait()
        pad = jnp.zeros((depth - 3 * hd, TK), BF)

        def spread(t, c):
            g = t * TK // toks
            kt = qkv[g, hd:2 * hd, pl.ds(pl.multiple_of(t * TK - g * toks, TK), TK)]
            kaug[pl.ds(pl.multiple_of(t * TK, TK), TK), :] = jnp.concatenate([kt, kt, kt, pad], axis=0).T
            return c

        lax.fori_loop(0, keys // TK, spread, 0, unroll=4)
        qaug[3 * hd:, :] = jnp.zeros((depth - 3 * hd, rows), BF)

        def fold(piece, op):
            return op(piece.reshape(piece.shape[0] // 8, 8, rows), axis=0)

        def block(k, c):
            dest = (me + 1 + k) % groups
            qt = qkv[x * cores + dest % cores, 0:hd, pl.ds(pl.multiple_of(dest // cores * rows, rows), rows)].astype(F32) * scale
            hi = qt.astype(BF)
            left_over = qt - hi.astype(F32)
            mid = left_over.astype(BF)
            qaug[0:hd, :] = hi
            qaug[hd:2 * hd, :] = mid
            qaug[2 * hd:3 * hd, :] = (left_over - mid.astype(F32)).astype(BF)

            def score(t, m8):
                at = pl.ds(pl.multiple_of(t * 2 * toks, 2 * toks), 2 * toks)
                s = jnp.dot(kaug[at, :], qaug[...], preferred_element_type=F32)
                scores[at, :] = s
                return jnp.maximum(m8, fold(s, jnp.max))

            m8 = lax.fori_loop(0, groups // 2, score, jnp.full((8, rows), -jnp.inf, F32))
            m = jnp.max(m8, axis=0, keepdims=True)

            def weigh(g, carry):
                l8, acc = carry
                ps = []
                for r in range(0, toks, ROWS):
                    p = jnp.exp2(scores[pl.ds(pl.multiple_of(g * toks, toks) + r, ROWS), :] - m)
                    l8 = l8 + fold(p, jnp.sum)
                    ps.append(p.astype(BF))
                return l8, acc + jnp.dot(qkv[g, 2 * hd:3 * hd, :], jnp.concatenate(ps, axis=0), preferred_element_type=F32)

            l8, acc = lax.fori_loop(0, groups, weigh, (jnp.zeros((8, rows), F32), jnp.zeros((hd, rows), F32)))
            made[k] = (acc / jnp.sum(l8, axis=0, keepdims=True)).astype(BF)

            @pl.when(k < groups - 1)
            def _():
                o_copy(k).start()

            return c

        lax.fori_loop(0, 1, block, 0)
        for copies in (wo_rest, w2_rest):
            arrived(copies, 3, 4)
            start(copies, 7)
        lax.fori_loop(1, 2, block, 0)
        rest_own.wait()
        wo_rest_own.wait()
        arrived(wo_rest, 2, 5, 6, 7)
        arrived(w2_rest, 2, 5, 6, 7)
        outs(0, cut, model)
        start(second, 0, 1)
        outs(1, cut, model)
        start(second, 2)
        outs(2, cut, model)
        start(second, 3)
        lax.fori_loop(2, groups, block, 0)

    pl.run_scoped(own_rows, pltpu.VMEM((groups, 3 * hd, toks), BF), pltpu.VMEM((keys, 256), BF), pltpu.VMEM((256, rows), BF),
                  pltpu.VMEM((keys, rows), F32))
    add_far(second, cut, model)
    oo[me] = made[groups - 1]
    for k in range(groups - 1):
        o_copy(k).wait()
    hv[3, :, width:] = oo[...].reshape(heads, rows).T
    outs(3, 0, model)
    res_load.wait()
    part[0] += res[...].astype(F32)
    for put in first[2:] + second[2:]:
        put.wait()
    for copy in w2_rest + wo_rest:
        copy.wait_send()
    y_ref[...] = (part[0] + near[0] + near[1]).astype(BF)


def mlp(x_loc, wide, oin, qkv, own, full, cores, side):
    rows, model = x_loc.shape
    groups = side * cores
    width, heads = groups * own[0].shape[0], groups * own[2].shape[0]
    anywhere = pl.BlockSpec(memory_space=pl.ANY)
    dma = lambda n: pltpu.SemaphoreType.DMA((n,))
    flops = 2 * side * rows * model * (2 * width + heads)
    return pl.pallas_call(
        functools.partial(mlp_kernel, side, cores),
        in_specs=[anywhere] * 10,
        out_specs=pl.BlockSpec(memory_space=pltpu.VMEM),
        out_shape=jax.ShapeDtypeStruct((rows, model), BF),
        scratch_shapes=[
            pltpu.VMEM((width + heads, model), BF),
            pltpu.VMEM(oin.shape, BF),
            pltpu.VMEM(oin.shape[:2] + (rows,), BF),
            pltpu.VMEM(oin.shape[:2] + (rows,), BF),
            pltpu.VMEM((side, rows, width + heads), BF),
            pltpu.VMEM((3, rows, model), F32),
            pltpu.VMEM((2, rows // 2, model), F32),
            pltpu.VMEM((2, rows, model), F32),
            pltpu.VMEM((rows, model), BF),
            dma(9), dma(groups // 2), dma(12), dma(12), dma(8), dma(8), dma(8), dma(8), dma(groups - 1), dma(groups - 1),
        ],
        compiler_params=pltpu.CompilerParams(vmem_limit_bytes=67043328, collective_id=1, has_side_effects=True),
        cost_estimate=pl.CostEstimate(flops=flops, bytes_accessed=4 * model * width, transcendentals=side * rows * width),
        name="mlp",
    )(wide, oin, qkv, *own, *full, x_loc)


def solution(mesh):
    data, tp = mesh.devices.shape
    side = math.isqrt(tp // 2)
    cores = tp // (side * side)
    grid = Mesh(mesh.devices.reshape(data, side, side, cores), ("data", "y", "x", "core"))

    def local_block(x_loc, ln_gamma, w_qkv, w_out, w_up, w_down):
        own = (w_up.T, w_down, w_out[0])
        oin, wide, w1, w2, wo, qkv = front(x_loc, ln_gamma, w_qkv[:, 0, :].T, own, cores, side)
        return mlp(x_loc, wide, oin, qkv, own, (w1, w2, wo), cores, side)

    row_spec = P(("data", "y", "x", "core"), None)
    tp_axes = ("y", "x", "core")
    return jax.shard_map(
        local_block,
        mesh=grid,
        in_specs=(row_spec, P(None), P(None, tp_axes, None), P(tp_axes, None, None), P(None, tp_axes), P(tp_axes, None)),
        out_specs=row_spec,
        check_vma=False,
    )
```
